32 devices in a mesh: grp: 2 (over y), blk: 4 (over z), uly: 4 (over x, core).
Axes of the slice: x: 2, y: 2, z: 4, core: 2. Of those that a mesh axis runs over, the one named last changes fastest.
Arguments:
- qkv: bfloat16 [2, 8, 16, 3, 32, 128], P('grp', 'blk', 'uly'), parts along dimension 0, may hold values from -6 to 6
- out_weight: bfloat16 [4096, 256], replicated, may hold values from -0.25 to 0.25
- lift_weight: bfloat16 [64, 512], P(None, 'uly'), may hold values from -0.75 to 0.75
- conv_weight: bfloat16 [4, 3, 3, 512, 512], P(None, None, None, 'uly'), may hold values from -0.15625 to 0.15625
Outputs:
- pixels: bfloat16 [2, 16, 32, 512], P('grp', 'blk', None, 'uly'), parts along dimension 0
The draws below stay inside these ranges and needn't reach their ends.
There are 2 independent parts, one for each index of `grp`. The reference program is written for one: setup_inputs(seed, part) draws one part's arguments, and reference() takes and returns one part's arrays. A program takes and returns all parts, laid end to end along the dimension named above; an argument that names none is the same for every part. Nothing has to cross between parts.
All inputs are finite; a program needn't handle non-finite values.
Results may differ from the reference program's by a relative error of at most 0.02.
Values may be sent and summed in bfloat16 or wider, within the bound.
No kernel may reach another device: no remote copies, remote signals or barrier semaphores. Data moves between devices by JAX's collectives and lax.ppermute only.
A program may use at most 64 MiB of HBM per device.

```python
import jax
import jax.numpy as jnp
from jax import lax

FRAMES = 1
HEADS = 32
HEAD = 128
PATCH = 2
LATENT = 64
CH = 512
LAYERS = 4
ROWS = 8
COLS = 16


def draw_qkv(key, part):
    shape = (FRAMES, ROWS, COLS, 3, HEADS, HEAD)
    base = jnp.clip(jax.random.normal(key, shape, jnp.float32) * 1.5, -6.0, 6.0)
    return base.astype(jnp.bfloat16)


def steps_of(stream_key, dims, pieces, least, largest):
    def one(axis_at, parts):
        draws = jax.random.uniform(jax.random.fold_in(jax.random.fold_in(stream_key, 6), axis_at), (parts,), jnp.float32, least / len(pieces), largest / len(pieces))
        return jnp.repeat(jnp.exp(draws), dims[axis_at] // parts).reshape((-1,) + (1,) * (len(dims) - axis_at - 1))

    factor_of = one(*pieces[0])
    for cut in pieces[1:]:
        factor_of = factor_of * one(*cut)
    return factor_of


def scatter_about(stream_key, dims, scale, limit, pieces=(), dtype=jnp.bfloat16):
    entries = jax.random.normal(stream_key, dims, jnp.float32) * scale
    if len(pieces) > 0:
        entries = steps_of(stream_key, dims, pieces, -0.22, 0.18) * entries
    return jnp.clip(entries, min=-limit, max=limit).astype(dtype)


def setup_inputs(seed: int = 0, part: int = 0) -> dict:
    streams_of = jax.random.split(jax.random.key(seed), 5)
    part_keys = jax.random.split(jax.random.fold_in(streams_of[4], part), 5)
    qkv = draw_qkv(jax.random.fold_in(jax.random.fold_in(streams_of[4], part), 71), part)
    out_weight = scatter_about(streams_of[1], (HEADS * HEAD, PATCH * PATCH * LATENT), (HEADS * HEAD // 8) ** -0.5, 0.25)
    lift_weight = scatter_about(streams_of[2], (LATENT, CH), LATENT ** -0.5, 0.75, ((1, 4),))
    conv_weight = scatter_about(streams_of[3], (LAYERS, 3, 3, CH, CH), (3 * CH) ** -0.5, 0.15625, ((3, 4),))
    return dict(qkv=qkv, out_weight=out_weight, lift_weight=lift_weight, conv_weight=conv_weight)


def head_attention(operands):
    queries, keys, values = operands
    scale = 1.0 / (queries.shape[-1] ** 0.5)
    scores = jnp.dot(queries.astype(jnp.float32), keys.astype(jnp.float32).T) * scale
    highest = jnp.max(scores, axis=1, keepdims=True)
    weights = jnp.exp(scores - highest)
    totals = jnp.sum(weights, axis=1, keepdims=True)
    rounded = lax.optimization_barrier(weights.astype(jnp.bfloat16))
    mixed = jnp.dot(rounded.astype(jnp.float32), values.astype(jnp.float32)) / totals
    return mixed.astype(jnp.bfloat16)


def reference(qkv, out_weight, lift_weight, conv_weight):
    frames, rows, cols = qkv.shape[0], qkv.shape[1], qkv.shape[2]
    heads, size = qkv.shape[4], qkv.shape[5]
    flat = qkv.reshape(frames * rows * cols, 3, heads, size)
    queries = jnp.transpose(flat[:, 0], (1, 0, 2))
    keys = jnp.transpose(flat[:, 1], (1, 0, 2))
    values = jnp.transpose(flat[:, 2], (1, 0, 2))
    attended = lax.map(head_attention, (queries, keys, values))
    attended = jnp.transpose(attended, (1, 0, 2)).reshape(frames * rows * cols, heads * size)
    patches = jnp.dot(attended, out_weight, preferred_element_type=jnp.float32).astype(jnp.bfloat16)
    latent_ch = lift_weight.shape[0]
    latent = patches.reshape(frames, rows, cols, PATCH, PATCH, latent_ch)
    latent = jnp.transpose(latent, (0, 1, 3, 2, 4, 5)).reshape(frames * rows * PATCH * cols * PATCH, latent_ch)
    lifted = jnp.dot(latent, lift_weight, preferred_element_type=jnp.float32).astype(jnp.bfloat16)
    channels = lift_weight.shape[1]
    current = lifted.reshape(frames, rows * PATCH, cols * PATCH, channels)
    height, width = rows * PATCH, cols * PATCH
    for layer in range(LAYERS):
        padded = jnp.pad(current, ((0, 0), (1, 1), (1, 1), (0, 0))).astype(jnp.float32)
        summed = jnp.zeros((frames, height, width, channels), jnp.float32)
        for above in range(3):
            for beside in range(3):
                window = padded[:, above:above + height, beside:beside + width, :]
                kernel = conv_weight[layer, above, beside].astype(jnp.float32)
                summed = summed + jnp.einsum("fyxc,dc->fyxd", window, kernel)
        current = jax.nn.silu(summed).astype(jnp.bfloat16)
    return current
```

```python
import jax
import jax.numpy as jnp
from jax import lax
from jax.sharding import PartitionSpec as P

PATCH = 2
LAYERS = 4


def swap(pieces, axis):
    count = len(pieces)
    return [pieces[0]] + [
        lax.ppermute(pieces[step], axis, [(i, i ^ step) for i in range(count)])
        for step in range(1, count)
    ]


def spread(piece, axis):
    return swap([piece] * lax.axis_size(axis), axis)


def cut(array, start, size, axis):
    return lax.dynamic_slice_in_dim(array, start, size, axis=axis)


def attend(queries, keys, values):
    scale = 1.0 / queries.shape[-1] ** 0.5
    scores = jnp.einsum("hqd,hkd->hqk", queries, keys, preferred_element_type=jnp.float32) * scale
    weights = jnp.exp(scores - jnp.max(scores, axis=2, keepdims=True))
    totals = jnp.sum(weights, axis=2)
    mixed = jnp.einsum(
        "hqk,hkd->hqd", weights.astype(jnp.bfloat16), values, preferred_element_type=jnp.float32
    )
    return (mixed / totals[:, :, None]).astype(jnp.bfloat16)


def ordered(blocks, me):
    stacked = jnp.stack(blocks)
    return jnp.concatenate(
        [cut(stacked, me ^ place, 1, 0) for place in range(len(blocks))], axis=0
    )


def window_by_swaps(qkv, out_weight, reach):
    frames, rows, cols, _, heads, size = qkv.shape
    lines, sides = lax.axis_size("blk"), lax.axis_size("uly")
    line, side = lax.axis_index("blk"), lax.axis_index("uly")
    group, share = heads // sides, heads // sides // lines
    got = swap([cut(qkv, (side ^ s) * group, group, 4) for s in range(sides)], "uly")
    grouped = jnp.stack(got, axis=3)
    grouped = jnp.transpose(grouped, (4, 5, 0, 1, 3, 2, 6))
    got = swap([cut(grouped, (line ^ t) * share, share, 1) for t in range(lines)], "blk")
    shared = ordered(got, line)
    shared = jnp.transpose(shared, (1, 2, 3, 0, 4, 5, 6, 7))
    flat = shared.reshape(3, share, -1, size)
    attended = attend(flat[0], flat[1], flat[2])
    attended = attended.reshape(share, frames, lines * rows, sides * cols, size)
    attended = jnp.transpose(attended, (1, 2, 3, 0, 4)).reshape(
        frames, lines * rows, sides * cols, share * size
    )
    padded = jnp.pad(attended, ((0, 0), (reach, reach), (0, 0), (0, 0)))
    got = swap([cut(padded, (line ^ t) * rows, rows + 2 * reach, 1) for t in range(lines)], "blk")
    partial = 0.0
    for t in range(lines):
        weight = cut(out_weight, ((side * lines) + (line ^ t)) * share * size, share * size, 0)
        partial = partial + jnp.einsum(
            "frcw,wp->frcp", got[t], weight, preferred_element_type=jnp.float32
        )
    partial = partial.astype(jnp.bfloat16)
    got = spread(partial, "uly")
    blocks = []
    for place in range(sides):
        total = 0.0
        for s in range(sides):
            at = (place ^ s) * cols
            total = total + got[s][:, :, at : at + cols].astype(jnp.float32)
        blocks.append(total.astype(jnp.bfloat16))
    patches = ordered(blocks, side)
    patches = jnp.transpose(patches, (1, 2, 0, 3, 4))
    return patches.reshape(frames, rows + 2 * reach, sides * cols, -1)


def window_by_gathers(qkv, out_weight, reach):
    frames, rows, cols, _, heads, size = qkv.shape
    grouped = lax.all_to_all(qkv, "blk", split_axis=4, concat_axis=1, tiled=True)
    flat = [
        lax.all_gather(grouped[:, :, :, which], "uly", axis=2, tiled=True) for which in (1, 2)
    ]
    flat = [grouped[:, :, :, 0]] + flat
    flat = [jnp.swapaxes(one.reshape(-1, one.shape[3], size), 0, 1) for one in flat]
    attended = jnp.swapaxes(attend(*flat), 0, 1)
    attended = attended.reshape(grouped.shape[:3] + grouped.shape[4:])
    restored = lax.all_to_all(attended, "blk", split_axis=1, concat_axis=3, tiled=True)
    patches = jnp.einsum(
        "frcw,wp->frcp",
        restored.reshape(frames, rows, cols, heads * size),
        out_weight,
        preferred_element_type=jnp.float32,
    ).astype(jnp.bfloat16)
    patches = lax.all_gather(patches, "uly", axis=2, tiled=True)
    patches = lax.all_gather(patches, "blk", axis=1, tiled=True)
    padded = jnp.pad(patches, ((0, 0), (reach, reach), (0, 0), (0, 0)))
    return cut(padded, lax.axis_index("blk") * rows, rows + 2 * reach, 1)


def unfold_patches(piece, latent_ch):
    frames, rows, cols = (piece.shape[0], piece.shape[1], piece.shape[2])
    parts = piece.reshape(frames, rows, cols, PATCH, PATCH, latent_ch)
    parts = jnp.transpose(parts, (0, 1, 3, 2, 4, 5))
    return parts.reshape(frames, rows * PATCH, cols * PATCH, latent_ch)


def convolve(current, kernels):
    return lax.conv_general_dilated(
        current,
        kernels,
        (1, 1),
        ((0, 0), (1, 1)),
        dimension_numbers=("NHWC", "HWOI", "NHWC"),
        preferred_element_type=jnp.float32,
    )


def activate(summed, first, height):
    rows = first + lax.broadcasted_iota(jnp.int32, summed.shape, 1)
    inside = (rows >= 0) & (rows < height)
    return jnp.where(inside, jax.nn.silu(summed), 0.0).astype(jnp.bfloat16)


def body(qkv, out_weight, lift_weight, conv_weight):
    rows, heads = qkv.shape[1], qkv.shape[4]
    lines, sides = lax.axis_size("blk"), lax.axis_size("uly")
    side = lax.axis_index("uly")
    latent_ch = lift_weight.shape[0]
    own = conv_weight.shape[3]
    reach = -(-LAYERS // PATCH)
    lifts = spread(lift_weight, "uly")
    folded = 0.0
    for s in range(sides):
        kernels = cut(conv_weight[0], (side ^ s) * own, own, 3)
        folded = folded + jnp.einsum(
            "abdc,ec->abde", kernels, lifts[s], preferred_element_type=jnp.float32
        )
    folded = ordered(spread(folded.astype(jnp.bfloat16), "uly"), side)
    folded = jnp.transpose(folded, (1, 2, 0, 3, 4)).reshape(3, 3, sides * own, latent_ch)
    powers = lines & (lines - 1) == 0 and sides & (sides - 1) == 0
    if powers and heads % (lines * sides) == 0:
        patches = window_by_swaps(qkv, out_weight, reach)
    else:
        patches = window_by_gathers(qkv, out_weight, reach)
    height = lines * rows * PATCH
    margin = LAYERS - 1
    start = lax.axis_index("blk") * rows * PATCH
    latent = unfold_patches(patches, latent_ch)
    spare = reach * PATCH - LAYERS
    latent = latent[:, spare : latent.shape[1] - spare]
    current = activate(convolve(latent, folded), start - margin, height)
    for layer in range(1, LAYERS):
        margin -= 1
        kernels = conv_weight[layer]
        if layer > 1:
            current = jnp.concatenate(spread(current, "uly"), axis=3)
            kernels = jnp.concatenate(
                [cut(kernels, (side ^ s) * own, own, 3) for s in range(sides)], axis=3
            )
        current = activate(convolve(current, kernels), start - margin, height)
    return current


def solution(mesh):
    in_specs = (
        P("grp", "blk", "uly", None, None, None),
        P(),
        P(None, "uly"),
        P(None, None, None, "uly", None),
    )
    out_specs = P("grp", "blk", None, "uly")
    return jax.shard_map(body, mesh=mesh, in_specs=in_specs, out_specs=out_specs, check_vma=False)
```

```python
import jax
import jax.numpy as jnp
from jax import lax
from jax.sharding import PartitionSpec as P

PATCH = 2
LAYERS = 4


def swap(pieces, axis):
    count = len(pieces)
    return [pieces[0]] + [
        lax.ppermute(pieces[step], axis, [(i, i ^ step) for i in range(count)])
        for step in range(1, count)
    ]


def spread(piece, axis):
    return swap([piece] * lax.axis_size(axis), axis)


def cut(array, start, size, axis):
    return lax.dynamic_slice_in_dim(array, start, size, axis=axis)


def attend(queries, keys, values):
    scale = 1.0 / queries.shape[-1] ** 0.5
    scores = jnp.einsum("hqd,hkd->hqk", queries, keys, preferred_element_type=jnp.float32) * scale
    weights = jnp.exp(scores - jnp.max(scores, axis=2, keepdims=True))
    totals = jnp.sum(weights, axis=2)
    mixed = jnp.einsum(
        "hqk,hkd->hqd", weights.astype(jnp.bfloat16), values, preferred_element_type=jnp.float32
    )
    return (mixed / totals[:, :, None]).astype(jnp.bfloat16)


def ordered(blocks, me):
    stacked = jnp.stack(blocks)
    return jnp.concatenate(
        [cut(stacked, me ^ place, 1, 0) for place in range(len(blocks))], axis=0
    )


def gathered(piece, side):
    blocks = ordered(spread(piece, "uly"), side)
    blocks = jnp.moveaxis(blocks, 0, -2)
    return blocks.reshape(piece.shape[:-1] + (-1,))


def window_by_swaps(qkv, out_weight, reach):
    frames, rows, cols, _, heads, size = qkv.shape
    lines, sides = lax.axis_size("blk"), lax.axis_size("uly")
    line, side = lax.axis_index("blk"), lax.axis_index("uly")
    group, share = heads // sides, heads // sides // lines
    got = swap([cut(qkv, (side ^ s) * group, group, 4) for s in range(sides)], "uly")
    grouped = jnp.stack(got, axis=3)
    grouped = jnp.transpose(grouped, (4, 5, 0, 1, 3, 2, 6))
    got = swap([cut(grouped, (line ^ t) * share, share, 1) for t in range(lines)], "blk")
    shared = ordered(got, line)
    shared = jnp.transpose(shared, (1, 2, 3, 0, 4, 5, 6, 7))
    flat = shared.reshape(3, share, -1, size)
    attended = attend(flat[0], flat[1], flat[2])
    attended = attended.reshape(share, frames, lines * rows, sides * cols, size)
    attended = jnp.transpose(attended, (1, 2, 3, 0, 4)).reshape(
        frames, lines * rows, sides * cols, share * size
    )
    padded = jnp.pad(attended, ((0, 0), (reach, reach), (0, 0), (0, 0)))
    got = swap([cut(padded, (line ^ t) * rows, rows + 2 * reach, 1) for t in range(lines)], "blk")
    partial = 0.0
    for t in range(lines):
        weight = cut(out_weight, ((side * lines) + (line ^ t)) * share * size, share * size, 0)
        partial = partial + jnp.einsum(
            "frcw,wp->frcp", got[t], weight, preferred_element_type=jnp.float32
        )
    partial = partial.astype(jnp.bfloat16)
    got = spread(partial, "uly")
    blocks = []
    for place in range(sides):
        total = 0.0
        for s in range(sides):
            at = (place ^ s) * cols
            total = total + got[s][:, :, at : at + cols].astype(jnp.float32)
        blocks.append(total.astype(jnp.bfloat16))
    patches = ordered(blocks, side)
    patches = jnp.transpose(patches, (1, 2, 0, 3, 4))
    return patches.reshape(frames, rows + 2 * reach, sides * cols, -1)


def window_by_gathers(qkv, out_weight, reach):
    frames, rows, cols, _, heads, size = qkv.shape
    grouped = lax.all_to_all(qkv, "blk", split_axis=4, concat_axis=1, tiled=True)
    flat = [
        lax.all_gather(grouped[:, :, :, which], "uly", axis=2, tiled=True) for which in (1, 2)
    ]
    flat = [grouped[:, :, :, 0]] + flat
    flat = [jnp.swapaxes(one.reshape(-1, one.shape[3], size), 0, 1) for one in flat]
    attended = jnp.swapaxes(attend(*flat), 0, 1)
    attended = attended.reshape(grouped.shape[:3] + grouped.shape[4:])
    restored = lax.all_to_all(attended, "blk", split_axis=1, concat_axis=3, tiled=True)
    patches = jnp.einsum(
        "frcw,wp->frcp",
        restored.reshape(frames, rows, cols, heads * size),
        out_weight,
        preferred_element_type=jnp.float32,
    ).astype(jnp.bfloat16)
    patches = lax.all_gather(patches, "uly", axis=2, tiled=True)
    patches = lax.all_gather(patches, "blk", axis=1, tiled=True)
    padded = jnp.pad(patches, ((0, 0), (reach, reach), (0, 0), (0, 0)))
    return cut(padded, lax.axis_index("blk") * rows, rows + 2 * reach, 1)


def unfold_patches(piece, latent_ch):
    frames, rows, cols = (piece.shape[0], piece.shape[1], piece.shape[2])
    parts = piece.reshape(frames, rows, cols, PATCH, PATCH, latent_ch)
    parts = jnp.transpose(parts, (0, 1, 3, 2, 4, 5))
    return parts.reshape(frames, rows * PATCH, cols * PATCH, latent_ch)


def convolve(current, kernels):
    return lax.conv_general_dilated(
        current,
        kernels,
        (1, 1),
        ((0, 0), (1, 1)),
        dimension_numbers=("NHWC", "HWOI", "NHWC"),
        preferred_element_type=jnp.float32,
    )


def activate(summed, first, height):
    rows = first + lax.broadcasted_iota(jnp.int32, summed.shape, 1)
    inside = (rows >= 0) & (rows < height)
    return jnp.where(inside, jax.nn.silu(summed), 0.0).astype(jnp.bfloat16)


def body(qkv, out_weight, lift_weight, conv_weight):
    rows, heads = qkv.shape[1], qkv.shape[4]
    lines, sides = lax.axis_size("blk"), lax.axis_size("uly")
    side = lax.axis_index("uly")
    latent_ch = lift_weight.shape[0]
    own = conv_weight.shape[3]
    reach = -(-LAYERS // PATCH)
    lifts = gathered(lift_weight, side)
    folded = jnp.einsum(
        "abdc,ec->abde", conv_weight[0], lifts, preferred_element_type=jnp.float32
    )
    folded = ordered(spread(folded.astype(jnp.bfloat16), "uly"), side)
    folded = jnp.transpose(folded, (1, 2, 0, 3, 4)).reshape(3, 3, sides * own, latent_ch)
    powers = lines & (lines - 1) == 0 and sides & (sides - 1) == 0
    if powers and heads % (lines * sides) == 0:
        patches = window_by_swaps(qkv, out_weight, reach)
    else:
        patches = window_by_gathers(qkv, out_weight, reach)
    height = lines * rows * PATCH
    margin = LAYERS - 1
    start = lax.axis_index("blk") * rows * PATCH
    latent = unfold_patches(patches, latent_ch)
    spare = reach * PATCH - LAYERS
    latent = latent[:, spare : latent.shape[1] - spare]
    current = activate(convolve(latent, folded), start - margin, height)
    for layer in range(1, LAYERS):
        margin -= 1
        kernels = conv_weight[layer]
        if layer > 1:
            current = gathered(current, side)
        current = activate(convolve(current, kernels), start - margin, height)
    return current


def solution(mesh):
    in_specs = (
        P("grp", "blk", "uly", None, None, None),
        P(),
        P(None, "uly"),
        P(None, None, None, "uly", None),
    )
    out_specs = P("grp", "blk", None, "uly")
    return jax.shard_map(body, mesh=mesh, in_specs=in_specs, out_specs=out_specs, check_vma=False)
```

```python
import functools

import jax
import jax.numpy as jnp
from jax import lax
from jax.experimental import pallas as pl
from jax.experimental.pallas import tpu as pltpu
from jax.sharding import PartitionSpec as P

PATCH = 2
LAYERS = 4


def swap(pieces, axis):
    count = len(pieces)
    return [pieces[0]] + [
        lax.ppermute(pieces[step], axis, [(i, i ^ step) for i in range(count)])
        for step in range(1, count)
    ]


def spread(piece, axis):
    return swap([piece] * lax.axis_size(axis), axis)


def cut(array, start, size, axis):
    return lax.dynamic_slice_in_dim(array, start, size, axis=axis)


def attend(queries, keys, values):
    scale = 1.0 / queries.shape[-1] ** 0.5
    scores = jnp.einsum("hqd,hkd->hqk", queries, keys, preferred_element_type=jnp.float32) * scale
    weights = jnp.exp(scores - jnp.max(scores, axis=2, keepdims=True))
    totals = jnp.sum(weights, axis=2)
    mixed = jnp.einsum(
        "hqk,hkd->hqd", weights.astype(jnp.bfloat16), values, preferred_element_type=jnp.float32
    )
    return (mixed / totals[:, :, None]).astype(jnp.bfloat16)


def ordered(blocks, me):
    stacked = jnp.stack(blocks)
    return jnp.concatenate(
        [cut(stacked, me ^ place, 1, 0) for place in range(len(blocks))], axis=0
    )


def gathered(piece, side):
    blocks = ordered(spread(piece, "uly"), side)
    blocks = jnp.moveaxis(blocks, 0, -2)
    return blocks.reshape(piece.shape[:-1] + (-1,))


def window_by_swaps(qkv, out_weight, reach):
    frames, rows, cols, _, heads, size = qkv.shape
    lines, sides = lax.axis_size("blk"), lax.axis_size("uly")
    line, side = lax.axis_index("blk"), lax.axis_index("uly")
    group, share = heads // sides, heads // sides // lines
    got = swap([cut(qkv, (side ^ s) * group, group, 4) for s in range(sides)], "uly")
    grouped = jnp.stack(got, axis=3)
    grouped = jnp.transpose(grouped, (4, 5, 0, 1, 3, 2, 6))
    got = swap([cut(grouped, (line ^ t) * share, share, 1) for t in range(lines)], "blk")
    shared = ordered(got, line)
    shared = jnp.transpose(shared, (1, 2, 3, 0, 4, 5, 6, 7))
    flat = shared.reshape(3, share, -1, size)
    attended = attend(flat[0], flat[1], flat[2])
    attended = attended.reshape(share, frames, lines * rows, sides * cols, size)
    attended = jnp.transpose(attended, (1, 2, 3, 0, 4)).reshape(
        frames, lines * rows, sides * cols, share * size
    )
    padded = jnp.pad(attended, ((0, 0), (reach, reach), (0, 0), (0, 0)))
    got = swap([cut(padded, (line ^ t) * rows, rows + 2 * reach, 1) for t in range(lines)], "blk")
    partial = 0.0
    for t in range(lines):
        weight = cut(out_weight, ((side * lines) + (line ^ t)) * share * size, share * size, 0)
        partial = partial + jnp.einsum(
            "frcw,wp->frcp", got[t], weight, preferred_element_type=jnp.float32
        )
    partial = partial.astype(jnp.bfloat16)
    got = spread(partial, "uly")
    blocks = []
    for place in range(sides):
        total = 0.0
        for s in range(sides):
            at = (place ^ s) * cols
            total = total + got[s][:, :, at : at + cols].astype(jnp.float32)
        blocks.append(total.astype(jnp.bfloat16))
    patches = ordered(blocks, side)
    patches = jnp.transpose(patches, (1, 2, 0, 3, 4))
    return patches.reshape(frames, rows + 2 * reach, sides * cols, -1)


def window_by_gathers(qkv, out_weight, reach):
    frames, rows, cols, _, heads, size = qkv.shape
    grouped = lax.all_to_all(qkv, "blk", split_axis=4, concat_axis=1, tiled=True)
    flat = [
        lax.all_gather(grouped[:, :, :, which], "uly", axis=2, tiled=True) for which in (1, 2)
    ]
    flat = [grouped[:, :, :, 0]] + flat
    flat = [jnp.swapaxes(one.reshape(-1, one.shape[3], size), 0, 1) for one in flat]
    attended = jnp.swapaxes(attend(*flat), 0, 1)
    attended = attended.reshape(grouped.shape[:3] + grouped.shape[4:])
    restored = lax.all_to_all(attended, "blk", split_axis=1, concat_axis=3, tiled=True)
    patches = jnp.einsum(
        "frcw,wp->frcp",
        restored.reshape(frames, rows, cols, heads * size),
        out_weight,
        preferred_element_type=jnp.float32,
    ).astype(jnp.bfloat16)
    patches = lax.all_gather(patches, "uly", axis=2, tiled=True)
    patches = lax.all_gather(patches, "blk", axis=1, tiled=True)
    padded = jnp.pad(patches, ((0, 0), (reach, reach), (0, 0), (0, 0)))
    return cut(padded, lax.axis_index("blk") * rows, rows + 2 * reach, 1)


def unfold_patches(piece, latent_ch):
    frames, rows, cols = (piece.shape[0], piece.shape[1], piece.shape[2])
    parts = piece.reshape(frames, rows, cols, PATCH, PATCH, latent_ch)
    parts = jnp.transpose(parts, (0, 1, 3, 2, 4, 5))
    return parts.reshape(frames, rows * PATCH, cols * PATCH, latent_ch)


def convolve(current, kernels):
    return lax.conv_general_dilated(
        current,
        kernels,
        (1, 1),
        ((0, 0), (1, 1)),
        dimension_numbers=("NHWC", "HWOI", "NHWC"),
        preferred_element_type=jnp.float32,
    )


def activate(summed, first, height):
    rows = first + lax.broadcasted_iota(jnp.int32, summed.shape, 1)
    inside = (rows >= 0) & (rows < height)
    return jnp.where(inside, jax.nn.silu(summed), 0.0).astype(jnp.bfloat16)


def dot(left, right):
    return jnp.dot(left, right, preferred_element_type=jnp.float32)


def dot_rows(left, right):
    return lax.dot_general(
        left, right, (((1,), (1,)), ((), ())), preferred_element_type=jnp.float32
    )


def picked(source, count):
    rows = source.shape[0]
    places = lax.broadcasted_iota(jnp.int32, (rows, count), 1)
    return jnp.where(places == source, 1.0, 0.0).astype(jnp.bfloat16)


def line_of(rows):
    return lax.broadcasted_iota(jnp.int32, (rows, 1), 0)


def bits(number):
    return number.bit_length() - 1


def call(kernel, inputs, outputs, scratch=()):
    whole = pl.BlockSpec(memory_space=pltpu.VMEM)
    return pl.pallas_call(
        kernel,
        out_shape=[jax.ShapeDtypeStruct(shape, jnp.bfloat16) for shape in outputs],
        in_specs=[whole] * len(inputs),
        out_specs=[whole] * len(outputs),
        scratch_shapes=[pltpu.VMEM(shape, jnp.bfloat16) for shape in scratch],
    )(*inputs)


def regroup_kernel(sides, lines, *refs):
    pieces, out, held = refs[:sides], refs[sides : sides + lines], refs[-1]
    tokens, _, group, size = pieces[0].shape
    flat = jnp.concatenate(
        [
            piece[:, which].astype(jnp.float32).reshape(tokens * group, size)
            for piece in pieces
            for which in range(3)
        ],
        axis=1,
    ).astype(jnp.bfloat16)
    at = line_of(group * tokens)
    source = ((at & (tokens - 1)) << bits(group)) + (at >> bits(tokens))
    held[...] = dot(picked(source, tokens * group), flat).astype(jnp.bfloat16)
    line = lax.axis_index("blk")
    span = group * tokens // lines
    for t in range(lines):
        out[t][...] = held[pl.ds(pl.multiple_of((line ^ t) * span, span), span), :]


def attention_kernel(sides, lines, share, *refs):
    pieces, out, held = refs[:lines], refs[lines : 2 * lines], refs[-1]
    tokens = pieces[0].shape[0] // share
    size = pieces[0].shape[1] // (3 * sides)
    block = sides * tokens
    scale = 1.0 / size**0.5
    line = lax.axis_index("blk")
    empty = jnp.zeros((block, held.shape[1]), jnp.bfloat16)
    held[:block] = empty
    held[held.shape[0] - block :] = empty
    wide = [piece[...].astype(jnp.float32) for piece in pieces]
    for head in range(share):
        q, k, v = [
            jnp.concatenate(
                [
                    piece[
                        head * tokens : (head + 1) * tokens,
                        (s * 3 + which) * size : (s * 3 + which + 1) * size,
                    ]
                    for piece in wide
                    for s in range(sides)
                ],
                axis=0,
            ).astype(jnp.bfloat16)
            for which in range(3)
        ]
        scores = dot_rows(q, k) * scale
        weights = jnp.exp(scores - jnp.max(scores, axis=1, keepdims=True))
        totals = jnp.sum(weights, axis=1, keepdims=True)
        mixed = (dot(weights.astype(jnp.bfloat16), v) / totals).astype(jnp.bfloat16)
        for t in range(lines):
            at = pl.multiple_of(((line ^ t) + 1) * block, block)
            held[pl.ds(at, block), head * size : (head + 1) * size] = mixed[
                t * block : (t + 1) * block
            ]
    for t in range(lines):
        at = pl.multiple_of((line ^ t) * block, block)
        out[t][...] = held[pl.ds(at, 3 * block), :]


def fold_kernel(sides, *refs):
    pieces, kernels, out, held = refs[:sides], refs[sides], refs[-2], refs[-1]
    latent, own = pieces[0].shape
    side = lax.axis_index("uly")
    for s in range(sides):
        held[:, pl.ds(pl.multiple_of((side ^ s) * own, own), own)] = pieces[s][...]
    lift = held[...]
    for tap in range(9):
        product = dot_rows(lift, kernels[tap // 3, tap % 3])
        out[tap * latent : (tap + 1) * latent, :] = product.astype(jnp.bfloat16)


def activated(summed, first, width, height):
    row = first + (line_of(summed.shape[0]) >> bits(width))
    inside = (row >= 0) & (row < height)
    return jnp.where(inside, jax.nn.silu(summed), 0.0)


def convolved(current, kernels, half):
    width = 2 * half
    own = kernels.shape[2]
    size = current.shape[0] - 2 * width
    summed = 0.0
    for above in range(3):
        taps = kernels[above].reshape(3 * own, kernels.shape[3])
        summed = summed + dot_rows(current[above * width : above * width + size], taps)
    summed = summed.reshape(size // width, 2, half, 3 * own)

    def part(parity, tap):
        return summed[:, parity, :, tap * own : (tap + 1) * own].reshape(size // 2, own)

    column = line_of(size // 2) & (half - 1)
    before = jnp.where(column == 0, 0.0, pltpu.roll(part(1, 0), 1, 0))
    after = jnp.where(column == half - 1, 0.0, pltpu.roll(part(0, 2), size // 2 - 1, 0))
    even = before + part(0, 1) + part(1, 2)
    odd = part(0, 0) + part(1, 1) + after
    both = [one.reshape(size // width, 1, half, own) for one in (even, odd)]
    return jnp.concatenate(both, axis=1).reshape(size, own)


def first_kernel(sides, rows, cols, height, *refs):
    partials, folded, kernels = refs[:sides], refs[sides : 2 * sides], refs[2 * sides]
    out, even_taps, odd_taps, held = refs[-4:]
    side, line = lax.axis_index("uly"), lax.axis_index("blk")
    half = sides * cols
    count = partials[0].shape[0]
    latent = folded[0].shape[0] // 9
    own = folded[0].shape[1]
    empty = jnp.zeros((latent, sides * own), jnp.bfloat16)
    for above in range(3):
        even_taps[above, 2 * latent : 3 * latent, :] = empty
        odd_taps[above, 3 * latent :, :] = empty
        for s in range(sides):
            lanes = pl.ds(pl.multiple_of((side ^ s) * own, own), own)
            for beside in range(3):
                at = (above * 3 + beside) * latent
                taps = folded[s][at : at + latent, :]
                to = (3, 0, 1)[beside] * latent
                even_taps[above, to : to + latent, lanes] = taps
                odd_taps[above, beside * latent : (beside + 1) * latent, lanes] = taps
    at = line_of(count)
    column = at & (cols - 1)
    group = (at >> bits(cols)) & (sides - 1)
    row = (at >> bits(half)) & (rows - 1)
    block = at >> bits(half * rows)
    total = 0.0
    for s in range(sides):
        source = (((block << bits(sides)) + (group ^ side ^ s)) << bits(rows)) + row
        source = (source << bits(cols)) + column
        total = total + dot(picked(source, count), partials[s][...])
    total = total.astype(jnp.bfloat16).astype(jnp.float32)
    wide = 2 * latent
    lines = [
        total[:, i * wide : (i + 1) * wide].reshape(count // half, 1, half, wide) for i in range(2)
    ]
    latents = jnp.concatenate(lines, axis=1).reshape(2 * count, wide)
    place = line_of(2 * count) & (half - 1)
    before = jnp.where(place == 0, 0.0, pltpu.roll(latents, 1, 0))
    after = jnp.where(place == half - 1, 0.0, pltpu.roll(latents, 2 * count - 1, 0))
    start = line * rows * PATCH - (LAYERS - 1)
    size = 2 * count - 2 * half
    for parity, (other, taps) in enumerate(((before, even_taps), (after, odd_taps))):
        current = jnp.concatenate([latents, other], axis=1).astype(jnp.bfloat16)
        summed = 0.0
        for above in range(3):
            summed = summed + dot(current[above * half : above * half + size], taps[above])
        summed = activated(summed, start, half, height).astype(jnp.bfloat16)
        held[:, parity] = summed.reshape(size // half, half, sides * own)
    current = held[...].reshape(2 * size, sides * own)
    summed = convolved(current, kernels, half)
    out[...] = activated(summed, start + 1, 2 * half, height).astype(jnp.bfloat16)


def layer_kernel(sides, half, first, step, height, last, *refs):
    pieces, kernels, out, held = refs[:sides], refs[sides], refs[-2], refs[-1]
    side, line = lax.axis_index("uly"), lax.axis_index("blk")
    own = pieces[0].shape[1]
    for s in range(sides):
        held[:, pl.ds(pl.multiple_of((side ^ s) * own, own), own)] = pieces[s][...]
    summed = convolved(held[...], kernels, half)
    width = 2 * half
    result = activated(summed, line * step + first, width, height).astype(jnp.bfloat16)
    if last:
        at = line_of(result.shape[0])
        column = at & (width - 1)
        source = (at - column) + ((column & 1) << bits(half)) + (column >> 1)
        result = dot(picked(source, result.shape[0]), result).astype(jnp.bfloat16)
    out[...] = result


def fits_kernels(qkv, lift_weight, conv_weight):
    frames, rows, cols, _, heads, size = qkv.shape
    lines, sides = lax.axis_size("blk"), lax.axis_size("uly")
    powers = all(n & (n - 1) == 0 for n in (lines, sides, rows, cols, heads))
    return (
        powers
        and frames == 1
        and rows * PATCH == LAYERS
        and heads % (lines * sides) == 0
        and rows * cols % 8 == 0
        and rows * cols * heads // (lines * sides) % 16 == 0
        and sides * cols % 16 == 0
        and heads // sides % 8 == 0
        and size % 128 == 0
        and conv_weight.shape[3] % 128 == 0
        and lift_weight.shape[0] * 2 % 128 == 0
    )


def body_by_kernels(qkv, out_weight, lift_weight, conv_weight):
    _, rows, cols, _, heads, size = qkv.shape
    lines, sides = lax.axis_size("blk"), lax.axis_size("uly")
    line, side = lax.axis_index("blk"), lax.axis_index("uly")
    group, share = heads // sides, heads // sides // lines
    latent, own = lift_weight.shape
    tokens, half = rows * cols, sides * cols
    height = lines * rows * PATCH
    width, all_ch = 2 * half, sides * own
    flat = qkv.reshape(tokens, 3, heads, size)
    got = swap([cut(flat, (side ^ s) * group, group, 2) for s in range(sides)], "uly")
    lifts = spread(lift_weight, "uly")
    span = (share * tokens, sides * 3 * size)
    shared = call(
        functools.partial(regroup_kernel, sides, lines),
        got,
        [span] * lines,
        [(group * tokens, span[1])],
    )
    got = swap(shared, "blk")
    (folded,) = call(
        functools.partial(fold_kernel, sides),
        [*lifts, conv_weight[0]],
        [(9 * latent, own)],
        [(latent, all_ch)],
    )
    folded = spread(folded, "uly")
    block = sides * tokens
    windows = call(
        functools.partial(attention_kernel, sides, lines, share),
        got,
        [(3 * block, share * size)] * lines,
        [((lines + 2) * block, share * size)],
    )
    got = swap(windows, "blk")
    partial = 0.0
    for t in range(lines):
        weight = cut(out_weight, ((side * lines) + (line ^ t)) * share * size, share * size, 0)
        partial = partial + dot(got[t], weight)
    got = spread(partial.astype(jnp.bfloat16), "uly")
    count = (rows + 2) * PATCH
    (current,) = call(
        functools.partial(first_kernel, sides, rows, cols, height),
        [*got, *folded, conv_weight[1]],
        [(count * width, own)],
        [(3, 4 * latent, all_ch)] * 2 + [(count + 2, 2, half, all_ch)],
    )
    for layer in range(2, LAYERS):
        got = spread(current, "uly")
        last = layer == LAYERS - 1
        kernel = functools.partial(
            layer_kernel, sides, half, layer + 1 - LAYERS, rows * PATCH, height, last
        )
        held = (count * width, all_ch)
        count -= 2
        (current,) = call(kernel, [*got, conv_weight[layer]], [(count * width, own)], [held])
    return current.reshape(1, count, width, own)


def body(qkv, out_weight, lift_weight, conv_weight):
    if fits_kernels(qkv, lift_weight, conv_weight):
        return body_by_kernels(qkv, out_weight, lift_weight, conv_weight)
    rows, heads = qkv.shape[1], qkv.shape[4]
    lines, sides = lax.axis_size("blk"), lax.axis_size("uly")
    side = lax.axis_index("uly")
    latent_ch = lift_weight.shape[0]
    own = conv_weight.shape[3]
    reach = -(-LAYERS // PATCH)
    lifts = gathered(lift_weight, side)
    folded = jnp.einsum(
        "abdc,ec->abde", conv_weight[0], lifts, preferred_element_type=jnp.float32
    )
    folded = ordered(spread(folded.astype(jnp.bfloat16), "uly"), side)
    folded = jnp.transpose(folded, (1, 2, 0, 3, 4)).reshape(3, 3, sides * own, latent_ch)
    powers = lines & (lines - 1) == 0 and sides & (sides - 1) == 0
    if powers and heads % (lines * sides) == 0:
        patches = window_by_swaps(qkv, out_weight, reach)
    else:
        patches = window_by_gathers(qkv, out_weight, reach)
    height = lines * rows * PATCH
    margin = LAYERS - 1
    start = lax.axis_index("blk") * rows * PATCH
    latent = unfold_patches(patches, latent_ch)
    spare = reach * PATCH - LAYERS
    latent = latent[:, spare : latent.shape[1] - spare]
    current = activate(convolve(latent, folded), start - margin, height)
    for layer in range(1, LAYERS):
        margin -= 1
        kernels = conv_weight[layer]
        if layer > 1:
            current = gathered(current, side)
        current = activate(convolve(current, kernels), start - margin, height)
    return current


def solution(mesh):
    in_specs = (
        P("grp", "blk", "uly", None, None, None),
        P(),
        P(None, "uly"),
        P(None, None, None, "uly", None),
    )
    out_specs = P("grp", "blk", None, "uly")
    return jax.shard_map(body, mesh=mesh, in_specs=in_specs, out_specs=out_specs, check_vma=False)
```

```python
import functools
import math

import jax
import jax.numpy as jnp
from jax import lax
from jax.experimental import pallas as pl
from jax.experimental.pallas import tpu as pltpu
from jax.sharding import PartitionSpec as P


PATCH = 2
LAYERS = 4
GRANT = 8 * 2**20


def swap(pieces, axis):
    count = len(pieces)
    got = [pieces[0]]
    for step in range(1, count):
        got.append(lax.ppermute(pieces[step], axis, [(i, i ^ step) for i in range(count)]))
    return got


def spread(piece, axis):
    return swap([piece] * lax.axis_size(axis), axis)


def cut(array, start, size, axis):
    return lax.dynamic_slice_in_dim(array, start, size, axis=axis)


def attend(queries, keys, values):
    scale = 1.0 / queries.shape[-1] ** 0.5
    scores = jnp.einsum("hqd,hkd->hqk", queries, keys, preferred_element_type=jnp.float32) * scale
    weights = jnp.exp(scores - jnp.max(scores, axis=2, keepdims=True))
    totals = jnp.sum(weights, axis=2)
    mixed = jnp.einsum(
        "hqk,hkd->hqd", weights.astype(jnp.bfloat16), values, preferred_element_type=jnp.float32
    )
    return (mixed / totals[:, :, None]).astype(jnp.bfloat16)


def ordered(blocks, me):
    stacked = jnp.stack(blocks)
    return jnp.concatenate(
        [cut(stacked, me ^ place, 1, 0) for place in range(len(blocks))], axis=0
    )


def gathered(piece, side):
    blocks = ordered(spread(piece, "uly"), side)
    blocks = jnp.moveaxis(blocks, 0, -2)
    return blocks.reshape(piece.shape[:-1] + (-1,))


def window_by_swaps(qkv, out_weight, reach):
    frames, rows, cols, _, heads, size = qkv.shape
    lines, sides = lax.axis_size("blk"), lax.axis_size("uly")
    line, side = lax.axis_index("blk"), lax.axis_index("uly")
    group, share = heads // sides, heads // sides // lines
    got = swap([cut(qkv, (side ^ s) * group, group, 4) for s in range(sides)], "uly")
    grouped = jnp.stack(got, axis=3)
    grouped = jnp.transpose(grouped, (4, 5, 0, 1, 3, 2, 6))
    got = swap([cut(grouped, (line ^ t) * share, share, 1) for t in range(lines)], "blk")
    shared = ordered(got, line)
    shared = jnp.transpose(shared, (1, 2, 3, 0, 4, 5, 6, 7))
    flat = shared.reshape(3, share, -1, size)
    attended = attend(flat[0], flat[1], flat[2])
    attended = attended.reshape(share, frames, lines * rows, sides * cols, size)
    attended = jnp.transpose(attended, (1, 2, 3, 0, 4)).reshape(
        frames, lines * rows, sides * cols, share * size
    )
    padded = jnp.pad(attended, ((0, 0), (reach, reach), (0, 0), (0, 0)))
    got = swap([cut(padded, (line ^ t) * rows, rows + 2 * reach, 1) for t in range(lines)], "blk")
    partial = 0.0
    for t in range(lines):
        weight = cut(out_weight, ((side * lines) + (line ^ t)) * share * size, share * size, 0)
        partial = partial + jnp.einsum(
            "frcw,wp->frcp", got[t], weight, preferred_element_type=jnp.float32
        )
    partial = partial.astype(jnp.bfloat16)
    got = spread(partial, "uly")
    blocks = []
    for place in range(sides):
        total = 0.0
        for s in range(sides):
            at = (place ^ s) * cols
            total = total + got[s][:, :, at : at + cols].astype(jnp.float32)
        blocks.append(total.astype(jnp.bfloat16))
    patches = ordered(blocks, side)
    patches = jnp.transpose(patches, (1, 2, 0, 3, 4))
    return patches.reshape(frames, rows + 2 * reach, sides * cols, -1)


def window_by_gathers(qkv, out_weight, reach):
    frames, rows, cols, _, heads, size = qkv.shape
    grouped = lax.all_to_all(qkv, "blk", split_axis=4, concat_axis=1, tiled=True)
    flat = [
        lax.all_gather(grouped[:, :, :, which], "uly", axis=2, tiled=True) for which in (1, 2)
    ]
    flat = [grouped[:, :, :, 0]] + flat
    flat = [jnp.swapaxes(one.reshape(-1, one.shape[3], size), 0, 1) for one in flat]
    attended = jnp.swapaxes(attend(*flat), 0, 1)
    attended = attended.reshape(grouped.shape[:3] + grouped.shape[4:])
    restored = lax.all_to_all(attended, "blk", split_axis=1, concat_axis=3, tiled=True)
    patches = jnp.einsum(
        "frcw,wp->frcp",
        restored.reshape(frames, rows, cols, heads * size),
        out_weight,
        preferred_element_type=jnp.float32,
    ).astype(jnp.bfloat16)
    patches = lax.all_gather(patches, "uly", axis=2, tiled=True)
    patches = lax.all_gather(patches, "blk", axis=1, tiled=True)
    padded = jnp.pad(patches, ((0, 0), (reach, reach), (0, 0), (0, 0)))
    return cut(padded, lax.axis_index("blk") * rows, rows + 2 * reach, 1)


def unfold_patches(piece, latent_ch):
    frames, rows, cols = (piece.shape[0], piece.shape[1], piece.shape[2])
    parts = piece.reshape(frames, rows, cols, PATCH, PATCH, latent_ch)
    parts = jnp.transpose(parts, (0, 1, 3, 2, 4, 5))
    return parts.reshape(frames, rows * PATCH, cols * PATCH, latent_ch)


def convolve(current, kernels):
    return lax.conv_general_dilated(
        current,
        kernels,
        (1, 1),
        ((0, 0), (1, 1)),
        dimension_numbers=("NHWC", "HWOI", "NHWC"),
        preferred_element_type=jnp.float32,
    )


def activate(summed, first, height):
    rows = first + lax.broadcasted_iota(jnp.int32, summed.shape, 1)
    inside = (rows >= 0) & (rows < height)
    return jnp.where(inside, jax.nn.silu(summed), 0.0).astype(jnp.bfloat16)


def dot(left, right):
    return jnp.dot(left, right, preferred_element_type=jnp.float32)


def dot_rows(left, right):
    return lax.dot_general(
        left, right, (((1,), (1,)), ((), ())), preferred_element_type=jnp.float32
    )


def picked(source, count):
    rows = source.shape[0]
    places = lax.broadcasted_iota(jnp.int32, (rows, count), 1)
    return jnp.where(places == source, 1.0, 0.0).astype(jnp.bfloat16)


def line_of(rows):
    return lax.broadcasted_iota(jnp.int32, (rows, 1), 0)


def bits(number):
    return number.bit_length() - 1


def call(kernel, flops, inputs, outputs, scratch=(), far=()):
    near = pl.BlockSpec(memory_space=pltpu.VMEM)
    kept = pl.BlockSpec(memory_space=pltpu.HBM)
    moved = sum(one.size for one in inputs) + sum(math.prod(shape) for shape in outputs)
    return pl.pallas_call(
        kernel,
        out_shape=[jax.ShapeDtypeStruct(shape, jnp.bfloat16) for shape in outputs],
        in_specs=[kept if place in far else near for place in range(len(inputs))],
        out_specs=[near] * len(outputs),
        scratch_shapes=[
            pltpu.VMEM(one, jnp.bfloat16) if isinstance(one, tuple) else one for one in scratch
        ],
        compiler_params=pltpu.CompilerParams(vmem_limit_bytes=GRANT),
        cost_estimate=pl.CostEstimate(
            flops=flops, transcendentals=0, bytes_accessed=2 * moved
        ),
    )(*[
        pltpu.with_memory_space_constraint(one, pltpu.HBM) if place in far else one
        for place, one in enumerate(inputs)
    ])


def pack_kernel(sides, flat, lift, *refs):
    out, sems = refs[:sides], refs[sides]
    group, count = out[0].shape[1], flat.shape[0]
    side = lax.axis_index("uly")
    copies = []
    for s in reversed(range(sides)):
        heads = pl.ds(pl.multiple_of((side ^ s) * group, group), group)
        for place, source, target in (
            (s, flat.at[:, heads], out[s].at[pl.ds(0, count)]),
            (sides + s, lift, out[s].at[pl.ds(count, lift.shape[0])]),
        ):
            copies.append(pltpu.make_async_copy(source, target, sems.at[place]))
    for copy in copies:
        copy.start()
    for copy in copies:
        copy.wait()


def load_kernel(kernels, *refs):
    out, sems = refs[:-1], refs[-1]
    copies = [
        pltpu.make_async_copy(kernels.at[layer], out[layer], sems.at[layer])
        for layer in range(len(out))
    ]
    for copy in copies:
        copy.start()
    for copy in copies:
        copy.wait()


def regroup_kernel(sides, lines, tokens, *refs):
    pieces, out, held = refs[:sides], refs[sides : sides + lines], refs[-1]
    _, group, size = pieces[0].shape
    flat = jnp.concatenate(
        [
            piece[: 3 * tokens]
            .reshape(tokens, 3, group, size)[:, which]
            .astype(jnp.float32)
            .reshape(tokens * group, size)
            for piece in pieces
            for which in range(3)
        ],
        axis=1,
    ).astype(jnp.bfloat16)
    at = line_of(group * tokens)
    source = ((at & (tokens - 1)) << bits(group)) + (at >> bits(tokens))
    held[...] = dot(picked(source, tokens * group), flat).astype(jnp.bfloat16)
    line = lax.axis_index("blk")
    span = group * tokens // lines
    for t in range(lines):
        out[t][...] = held[pl.ds(pl.multiple_of((line ^ t) * span, span), span), :]


def attention_kernel(sides, lines, share, *refs):
    pieces, out, held = refs[:lines], refs[lines : 2 * lines], refs[-1]
    tokens = pieces[0].shape[0] // share
    size = pieces[0].shape[1] // (3 * sides)
    block = sides * tokens
    scale = 1.0 / size**0.5
    line = lax.axis_index("blk")
    empty = jnp.zeros((block, held.shape[1]), jnp.bfloat16)
    held[:block] = empty
    held[held.shape[0] - block :] = empty
    wide = [piece[...].astype(jnp.float32) for piece in pieces]
    for head in range(share):
        q, k, v = [
            jnp.concatenate(
                [
                    piece[
                        head * tokens : (head + 1) * tokens,
                        (s * 3 + which) * size : (s * 3 + which + 1) * size,
                    ]
                    for piece in wide
                    for s in range(sides)
                ],
                axis=0,
            ).astype(jnp.bfloat16)
            for which in range(3)
        ]
        scores = dot_rows(q, k) * scale
        weights = jnp.exp(scores - jnp.max(scores, axis=1, keepdims=True))
        totals = jnp.sum(weights, axis=1, keepdims=True)
        mixed = (dot(weights.astype(jnp.bfloat16), v) / totals).astype(jnp.bfloat16)
        for t in range(lines):
            at = pl.multiple_of(((line ^ t) + 1) * block, block)
            held[pl.ds(at, block), head * size : (head + 1) * size] = mixed[
                t * block : (t + 1) * block
            ]
    for t in range(lines):
        at = pl.multiple_of((line ^ t) * block, block)
        out[t][...] = held[pl.ds(at, 3 * block), :]


def project_kernel(lines, *refs):
    pieces, weights, out = refs[:lines], refs[lines], refs[-1]
    line, side = lax.axis_index("blk"), lax.axis_index("uly")
    depth = pieces[0].shape[1]
    summed = 0.0
    for t in range(lines):
        at = pl.multiple_of((side * lines + (line ^ t)) * depth, depth)
        summed = summed + dot(pieces[t][...], weights[pl.ds(at, depth), :])
    out[...] = summed.astype(jnp.bfloat16)


def fold_kernel(sides, skip, *refs):
    pieces, kernels, out, held = refs[:sides], refs[sides], refs[-2], refs[-1]
    latent, own = out.shape[0] // 9, out.shape[1]
    side = lax.axis_index("uly")
    for s in range(sides):
        lift = pieces[s][skip:].astype(jnp.float32).reshape(latent, own).astype(jnp.bfloat16)
        held[:, pl.ds(pl.multiple_of((side ^ s) * own, own), own)] = lift
    lift = held[...]
    for tap in range(9):
        product = dot_rows(lift, kernels[tap // 3, tap % 3])
        out[tap * latent : (tap + 1) * latent, :] = product.astype(jnp.bfloat16)


def activated(summed, first, width, height):
    row = first + (line_of(summed.shape[0]) >> bits(width))
    inside = (row >= 0) & (row < height)
    return jnp.where(inside, jax.nn.silu(summed), 0.0)


def convolved(current, kernels, half):
    width = 2 * half
    own = kernels.shape[2]
    size = current.shape[0] - 2 * width
    summed = 0.0
    for above in range(3):
        taps = kernels[above].reshape(3 * own, kernels.shape[3])
        summed = summed + dot_rows(current[above * width : above * width + size], taps)
    summed = summed.reshape(size // width, 2, half, 3 * own)

    def part(parity, tap):
        return summed[:, parity, :, tap * own : (tap + 1) * own].reshape(size // 2, own)

    column = line_of(size // 2) & (half - 1)
    before = jnp.where(column == 0, 0.0, pltpu.roll(part(1, 0), 1, 0))
    after = jnp.where(column == half - 1, 0.0, pltpu.roll(part(0, 2), size // 2 - 1, 0))
    even = before + part(0, 1) + part(1, 2)
    odd = part(0, 0) + part(1, 1) + after
    both = [one.reshape(size // width, 1, half, own) for one in (even, odd)]
    return jnp.concatenate(both, axis=1).reshape(size, own)


def first_kernel(sides, rows, cols, height, *refs):
    partials, folded, kernels = refs[:sides], refs[sides : 2 * sides], refs[2 * sides]
    out, even_taps, odd_taps, held = refs[-4:]
    side, line = lax.axis_index("uly"), lax.axis_index("blk")
    half = sides * cols
    count = partials[0].shape[0]
    latent = folded[0].shape[0] // 9
    own = folded[0].shape[1]
    empty = jnp.zeros((latent, sides * own), jnp.bfloat16)
    for above in range(3):
        even_taps[above, 2 * latent : 3 * latent, :] = empty
        odd_taps[above, 3 * latent :, :] = empty
        for s in range(sides):
            lanes = pl.ds(pl.multiple_of((side ^ s) * own, own), own)
            for beside in range(3):
                at = (above * 3 + beside) * latent
                taps = folded[s][at : at + latent, :]
                to = (3, 0, 1)[beside] * latent
                even_taps[above, to : to + latent, lanes] = taps
                odd_taps[above, beside * latent : (beside + 1) * latent, lanes] = taps
    at = line_of(count)
    column = at & (cols - 1)
    group = (at >> bits(cols)) & (sides - 1)
    row = (at >> bits(half)) & (rows - 1)
    block = at >> bits(half * rows)
    total = 0.0
    for s in range(sides):
        source = (((block << bits(sides)) + (group ^ side ^ s)) << bits(rows)) + row
        source = (source << bits(cols)) + column
        total = total + dot(picked(source, count), partials[s][...])
    total = total.astype(jnp.bfloat16).astype(jnp.float32)
    wide = 2 * latent
    lines = [
        total[:, i * wide : (i + 1) * wide].reshape(count // half, 1, half, wide) for i in range(2)
    ]
    latents = jnp.concatenate(lines, axis=1).reshape(2 * count, wide)
    place = line_of(2 * count) & (half - 1)
    before = jnp.where(place == 0, 0.0, pltpu.roll(latents, 1, 0))
    after = jnp.where(place == half - 1, 0.0, pltpu.roll(latents, 2 * count - 1, 0))
    start = line * rows * PATCH - (LAYERS - 1)
    size = 2 * count - 2 * half
    for parity, (other, taps) in enumerate(((before, even_taps), (after, odd_taps))):
        current = jnp.concatenate([latents, other], axis=1).astype(jnp.bfloat16)
        summed = 0.0
        for above in range(3):
            summed = summed + dot(current[above * half : above * half + size], taps[above])
        summed = activated(summed, start, half, height).astype(jnp.bfloat16)
        held[:, parity] = summed.reshape(size // half, half, sides * own)
    current = held[...].reshape(2 * size, sides * own)
    summed = convolved(current, kernels, half)
    out[...] = activated(summed, start + 1, 2 * half, height).astype(jnp.bfloat16)


def layer_kernel(layer, sides, half, step, height, *refs):
    pieces, kernels, out, held = refs[:sides], refs[sides], refs[-2], refs[-1]
    side, line = lax.axis_index("uly"), lax.axis_index("blk")
    own = pieces[0].shape[1]
    for s in range(sides):
        held[:, pl.ds(pl.multiple_of((side ^ s) * own, own), own)] = pieces[s][...]
    summed = convolved(held[...], kernels, half)
    width = 2 * half
    first = line * step + layer + 1 - LAYERS
    result = activated(summed, first, width, height).astype(jnp.bfloat16)
    if layer == LAYERS - 1:
        at = line_of(result.shape[0])
        column = at & (width - 1)
        source = (at - column) + ((column & 1) << bits(half)) + (column >> 1)
        result = dot(picked(source, result.shape[0]), result).astype(jnp.bfloat16)
    out[...] = result


def fits_kernels(qkv, lift_weight, conv_weight):
    frames, rows, cols, _, heads, size = qkv.shape
    lines, sides = lax.axis_size("blk"), lax.axis_size("uly")
    powers = all(n & (n - 1) == 0 for n in (lines, sides, rows, cols, heads))
    return (
        powers
        and frames == 1
        and rows * PATCH == LAYERS
        and heads % (lines * sides) == 0
        and rows * cols % 8 == 0
        and rows * cols * heads // (lines * sides) % 16 == 0
        and sides * cols % 16 == 0
        and heads // sides % 8 == 0
        and size % 128 == 0
        and conv_weight.shape[3] % 128 == 0
        and lift_weight.size % (heads // sides * size) == 0
        and conv_weight.shape[3] == size
        and lift_weight.shape[0] * 2 % 128 == 0
    )


def body_by_kernels(qkv, out_weight, lift_weight, conv_weight):
    _, rows, cols, _, heads, size = qkv.shape
    lines, sides = lax.axis_size("blk"), lax.axis_size("uly")
    group, share = heads // sides, heads // sides // lines
    latent, own = lift_weight.shape
    tokens, half = rows * cols, sides * cols
    height = lines * rows * PATCH
    width, all_ch = 2 * half, sides * own
    pieces = call(
        functools.partial(pack_kernel, sides),
        0,
        [qkv.reshape(3 * tokens, heads, size), lift_weight.reshape(-1, group, size)],
        [(3 * tokens + lift_weight.size // (group * size), group, size)] * sides,
        [pltpu.SemaphoreType.DMA((2 * sides,))],
        far=(0, 1),
    )
    got = swap(pieces, "uly")
    kernels = call(
        load_kernel,
        10**8,
        [conv_weight],
        [conv_weight.shape[1:]] * LAYERS,
        [pltpu.SemaphoreType.DMA((LAYERS,))],
        far=(0,),
    )
    span = (share * tokens, sides * 3 * size)
    shared = call(
        functools.partial(regroup_kernel, sides, lines, tokens),
        2 * (group * tokens) ** 2 * span[1],
        got,
        [span] * lines,
        [(group * tokens, span[1])],
    )
    (folded,) = call(
        functools.partial(fold_kernel, sides, 3 * tokens),
        2 * 9 * latent * all_ch * own,
        [*got, kernels[0]],
        [(9 * latent, own)],
        [(latent, all_ch)],
    )
    got = swap(shared, "blk")
    folded = spread(folded, "uly")
    block = sides * tokens
    windows = call(
        functools.partial(attention_kernel, sides, lines, share),
        4 * share * size * (lines * block) ** 2,
        got,
        [(3 * block, share * size)] * lines,
        [((lines + 2) * block, share * size)],
    )
    got = swap(windows, "blk")
    (partial,) = call(
        functools.partial(project_kernel, lines),
        2 * 3 * block * lines * share * size * out_weight.shape[1],
        [*got, out_weight],
        [(3 * block, out_weight.shape[1])],
    )
    got = spread(partial, "uly")
    count = (rows + 2) * PATCH
    (current,) = call(
        functools.partial(first_kernel, sides, rows, cols, height),
        18 * count * width * all_ch * own,
        [*got, *folded, kernels[1]],
        [(count * width, own)],
        [(3, 4 * latent, all_ch)] * 2 + [(count + 2, 2, half, all_ch)],
    )
    for layer in range(2, LAYERS):
        got = spread(current, "uly")
        kernel = functools.partial(layer_kernel, layer, sides, half, rows * PATCH, height)
        held = (count * width, all_ch)
        count -= 2
        (current,) = call(
            kernel,
            18 * count * width * all_ch * own,
            [*got, kernels[layer]],
            [(count * width, own)],
            [held],
        )
    return current.reshape(1, count, width, own)


def body(qkv, out_weight, lift_weight, conv_weight):
    if fits_kernels(qkv, lift_weight, conv_weight):
        return body_by_kernels(qkv, out_weight, lift_weight, conv_weight)
    rows, heads = qkv.shape[1], qkv.shape[4]
    lines, sides = lax.axis_size("blk"), lax.axis_size("uly")
    side = lax.axis_index("uly")
    latent_ch = lift_weight.shape[0]
    own = conv_weight.shape[3]
    reach = -(-LAYERS // PATCH)
    lifts = gathered(lift_weight, side)
    folded = jnp.einsum(
        "abdc,ec->abde", conv_weight[0], lifts, preferred_element_type=jnp.float32
    )
    folded = ordered(spread(folded.astype(jnp.bfloat16), "uly"), side)
    folded = jnp.transpose(folded, (1, 2, 0, 3, 4)).reshape(3, 3, sides * own, latent_ch)
    powers = lines & (lines - 1) == 0 and sides & (sides - 1) == 0
    if powers and heads % (lines * sides) == 0:
        patches = window_by_swaps(qkv, out_weight, reach)
    else:
        patches = window_by_gathers(qkv, out_weight, reach)
    height = lines * rows * PATCH
    margin = LAYERS - 1
    start = lax.axis_index("blk") * rows * PATCH
    latent = unfold_patches(patches, latent_ch)
    spare = reach * PATCH - LAYERS
    latent = latent[:, spare : latent.shape[1] - spare]
    current = activate(convolve(latent, folded), start - margin, height)
    for layer in range(1, LAYERS):
        margin -= 1
        kernels = conv_weight[layer]
        if layer > 1:
            current = gathered(current, side)
        current = activate(convolve(current, kernels), start - margin, height)
    return current


def solution(mesh):
    in_specs = (
        P("grp", "blk", "uly", None, None, None),
        P(),
        P(None, "uly"),
        P(None, None, None, "uly", None),
    )
    out_specs = P("grp", "blk", None, "uly")
    return jax.shard_map(
        body, mesh=mesh, in_specs=in_specs, out_specs=out_specs, check_vma=False
    )
```

```python
import functools
import math

import jax
import jax.numpy as jnp
from jax import lax
from jax.experimental import pallas as pl
from jax.experimental.pallas import tpu as pltpu
from jax.sharding import PartitionSpec as P


PATCH = 2
LAYERS = 4
GRANT = 8 * 2**20
SHARED = (1, 2)


def swap(pieces, axis):
    count = lax.axis_size(axis)
    got = [pieces[0]]
    for step in range(1, len(pieces)):
        got.append(lax.ppermute(pieces[step], axis, [(i, i ^ step) for i in range(count)]))
    return got


def spread(piece, axis):
    return swap([piece] * lax.axis_size(axis), axis)


def cut(array, start, size, axis):
    return lax.dynamic_slice_in_dim(array, start, size, axis=axis)


def attend(queries, keys, values):
    scale = 1.0 / queries.shape[-1] ** 0.5
    scores = jnp.einsum("hqd,hkd->hqk", queries, keys, preferred_element_type=jnp.float32) * scale
    weights = jnp.exp(scores - jnp.max(scores, axis=2, keepdims=True))
    totals = jnp.sum(weights, axis=2)
    mixed = jnp.einsum(
        "hqk,hkd->hqd", weights.astype(jnp.bfloat16), values, preferred_element_type=jnp.float32
    )
    return (mixed / totals[:, :, None]).astype(jnp.bfloat16)


def ordered(blocks, me):
    stacked = jnp.stack(blocks)
    return jnp.concatenate(
        [cut(stacked, me ^ place, 1, 0) for place in range(len(blocks))], axis=0
    )


def gathered(piece, side):
    blocks = ordered(spread(piece, "uly"), side)
    blocks = jnp.moveaxis(blocks, 0, -2)
    return blocks.reshape(piece.shape[:-1] + (-1,))


def window_by_swaps(qkv, out_weight, reach):
    frames, rows, cols, _, heads, size = qkv.shape
    lines, sides = lax.axis_size("blk"), lax.axis_size("uly")
    line, side = lax.axis_index("blk"), lax.axis_index("uly")
    group, share = heads // sides, heads // sides // lines
    got = swap([cut(qkv, (side ^ s) * group, group, 4) for s in range(sides)], "uly")
    grouped = jnp.stack(got, axis=3)
    grouped = jnp.transpose(grouped, (4, 5, 0, 1, 3, 2, 6))
    got = swap([cut(grouped, (line ^ t) * share, share, 1) for t in range(lines)], "blk")
    shared = ordered(got, line)
    shared = jnp.transpose(shared, (1, 2, 3, 0, 4, 5, 6, 7))
    flat = shared.reshape(3, share, -1, size)
    attended = attend(flat[0], flat[1], flat[2])
    attended = attended.reshape(share, frames, lines * rows, sides * cols, size)
    attended = jnp.transpose(attended, (1, 2, 3, 0, 4)).reshape(
        frames, lines * rows, sides * cols, share * size
    )
    padded = jnp.pad(attended, ((0, 0), (reach, reach), (0, 0), (0, 0)))
    got = swap([cut(padded, (line ^ t) * rows, rows + 2 * reach, 1) for t in range(lines)], "blk")
    partial = 0.0
    for t in range(lines):
        weight = cut(out_weight, ((side * lines) + (line ^ t)) * share * size, share * size, 0)
        partial = partial + jnp.einsum(
            "frcw,wp->frcp", got[t], weight, preferred_element_type=jnp.float32
        )
    partial = partial.astype(jnp.bfloat16)
    got = spread(partial, "uly")
    blocks = []
    for place in range(sides):
        total = 0.0
        for s in range(sides):
            at = (place ^ s) * cols
            total = total + got[s][:, :, at : at + cols].astype(jnp.float32)
        blocks.append(total.astype(jnp.bfloat16))
    patches = ordered(blocks, side)
    patches = jnp.transpose(patches, (1, 2, 0, 3, 4))
    return patches.reshape(frames, rows + 2 * reach, sides * cols, -1)


def window_by_gathers(qkv, out_weight, reach):
    frames, rows, cols, _, heads, size = qkv.shape
    grouped = lax.all_to_all(qkv, "blk", split_axis=4, concat_axis=1, tiled=True)
    flat = [
        lax.all_gather(grouped[:, :, :, which], "uly", axis=2, tiled=True) for which in (1, 2)
    ]
    flat = [grouped[:, :, :, 0]] + flat
    flat = [jnp.swapaxes(one.reshape(-1, one.shape[3], size), 0, 1) for one in flat]
    attended = jnp.swapaxes(attend(*flat), 0, 1)
    attended = attended.reshape(grouped.shape[:3] + grouped.shape[4:])
    restored = lax.all_to_all(attended, "blk", split_axis=1, concat_axis=3, tiled=True)
    patches = jnp.einsum(
        "frcw,wp->frcp",
        restored.reshape(frames, rows, cols, heads * size),
        out_weight,
        preferred_element_type=jnp.float32,
    ).astype(jnp.bfloat16)
    patches = lax.all_gather(patches, "uly", axis=2, tiled=True)
    patches = lax.all_gather(patches, "blk", axis=1, tiled=True)
    padded = jnp.pad(patches, ((0, 0), (reach, reach), (0, 0), (0, 0)))
    return cut(padded, lax.axis_index("blk") * rows, rows + 2 * reach, 1)


def unfold_patches(piece, latent_ch):
    frames, rows, cols = (piece.shape[0], piece.shape[1], piece.shape[2])
    parts = piece.reshape(frames, rows, cols, PATCH, PATCH, latent_ch)
    parts = jnp.transpose(parts, (0, 1, 3, 2, 4, 5))
    return parts.reshape(frames, rows * PATCH, cols * PATCH, latent_ch)


def convolve(current, kernels):
    return lax.conv_general_dilated(
        current,
        kernels,
        (1, 1),
        ((0, 0), (1, 1)),
        dimension_numbers=("NHWC", "HWOI", "NHWC"),
        preferred_element_type=jnp.float32,
    )


def activate(summed, first, height):
    rows = first + lax.broadcasted_iota(jnp.int32, summed.shape, 1)
    inside = (rows >= 0) & (rows < height)
    return jnp.where(inside, jax.nn.silu(summed), 0.0).astype(jnp.bfloat16)


def dot(left, right):
    return jnp.dot(left, right, preferred_element_type=jnp.float32)


def dot_rows(left, right):
    return lax.dot_general(
        left, right, (((1,), (1,)), ((), ())), preferred_element_type=jnp.float32
    )


def picked(source, count):
    rows = source.shape[0]
    places = lax.broadcasted_iota(jnp.int32, (rows, count), 1)
    return jnp.where(places == source, 1.0, 0.0).astype(jnp.bfloat16)


def line_of(rows):
    return lax.broadcasted_iota(jnp.int32, (rows, 1), 0)


def bits(number):
    return number.bit_length() - 1


def call(kernel, flops, inputs, outputs, scratch=(), far=()):
    near = pl.BlockSpec(memory_space=pltpu.VMEM)
    kept = pl.BlockSpec(memory_space=pltpu.HBM)
    moved = sum(one.size for one in inputs) + sum(math.prod(shape) for shape in outputs)
    return pl.pallas_call(
        kernel,
        out_shape=[jax.ShapeDtypeStruct(shape, jnp.bfloat16) for shape in outputs],
        in_specs=[kept if place in far else near for place in range(len(inputs))],
        out_specs=[near] * len(outputs),
        scratch_shapes=[
            pltpu.VMEM(one, jnp.bfloat16) if isinstance(one, tuple) else one for one in scratch
        ],
        compiler_params=pltpu.CompilerParams(vmem_limit_bytes=GRANT),
        cost_estimate=pl.CostEstimate(
            flops=flops, transcendentals=0, bytes_accessed=2 * moved
        ),
    )(*[
        pltpu.with_memory_space_constraint(one, pltpu.HBM) if place in far else one
        for place, one in enumerate(inputs)
    ])


def pack_kernel(sides, flat, lift, *refs):
    out, sems = refs[:sides], refs[sides]
    group, count = out[0].shape[1], flat.shape[0]
    side = lax.axis_index("uly")
    copies = []
    for s in reversed(range(sides)):
        heads = pl.ds(pl.multiple_of((side ^ s) * group, group), group)
        for place, source, target in (
            (s, flat.at[:, heads], out[s].at[pl.ds(0, count)]),
            (sides + s, lift, out[s].at[pl.ds(count, lift.shape[0])]),
        ):
            copies.append(pltpu.make_async_copy(source, target, sems.at[place]))
    for copy in copies:
        copy.start()
    for copy in copies:
        copy.wait()


def load_kernel(layers, kernels, *refs):
    out, sems = refs[:-1], refs[-1]
    sources = [kernels.at[layer] for layer in range(layers)]
    part = out[-1].shape[3]
    half = pl.ds(pl.multiple_of(lax.axis_index("grp") * part, part), part)
    sources += [kernels.at[layer, :, :, :, half] for layer in SHARED]
    copies = [
        pltpu.make_async_copy(sources[place], out[place], sems.at[place])
        for place in reversed(range(len(sources)))
    ]
    for copy in copies:
        copy.start()
    for copy in copies:
        copy.wait()


def regroup_kernel(sides, lines, tokens, *refs):
    pieces, out, held = refs[:sides], refs[sides : sides + lines], refs[-1]
    _, group, size = pieces[0].shape
    flat = jnp.concatenate(
        [
            piece[: 3 * tokens]
            .reshape(tokens, 3, group, size)[:, which]
            .astype(jnp.float32)
            .reshape(tokens * group, size)
            for piece in pieces
            for which in range(3)
        ],
        axis=1,
    ).astype(jnp.bfloat16)
    at = line_of(group * tokens)
    source = ((at & (tokens - 1)) << bits(group)) + (at >> bits(tokens))
    held[...] = dot(picked(source, tokens * group), flat).astype(jnp.bfloat16)
    line = lax.axis_index("blk")
    span = group * tokens // lines
    for t in range(lines):
        out[t][...] = held[pl.ds(pl.multiple_of((line ^ t) * span, span), span), :]


def attention_kernel(sides, lines, share, *refs):
    pieces, out, held = refs[:lines], refs[lines : 2 * lines], refs[-1]
    tokens = pieces[0].shape[0] // share
    size = pieces[0].shape[1] // (3 * sides)
    block = sides * tokens
    scale = 1.0 / size**0.5
    line = lax.axis_index("blk")
    empty = jnp.zeros((block, held.shape[1]), jnp.bfloat16)
    held[:block] = empty
    held[held.shape[0] - block :] = empty
    wide = [piece[...].astype(jnp.float32) for piece in pieces]
    for head in range(share):
        q, k, v = [
            jnp.concatenate(
                [
                    piece[
                        head * tokens : (head + 1) * tokens,
                        (s * 3 + which) * size : (s * 3 + which + 1) * size,
                    ]
                    for piece in wide
                    for s in range(sides)
                ],
                axis=0,
            ).astype(jnp.bfloat16)
            for which in range(3)
        ]
        scores = dot_rows(q, k) * scale
        weights = jnp.exp(scores - jnp.max(scores, axis=1, keepdims=True))
        totals = jnp.sum(weights, axis=1, keepdims=True)
        mixed = (dot(weights.astype(jnp.bfloat16), v) / totals).astype(jnp.bfloat16)
        for t in range(lines):
            at = pl.multiple_of(((line ^ t) + 1) * block, block)
            held[pl.ds(at, block), head * size : (head + 1) * size] = mixed[
                t * block : (t + 1) * block
            ]
    for t in range(lines):
        at = pl.multiple_of((line ^ t) * block, block)
        out[t][...] = held[pl.ds(at, 3 * block), :]


def project_kernel(lines, *refs):
    pieces, weights, out = refs[:lines], refs[lines], refs[-1]
    line, side = lax.axis_index("blk"), lax.axis_index("uly")
    depth = pieces[0].shape[1]
    summed = 0.0
    for t in range(lines):
        at = pl.multiple_of((side * lines + (line ^ t)) * depth, depth)
        summed = summed + dot(pieces[t][...], weights[pl.ds(at, depth), :])
    out[...] = summed.astype(jnp.bfloat16)


def fold_kernel(sides, skip, *refs):
    pieces, kernels, out, held = refs[:sides], refs[sides], refs[-2], refs[-1]
    latent, own = out.shape[0] // 9, out.shape[1]
    side = lax.axis_index("uly")
    for s in range(sides):
        lift = pieces[s][skip:].astype(jnp.float32).reshape(latent, own).astype(jnp.bfloat16)
        held[:, pl.ds(pl.multiple_of((side ^ s) * own, own), own)] = lift
    lift = held[...]
    for tap in range(9):
        product = dot_rows(lift, kernels[tap // 3, tap % 3])
        out[tap * latent : (tap + 1) * latent, :] = product.astype(jnp.bfloat16)


def activated(summed, first, width, height):
    row = first + (line_of(summed.shape[0]) >> bits(width))
    inside = (row >= 0) & (row < height)
    return jnp.where(inside, jax.nn.silu(summed), 0.0)


def shifted(summed, half, own):
    size = summed.shape[0]
    summed = summed.reshape(size // (2 * half), 2, half, 3 * own)

    def part(parity, tap):
        return summed[:, parity, :, tap * own : (tap + 1) * own].reshape(size // 2, own)

    column = line_of(size // 2) & (half - 1)
    before = jnp.where(column == 0, 0.0, pltpu.roll(part(1, 0), 1, 0))
    after = jnp.where(column == half - 1, 0.0, pltpu.roll(part(0, 2), size // 2 - 1, 0))
    even = before + part(0, 1) + part(1, 2)
    odd = part(0, 0) + part(1, 1) + after
    both = [one.reshape(size // (2 * half), 1, half, own) for one in (even, odd)]
    return jnp.concatenate(both, axis=1).reshape(size, own)


def convolved(current, kernels, mates, half):
    width = 2 * half
    own = kernels.shape[2]
    size = current.shape[0] - 2 * width

    def product(parts):
        summed = 0.0
        for above in range(3):
            for taps, lanes in parts:
                taps = taps[above].reshape(3 * own, taps.shape[3])
                summed = summed + dot_rows(current[above * width : above * width + size, lanes], taps)
        return shifted(summed, half, own)

    sums = [product([(kernels, slice(None))])]
    if mates:
        group = lax.axis_index("grp")
        part = mates[0].shape[3]
        starts = [pl.multiple_of(place * part, part) for place in (group, 1 - group)]
        sums.append(product([(m, pl.ds(start, part)) for m, start in zip(mates, starts)]))
    return sums


def first_kernel(sides, rows, cols, height, *refs):
    partials, folded, kernels = refs[:sides], refs[sides : 2 * sides], refs[2 * sides]
    mates = refs[2 * sides + 1 : -4]
    out, even_taps, odd_taps, held = refs[-4:]
    side, line = lax.axis_index("uly"), lax.axis_index("blk")
    half = sides * cols
    count = partials[0].shape[0]
    latent = folded[0].shape[0] // 9
    own = folded[0].shape[1]
    empty = jnp.zeros((latent, sides * own), jnp.bfloat16)
    for above in range(3):
        even_taps[above, 2 * latent : 3 * latent, :] = empty
        odd_taps[above, 3 * latent :, :] = empty
        for s in range(sides):
            lanes = pl.ds(pl.multiple_of((side ^ s) * own, own), own)
            for beside in range(3):
                at = (above * 3 + beside) * latent
                taps = folded[s][at : at + latent, :]
                to = (3, 0, 1)[beside] * latent
                even_taps[above, to : to + latent, lanes] = taps
                odd_taps[above, beside * latent : (beside + 1) * latent, lanes] = taps
    at = line_of(count)
    column = at & (cols - 1)
    group = (at >> bits(cols)) & (sides - 1)
    row = (at >> bits(half)) & (rows - 1)
    block = at >> bits(half * rows)
    total = 0.0
    for s in range(sides):
        source = (((block << bits(sides)) + (group ^ side ^ s)) << bits(rows)) + row
        source = (source << bits(cols)) + column
        total = total + dot(picked(source, count), partials[s][...])
    total = total.astype(jnp.bfloat16).astype(jnp.float32)
    wide = 2 * latent
    lines = [
        total[:, i * wide : (i + 1) * wide].reshape(count // half, 1, half, wide) for i in range(2)
    ]
    latents = jnp.concatenate(lines, axis=1).reshape(2 * count, wide)
    place = line_of(2 * count) & (half - 1)
    before = jnp.where(place == 0, 0.0, pltpu.roll(latents, 1, 0))
    after = jnp.where(place == half - 1, 0.0, pltpu.roll(latents, 2 * count - 1, 0))
    start = line * rows * PATCH - (LAYERS - 1)
    size = 2 * count - 2 * half
    for parity, (other, taps) in enumerate(((before, even_taps), (after, odd_taps))):
        current = jnp.concatenate([latents, other], axis=1).astype(jnp.bfloat16)
        summed = 0.0
        for above in range(3):
            summed = summed + dot(current[above * half : above * half + size], taps[above])
        summed = activated(summed, start, half, height).astype(jnp.bfloat16)
        for row in range(size // half):
            at = (2 * row + parity) * half
            held[at : at + half, :] = summed[row * half : (row + 1) * half]
    for place, summed in enumerate(convolved(held, kernels, mates, half)):
        result = activated(summed, start + 1, 2 * half, height).astype(jnp.bfloat16)
        out[:, place * own : (place + 1) * own] = result


def layer_kernel(layer, pieces_in, sides, half, step, height, *refs):
    pieces, kernels, mates = refs[:pieces_in], refs[pieces_in], refs[pieces_in + 1 : -2]
    out, held = refs[-2:]
    side, line = lax.axis_index("uly"), lax.axis_index("blk")
    own = kernels.shape[2]
    for s in range(pieces_in):
        for place in range(pieces[s].shape[1] // own):
            to = side ^ s ^ (place * (sides // 2))
            lanes = pl.ds(pl.multiple_of(to * own, own), own)
            held[:, lanes] = pieces[s][:, place * own : (place + 1) * own]
    width = 2 * half
    first = line * step + layer + 1 - LAYERS
    for place, summed in enumerate(convolved(held, kernels, mates, half)):
        result = activated(summed, first, width, height).astype(jnp.bfloat16)
        if layer == LAYERS - 1:
            at = line_of(result.shape[0])
            column = at & (width - 1)
            source = (at - column) + ((column & 1) << bits(half)) + (column >> 1)
            result = dot(picked(source, result.shape[0]), result).astype(jnp.bfloat16)
        out[:, place * own : (place + 1) * own] = result


def fits_kernels(qkv, lift_weight, conv_weight):
    frames, rows, cols, _, heads, size = qkv.shape
    lines, sides = lax.axis_size("blk"), lax.axis_size("uly")
    powers = all(n & (n - 1) == 0 for n in (lines, sides, rows, cols, heads))
    return (
        powers
        and lax.axis_size("grp") == 2
        and sides >= 4
        and frames == 1
        and rows * PATCH == LAYERS
        and heads % (lines * sides) == 0
        and rows * cols % 8 == 0
        and rows * cols * heads // (lines * sides) % 16 == 0
        and sides * cols % 16 == 0
        and heads // sides % 8 == 0
        and size % 128 == 0
        and conv_weight.shape[3] % 128 == 0
        and lift_weight.size % (heads // sides * size) == 0
        and conv_weight.shape[3] == size
        and lift_weight.shape[0] * 2 % 128 == 0
    )


def body_by_kernels(qkv, out_weight, lift_weight, conv_weight):
    _, rows, cols, _, heads, size = qkv.shape
    lines, sides = lax.axis_size("blk"), lax.axis_size("uly")
    group, share = heads // sides, heads // sides // lines
    latent, own = lift_weight.shape
    tokens, half = rows * cols, sides * cols
    height = lines * rows * PATCH
    width, all_ch = 2 * half, sides * own
    pieces = call(
        functools.partial(pack_kernel, sides),
        0,
        [qkv.reshape(3 * tokens, heads, size), lift_weight.reshape(-1, group, size)],
        [(3 * tokens + lift_weight.size // (group * size), group, size)] * sides,
        [pltpu.SemaphoreType.DMA((2 * sides,))],
        far=(0, 1),
    )
    got = swap(pieces, "uly")
    *kernels, part_1, part_2 = call(
        functools.partial(load_kernel, LAYERS),
        10**8,
        [conv_weight],
        [conv_weight.shape[1:]] * LAYERS
        + [conv_weight.shape[1:4] + (all_ch // 2,)] * len(SHARED),
        [pltpu.SemaphoreType.DMA((LAYERS + len(SHARED),))],
        far=(0,),
    )
    mates = {}
    for layer, part in zip(SHARED, (part_1, part_2)):
        part = lax.ppermute(part, "uly", [(i, i ^ (sides // 2)) for i in range(sides)])
        other = lax.ppermute(part, "grp", [(0, 1), (1, 0)])
        mates[layer] = [part, other]
    span = (share * tokens, sides * 3 * size)
    shared = call(
        functools.partial(regroup_kernel, sides, lines, tokens),
        2 * (group * tokens) ** 2 * span[1],
        got,
        [span] * lines,
        [(group * tokens, span[1])],
    )
    (folded,) = call(
        functools.partial(fold_kernel, sides, 3 * tokens),
        2 * 9 * latent * all_ch * own,
        [*got, kernels[0]],
        [(9 * latent, own)],
        [(latent, all_ch)],
    )
    got = swap(shared, "blk")
    folded = spread(folded, "uly")
    block = sides * tokens
    windows = call(
        functools.partial(attention_kernel, sides, lines, share),
        4 * share * size * (lines * block) ** 2,
        got,
        [(3 * block, share * size)] * lines,
        [((lines + 2) * block, share * size)],
    )
    got = swap(windows, "blk")
    (partial,) = call(
        functools.partial(project_kernel, lines),
        2 * 3 * block * lines * share * size * out_weight.shape[1],
        [*got, out_weight],
        [(3 * block, out_weight.shape[1])],
    )
    got = spread(partial, "uly")
    count = (rows + 2) * PATCH
    (current,) = call(
        functools.partial(first_kernel, sides, rows, cols, height),
        36 * count * width * all_ch * own,
        [*got, *folded, kernels[1], *mates[1]],
        [(count * width, 2 * own)],
        [(3, 4 * latent, all_ch)] * 2 + [((count + 2) * width, all_ch)],
    )
    for layer in range(2, LAYERS):
        got = swap([current] * (sides // 2), "uly")
        extra = mates.get(layer, [])
        kernel = functools.partial(
            layer_kernel, layer, len(got), sides, half, rows * PATCH, height
        )
        held = (count * width, all_ch)
        count -= 2
        (current,) = call(
            kernel,
            18 * count * width * all_ch * own * (2 if extra else 1),
            [*got, kernels[layer], *extra],
            [(count * width, own * (2 if extra else 1))],
            [held],
        )
    return current.reshape(1, count, width, own)


def body(qkv, out_weight, lift_weight, conv_weight):
    if fits_kernels(qkv, lift_weight, conv_weight):
        return body_by_kernels(qkv, out_weight, lift_weight, conv_weight)
    rows, heads = qkv.shape[1], qkv.shape[4]
    lines, sides = lax.axis_size("blk"), lax.axis_size("uly")
    side = lax.axis_index("uly")
    latent_ch = lift_weight.shape[0]
    own = conv_weight.shape[3]
    reach = -(-LAYERS // PATCH)
    lifts = gathered(lift_weight, side)
    folded = jnp.einsum(
        "abdc,ec->abde", conv_weight[0], lifts, preferred_element_type=jnp.float32
    )
    folded = ordered(spread(folded.astype(jnp.bfloat16), "uly"), side)
    folded = jnp.transpose(folded, (1, 2, 0, 3, 4)).reshape(3, 3, sides * own, latent_ch)
    powers = lines & (lines - 1) == 0 and sides & (sides - 1) == 0
    if powers and heads % (lines * sides) == 0:
        patches = window_by_swaps(qkv, out_weight, reach)
    else:
        patches = window_by_gathers(qkv, out_weight, reach)
    height = lines * rows * PATCH
    margin = LAYERS - 1
    start = lax.axis_index("blk") * rows * PATCH
    latent = unfold_patches(patches, latent_ch)
    spare = reach * PATCH - LAYERS
    latent = latent[:, spare : latent.shape[1] - spare]
    current = activate(convolve(latent, folded), start - margin, height)
    for layer in range(1, LAYERS):
        margin -= 1
        kernels = conv_weight[layer]
        if layer > 1:
            current = gathered(current, side)
        current = activate(convolve(current, kernels), start - margin, height)
    return current


def solution(mesh):
    in_specs = (
        P("grp", "blk", "uly", None, None, None),
        P(),
        P(None, "uly"),
        P(None, None, None, "uly", None),
    )
    out_specs = P("grp", "blk", None, "uly")
    return jax.shard_map(
        body, mesh=mesh, in_specs=in_specs, out_specs=out_specs, check_vma=False
    )
```

```python
import functools
import math

import jax
import jax.numpy as jnp
from jax import lax
from jax.experimental import pallas as pl
from jax.experimental.pallas import tpu as pltpu
from jax.sharding import PartitionSpec as P


PATCH = 2
LAYERS = 4
GRANT = 8 * 2**20
SHARED = 2


def swap(pieces, axis):
    count = lax.axis_size(axis)
    got = [pieces[0]]
    for step in range(1, len(pieces)):
        got.append(lax.ppermute(pieces[step], axis, [(i, i ^ step) for i in range(count)]))
    return got


def spread(piece, axis):
    return swap([piece] * lax.axis_size(axis), axis)


def cut(array, start, size, axis):
    return lax.dynamic_slice_in_dim(array, start, size, axis=axis)


def attend(queries, keys, values):
    scale = 1.0 / queries.shape[-1] ** 0.5
    scores = jnp.einsum("hqd,hkd->hqk", queries, keys, preferred_element_type=jnp.float32) * scale
    weights = jnp.exp(scores - jnp.max(scores, axis=2, keepdims=True))
    totals = jnp.sum(weights, axis=2)
    mixed = jnp.einsum(
        "hqk,hkd->hqd", weights.astype(jnp.bfloat16), values, preferred_element_type=jnp.float32
    )
    return (mixed / totals[:, :, None]).astype(jnp.bfloat16)


def ordered(blocks, me):
    stacked = jnp.stack(blocks)
    return jnp.concatenate(
        [cut(stacked, me ^ place, 1, 0) for place in range(len(blocks))], axis=0
    )


def gathered(piece, side):
    blocks = ordered(spread(piece, "uly"), side)
    blocks = jnp.moveaxis(blocks, 0, -2)
    return blocks.reshape(piece.shape[:-1] + (-1,))


def window_by_swaps(qkv, out_weight, reach):
    frames, rows, cols, _, heads, size = qkv.shape
    lines, sides = lax.axis_size("blk"), lax.axis_size("uly")
    line, side = lax.axis_index("blk"), lax.axis_index("uly")
    group, share = heads // sides, heads // sides // lines
    got = swap([cut(qkv, (side ^ s) * group, group, 4) for s in range(sides)], "uly")
    grouped = jnp.stack(got, axis=3)
    grouped = jnp.transpose(grouped, (4, 5, 0, 1, 3, 2, 6))
    got = swap([cut(grouped, (line ^ t) * share, share, 1) for t in range(lines)], "blk")
    shared = ordered(got, line)
    shared = jnp.transpose(shared, (1, 2, 3, 0, 4, 5, 6, 7))
    flat = shared.reshape(3, share, -1, size)
    attended = attend(flat[0], flat[1], flat[2])
    attended = attended.reshape(share, frames, lines * rows, sides * cols, size)
    attended = jnp.transpose(attended, (1, 2, 3, 0, 4)).reshape(
        frames, lines * rows, sides * cols, share * size
    )
    padded = jnp.pad(attended, ((0, 0), (reach, reach), (0, 0), (0, 0)))
    got = swap([cut(padded, (line ^ t) * rows, rows + 2 * reach, 1) for t in range(lines)], "blk")
    partial = 0.0
    for t in range(lines):
        weight = cut(out_weight, ((side * lines) + (line ^ t)) * share * size, share * size, 0)
        partial = partial + jnp.einsum(
            "frcw,wp->frcp", got[t], weight, preferred_element_type=jnp.float32
        )
    partial = partial.astype(jnp.bfloat16)
    got = spread(partial, "uly")
    blocks = []
    for place in range(sides):
        total = 0.0
        for s in range(sides):
            at = (place ^ s) * cols
            total = total + got[s][:, :, at : at + cols].astype(jnp.float32)
        blocks.append(total.astype(jnp.bfloat16))
    patches = ordered(blocks, side)
    patches = jnp.transpose(patches, (1, 2, 0, 3, 4))
    return patches.reshape(frames, rows + 2 * reach, sides * cols, -1)


def window_by_gathers(qkv, out_weight, reach):
    frames, rows, cols, _, heads, size = qkv.shape
    grouped = lax.all_to_all(qkv, "blk", split_axis=4, concat_axis=1, tiled=True)
    flat = [
        lax.all_gather(grouped[:, :, :, which], "uly", axis=2, tiled=True) for which in (1, 2)
    ]
    flat = [grouped[:, :, :, 0]] + flat
    flat = [jnp.swapaxes(one.reshape(-1, one.shape[3], size), 0, 1) for one in flat]
    attended = jnp.swapaxes(attend(*flat), 0, 1)
    attended = attended.reshape(grouped.shape[:3] + grouped.shape[4:])
    restored = lax.all_to_all(attended, "blk", split_axis=1, concat_axis=3, tiled=True)
    patches = jnp.einsum(
        "frcw,wp->frcp",
        restored.reshape(frames, rows, cols, heads * size),
        out_weight,
        preferred_element_type=jnp.float32,
    ).astype(jnp.bfloat16)
    patches = lax.all_gather(patches, "uly", axis=2, tiled=True)
    patches = lax.all_gather(patches, "blk", axis=1, tiled=True)
    padded = jnp.pad(patches, ((0, 0), (reach, reach), (0, 0), (0, 0)))
    return cut(padded, lax.axis_index("blk") * rows, rows + 2 * reach, 1)


def unfold_patches(piece, latent_ch):
    frames, rows, cols = (piece.shape[0], piece.shape[1], piece.shape[2])
    parts = piece.reshape(frames, rows, cols, PATCH, PATCH, latent_ch)
    parts = jnp.transpose(parts, (0, 1, 3, 2, 4, 5))
    return parts.reshape(frames, rows * PATCH, cols * PATCH, latent_ch)


def convolve(current, kernels):
    return lax.conv_general_dilated(
        current,
        kernels,
        (1, 1),
        ((0, 0), (1, 1)),
        dimension_numbers=("NHWC", "HWOI", "NHWC"),
        preferred_element_type=jnp.float32,
    )


def activate(summed, first, height):
    rows = first + lax.broadcasted_iota(jnp.int32, summed.shape, 1)
    inside = (rows >= 0) & (rows < height)
    return jnp.where(inside, jax.nn.silu(summed), 0.0).astype(jnp.bfloat16)


def dot(left, right):
    return jnp.dot(left, right, preferred_element_type=jnp.float32)


def dot_rows(left, right):
    return lax.dot_general(
        left, right, (((1,), (1,)), ((), ())), preferred_element_type=jnp.float32
    )


def picked(source, count):
    rows = source.shape[0]
    places = lax.broadcasted_iota(jnp.int32, (rows, count), 1)
    return jnp.where(places == source, 1.0, 0.0).astype(jnp.bfloat16)


def line_of(rows):
    return lax.broadcasted_iota(jnp.int32, (rows, 1), 0)


def bits(number):
    return number.bit_length() - 1


def call(kernel, flops, inputs, outputs, scratch=(), far=()):
    near = pl.BlockSpec(memory_space=pltpu.VMEM)
    kept = pl.BlockSpec(memory_space=pltpu.HBM)
    moved = sum(one.size for one in inputs) + sum(math.prod(shape) for shape in outputs)
    return pl.pallas_call(
        kernel,
        out_shape=[jax.ShapeDtypeStruct(shape, jnp.bfloat16) for shape in outputs],
        in_specs=[kept if place in far else near for place in range(len(inputs))],
        out_specs=[near] * len(outputs),
        scratch_shapes=[
            pltpu.VMEM(one, jnp.bfloat16) if isinstance(one, tuple) else one for one in scratch
        ],
        compiler_params=pltpu.CompilerParams(vmem_limit_bytes=GRANT),
        cost_estimate=pl.CostEstimate(
            flops=flops, transcendentals=0, bytes_accessed=2 * moved
        ),
    )(*[
        pltpu.with_memory_space_constraint(one, pltpu.HBM) if place in far else one
        for place, one in enumerate(inputs)
    ])


def pack_kernel(sides, flat, lift, *refs):
    out, sems = refs[:sides], refs[sides]
    group, count = out[0].shape[1], flat.shape[0]
    side = lax.axis_index("uly")
    copies = []
    for s in reversed(range(sides)):
        heads = pl.ds(pl.multiple_of((side ^ s) * group, group), group)
        for place, source, target in (
            (s, flat.at[:, heads], out[s].at[pl.ds(0, count)]),
            (sides + s, lift, out[s].at[pl.ds(count, lift.shape[0])]),
        ):
            copies.append(pltpu.make_async_copy(source, target, sems.at[place]))
    for copy in copies:
        copy.start()
    for copy in copies:
        copy.wait()


def load_kernel(layers, kernels, *refs):
    out, sems = refs[:-1], refs[-1]
    sources = [kernels.at[layer] for layer in layers]
    if len(out) > len(layers):
        part = out[-1].shape[3]
        half = pl.ds(pl.multiple_of(lax.axis_index("grp") * part, part), part)
        sources.append(kernels.at[SHARED, :, :, :, half])
    copies = [
        pltpu.make_async_copy(sources[place], out[place], sems.at[place])
        for place in reversed(range(len(sources)))
    ]
    for copy in copies:
        copy.start()
    for copy in copies:
        copy.wait()


def regroup_kernel(sides, lines, tokens, *refs):
    pieces, out, held = refs[:sides], refs[sides : sides + lines], refs[-1]
    _, group, size = pieces[0].shape
    flat = jnp.concatenate(
        [
            piece[: 3 * tokens]
            .reshape(tokens, 3, group, size)[:, which]
            .astype(jnp.float32)
            .reshape(tokens * group, size)
            for piece in pieces
            for which in range(3)
        ],
        axis=1,
    ).astype(jnp.bfloat16)
    at = line_of(group * tokens)
    source = ((at & (tokens - 1)) << bits(group)) + (at >> bits(tokens))
    held[...] = dot(picked(source, tokens * group), flat).astype(jnp.bfloat16)
    line = lax.axis_index("blk")
    span = group * tokens // lines
    for t in range(lines):
        out[t][...] = held[pl.ds(pl.multiple_of((line ^ t) * span, span), span), :]


def attention_kernel(sides, lines, share, *refs):
    pieces, out, held = refs[:lines], refs[lines : 2 * lines], refs[-1]
    tokens = pieces[0].shape[0] // share
    size = pieces[0].shape[1] // (3 * sides)
    block = sides * tokens
    scale = 1.0 / size**0.5
    line = lax.axis_index("blk")
    empty = jnp.zeros((block, held.shape[1]), jnp.bfloat16)
    held[:block] = empty
    held[held.shape[0] - block :] = empty
    wide = [piece[...].astype(jnp.float32) for piece in pieces]
    for head in range(share):
        q, k, v = [
            jnp.concatenate(
                [
                    piece[
                        head * tokens : (head + 1) * tokens,
                        (s * 3 + which) * size : (s * 3 + which + 1) * size,
                    ]
                    for piece in wide
                    for s in range(sides)
                ],
                axis=0,
            ).astype(jnp.bfloat16)
            for which in range(3)
        ]
        scores = dot_rows(q, k) * scale
        weights = jnp.exp(scores - jnp.max(scores, axis=1, keepdims=True))
        totals = jnp.sum(weights, axis=1, keepdims=True)
        mixed = (dot(weights.astype(jnp.bfloat16), v) / totals).astype(jnp.bfloat16)
        for t in range(lines):
            at = pl.multiple_of(((line ^ t) + 1) * block, block)
            held[pl.ds(at, block), head * size : (head + 1) * size] = mixed[
                t * block : (t + 1) * block
            ]
    for t in range(lines):
        at = pl.multiple_of((line ^ t) * block, block)
        out[t][...] = held[pl.ds(at, 3 * block), :]


def project_kernel(lines, *refs):
    pieces, weights, out = refs[:lines], refs[lines], refs[-1]
    line, side = lax.axis_index("blk"), lax.axis_index("uly")
    depth = pieces[0].shape[1]
    summed = 0.0
    for t in range(lines):
        at = pl.multiple_of((side * lines + (line ^ t)) * depth, depth)
        summed = summed + dot(pieces[t][...], weights[pl.ds(at, depth), :])
    out[...] = summed.astype(jnp.bfloat16)


def fold_kernel(sides, skip, *refs):
    pieces, kernels, out, held = refs[:sides], refs[sides], refs[-2], refs[-1]
    latent, own = out.shape[0] // 9, out.shape[1]
    side = lax.axis_index("uly")
    for s in range(sides):
        lift = pieces[s][skip:].astype(jnp.float32).reshape(latent, own).astype(jnp.bfloat16)
        held[:, pl.ds(pl.multiple_of((side ^ s) * own, own), own)] = lift
    lift = held[...]
    for tap in range(9):
        product = dot_rows(lift, kernels[tap // 3, tap % 3])
        out[tap * latent : (tap + 1) * latent, :] = product.astype(jnp.bfloat16)


def activated(summed, first, width, height):
    row = first + (line_of(summed.shape[0]) >> bits(width))
    inside = (row >= 0) & (row < height)
    return jnp.where(inside, jax.nn.silu(summed), 0.0)


def shifted(summed, half, own):
    size = summed.shape[0]
    summed = summed.reshape(size // (2 * half), 2, half, 3 * own)

    def part(parity, tap):
        return summed[:, parity, :, tap * own : (tap + 1) * own].reshape(size // 2, own)

    column = line_of(size // 2) & (half - 1)
    before = jnp.where(column == 0, 0.0, pltpu.roll(part(1, 0), 1, 0))
    after = jnp.where(column == half - 1, 0.0, pltpu.roll(part(0, 2), size // 2 - 1, 0))
    even = before + part(0, 1) + part(1, 2)
    odd = part(0, 0) + part(1, 1) + after
    both = [one.reshape(size // (2 * half), 1, half, own) for one in (even, odd)]
    return jnp.concatenate(both, axis=1).reshape(size, own)


def convolved(current, kernels, mates, half):
    width = 2 * half
    own = kernels.shape[2]
    size = current.shape[0] - 2 * width

    def product(parts):
        summed = 0.0
        for above in range(3):
            for taps, lanes in parts:
                taps = taps[above].reshape(3 * own, taps.shape[3])
                summed = summed + dot_rows(current[above * width : above * width + size, lanes], taps)
        return shifted(summed, half, own)

    sums = [product([(kernels, slice(None))])]
    if mates:
        group = lax.axis_index("grp")
        part = mates[0].shape[3]
        starts = [pl.multiple_of(place * part, part) for place in (group, 1 - group)]
        sums.append(product([(m, pl.ds(start, part)) for m, start in zip(mates, starts)]))
    return sums


def first_kernel(sides, rows, cols, height, *refs):
    partials, folded, kernels = refs[:sides], refs[sides : 2 * sides], refs[2 * sides]
    mates = refs[2 * sides + 1 : -4]
    out, even_taps, odd_taps, held = refs[-4:]
    side, line = lax.axis_index("uly"), lax.axis_index("blk")
    half = sides * cols
    count = partials[0].shape[0]
    latent = folded[0].shape[0] // 9
    own = folded[0].shape[1]
    empty = jnp.zeros((latent, sides * own), jnp.bfloat16)
    for above in range(3):
        even_taps[above, 2 * latent : 3 * latent, :] = empty
        odd_taps[above, 3 * latent :, :] = empty
        for s in range(sides):
            lanes = pl.ds(pl.multiple_of((side ^ s) * own, own), own)
            for beside in range(3):
                at = (above * 3 + beside) * latent
                taps = folded[s][at : at + latent, :]
                to = (3, 0, 1)[beside] * latent
                even_taps[above, to : to + latent, lanes] = taps
                odd_taps[above, beside * latent : (beside + 1) * latent, lanes] = taps
    at = line_of(count)
    column = at & (cols - 1)
    group = (at >> bits(cols)) & (sides - 1)
    row = (at >> bits(half)) & (rows - 1)
    block = at >> bits(half * rows)
    total = 0.0
    for s in range(sides):
        source = (((block << bits(sides)) + (group ^ side ^ s)) << bits(rows)) + row
        source = (source << bits(cols)) + column
        total = total + dot(picked(source, count), partials[s][...])
    total = total.astype(jnp.bfloat16).astype(jnp.float32)
    wide = 2 * latent
    lines = [
        total[:, i * wide : (i + 1) * wide].reshape(count // half, 1, half, wide) for i in range(2)
    ]
    latents = jnp.concatenate(lines, axis=1).reshape(2 * count, wide)
    place = line_of(2 * count) & (half - 1)
    before = jnp.where(place == 0, 0.0, pltpu.roll(latents, 1, 0))
    after = jnp.where(place == half - 1, 0.0, pltpu.roll(latents, 2 * count - 1, 0))
    start = line * rows * PATCH - (LAYERS - 1)
    size = 2 * count - 2 * half
    for parity, (other, taps) in enumerate(((before, even_taps), (after, odd_taps))):
        current = jnp.concatenate([latents, other], axis=1).astype(jnp.bfloat16)
        summed = 0.0
        for above in range(3):
            summed = summed + dot(current[above * half : above * half + size], taps[above])
        summed = activated(summed, start, half, height).astype(jnp.bfloat16)
        for row in range(size // half):
            at = (2 * row + parity) * half
            held[at : at + half, :] = summed[row * half : (row + 1) * half]
    for place, summed in enumerate(convolved(held, kernels, mates, half)):
        result = activated(summed, start + 1, 2 * half, height).astype(jnp.bfloat16)
        out[:, place * own : (place + 1) * own] = result


def layer_kernel(layer, pieces_in, sides, half, step, height, *refs):
    pieces, kernels, mates = refs[:pieces_in], refs[pieces_in], refs[pieces_in + 1 : -2]
    out, held = refs[-2:]
    side, line = lax.axis_index("uly"), lax.axis_index("blk")
    own = kernels.shape[2]
    for s in range(pieces_in):
        for place in range(pieces[s].shape[1] // own):
            to = side ^ s ^ (place * (sides // 2))
            lanes = pl.ds(pl.multiple_of(to * own, own), own)
            held[:, lanes] = pieces[s][:, place * own : (place + 1) * own]
    width = 2 * half
    first = line * step + layer + 1 - LAYERS
    for place, summed in enumerate(convolved(held, kernels, mates, half)):
        result = activated(summed, first, width, height).astype(jnp.bfloat16)
        if layer == LAYERS - 1:
            at = line_of(result.shape[0])
            column = at & (width - 1)
            source = (at - column) + ((column & 1) << bits(half)) + (column >> 1)
            result = dot(picked(source, result.shape[0]), result).astype(jnp.bfloat16)
        out[:, place * own : (place + 1) * own] = result


def fits_kernels(qkv, lift_weight, conv_weight):
    frames, rows, cols, _, heads, size = qkv.shape
    lines, sides = lax.axis_size("blk"), lax.axis_size("uly")
    powers = all(n & (n - 1) == 0 for n in (lines, sides, rows, cols, heads))
    return (
        powers
        and lax.axis_size("grp") == 2
        and sides >= 4
        and frames == 1
        and rows * PATCH == LAYERS
        and heads % (lines * sides) == 0
        and rows * cols % 8 == 0
        and rows * cols * heads // (lines * sides) % 16 == 0
        and sides * cols % 16 == 0
        and heads // sides % 8 == 0
        and size % 128 == 0
        and conv_weight.shape[3] % 128 == 0
        and lift_weight.size % (heads // sides * size) == 0
        and conv_weight.shape[3] == size
        and lift_weight.shape[0] * 2 % 128 == 0
    )


def body_by_kernels(qkv, out_weight, lift_weight, conv_weight):
    _, rows, cols, _, heads, size = qkv.shape
    lines, sides = lax.axis_size("blk"), lax.axis_size("uly")
    group, share = heads // sides, heads // sides // lines
    latent, own = lift_weight.shape
    tokens, half = rows * cols, sides * cols
    height = lines * rows * PATCH
    width, all_ch = 2 * half, sides * own
    pieces = call(
        functools.partial(pack_kernel, sides),
        0,
        [qkv.reshape(3 * tokens, heads, size), lift_weight.reshape(-1, group, size)],
        [(3 * tokens + lift_weight.size // (group * size), group, size)] * sides,
        [pltpu.SemaphoreType.DMA((2 * sides,))],
        far=(0, 1),
    )
    got = swap(pieces, "uly")

    def load(layers, extra):
        shapes = [conv_weight.shape[1:]] * len(layers) + extra
        return call(
            functools.partial(load_kernel, layers),
            10**8,
            [conv_weight],
            shapes,
            [pltpu.SemaphoreType.DMA((len(shapes),))],
            far=(0,),
        )

    kernels = {}
    kernels[0], part = load([0], [conv_weight.shape[1:4] + (all_ch // 2,)])
    later = list(range(1, LAYERS))
    kernels.update(zip(later, load(later, [])))
    far = sides // 2
    across = [(i, i ^ far) for i in range(sides)]
    part = lax.ppermute(part, "uly", across)
    other = lax.ppermute(part, "grp", [(0, 1), (1, 0)])
    mates = {SHARED: [part, other]}
    span = (share * tokens, sides * 3 * size)
    shared = call(
        functools.partial(regroup_kernel, sides, lines, tokens),
        2 * (group * tokens) ** 2 * span[1],
        got,
        [span] * lines,
        [(group * tokens, span[1])],
    )
    (folded,) = call(
        functools.partial(fold_kernel, sides, 3 * tokens),
        2 * 9 * latent * all_ch * own,
        [*got, kernels[0]],
        [(9 * latent, own)],
        [(latent, all_ch)],
    )
    got = swap(shared, "blk")
    beyond = lax.ppermute(folded, "uly", across)
    folded = swap([folded] * far, "uly") + swap([beyond] * far, "uly")
    block = sides * tokens
    windows = call(
        functools.partial(attention_kernel, sides, lines, share),
        4 * share * size * (lines * block) ** 2,
        got,
        [(3 * block, share * size)] * lines,
        [((lines + 2) * block, share * size)],
    )
    got = swap(windows, "blk")
    (partial,) = call(
        functools.partial(project_kernel, lines),
        2 * 3 * block * lines * share * size * out_weight.shape[1],
        [*got, out_weight],
        [(3 * block, out_weight.shape[1])],
    )
    got = spread(partial, "uly")
    count = (rows + 2) * PATCH
    (current,) = call(
        functools.partial(first_kernel, sides, rows, cols, height),
        18 * count * width * all_ch * own,
        [*got, *folded, kernels[1]],
        [(count * width, own)],
        [(3, 4 * latent, all_ch)] * 2 + [((count + 2) * width, all_ch)],
    )
    for layer in range(2, LAYERS):
        whole = current.shape[1] == own
        got = swap([current] * (sides if whole else far), "uly")
        extra = mates.get(layer, [])
        kernel = functools.partial(
            layer_kernel, layer, len(got), sides, half, rows * PATCH, height
        )
        held = (count * width, all_ch)
        count -= 2
        (current,) = call(
            kernel,
            18 * count * width * all_ch * own * (2 if extra else 1),
            [*got, kernels[layer], *extra],
            [(count * width, own * (2 if extra else 1))],
            [held],
        )
    return current.reshape(1, count, width, own)


def body(qkv, out_weight, lift_weight, conv_weight):
    if fits_kernels(qkv, lift_weight, conv_weight):
        return body_by_kernels(qkv, out_weight, lift_weight, conv_weight)
    rows, heads = qkv.shape[1], qkv.shape[4]
    lines, sides = lax.axis_size("blk"), lax.axis_size("uly")
    side = lax.axis_index("uly")
    latent_ch = lift_weight.shape[0]
    own = conv_weight.shape[3]
    reach = -(-LAYERS // PATCH)
    lifts = gathered(lift_weight, side)
    folded = jnp.einsum(
        "abdc,ec->abde", conv_weight[0], lifts, preferred_element_type=jnp.float32
    )
    folded = ordered(spread(folded.astype(jnp.bfloat16), "uly"), side)
    folded = jnp.transpose(folded, (1, 2, 0, 3, 4)).reshape(3, 3, sides * own, latent_ch)
    powers = lines & (lines - 1) == 0 and sides & (sides - 1) == 0
    if powers and heads % (lines * sides) == 0:
        patches = window_by_swaps(qkv, out_weight, reach)
    else:
        patches = window_by_gathers(qkv, out_weight, reach)
    height = lines * rows * PATCH
    margin = LAYERS - 1
    start = lax.axis_index("blk") * rows * PATCH
    latent = unfold_patches(patches, latent_ch)
    spare = reach * PATCH - LAYERS
    latent = latent[:, spare : latent.shape[1] - spare]
    current = activate(convolve(latent, folded), start - margin, height)
    for layer in range(1, LAYERS):
        margin -= 1
        kernels = conv_weight[layer]
        if layer > 1:
            current = gathered(current, side)
        current = activate(convolve(current, kernels), start - margin, height)
    return current


def solution(mesh):
    in_specs = (
        P("grp", "blk", "uly", None, None, None),
        P(),
        P(None, "uly"),
        P(None, None, None, "uly", None),
    )
    out_specs = P("grp", "blk", None, "uly")
    return jax.shard_map(
        body, mesh=mesh, in_specs=in_specs, out_specs=out_specs, check_vma=False
    )
```

```python
import functools
import math

import jax
import jax.numpy as jnp
from jax import lax
from jax.experimental import pallas as pl
from jax.experimental.pallas import tpu as pltpu
from jax.sharding import PartitionSpec as P


PATCH = 2
LAYERS = 4
GRANT = 8 * 2**20
SHARED = 2


def swap(pieces, axis):
    count = lax.axis_size(axis)
    got = [pieces[0]]
    for step in range(1, len(pieces)):
        got.append(lax.ppermute(pieces[step], axis, [(i, i ^ step) for i in range(count)]))
    return got


def spread(piece, axis):
    return swap([piece] * lax.axis_size(axis), axis)


def cut(array, start, size, axis):
    return lax.dynamic_slice_in_dim(array, start, size, axis=axis)


def attend(queries, keys, values):
    scale = 1.0 / queries.shape[-1] ** 0.5
    scores = jnp.einsum("hqd,hkd->hqk", queries, keys, preferred_element_type=jnp.float32) * scale
    weights = jnp.exp(scores - jnp.max(scores, axis=2, keepdims=True))
    totals = jnp.sum(weights, axis=2)
    mixed = jnp.einsum(
        "hqk,hkd->hqd", weights.astype(jnp.bfloat16), values, preferred_element_type=jnp.float32
    )
    return (mixed / totals[:, :, None]).astype(jnp.bfloat16)


def ordered(blocks, me):
    stacked = jnp.stack(blocks)
    return jnp.concatenate(
        [cut(stacked, me ^ place, 1, 0) for place in range(len(blocks))], axis=0
    )


def gathered(piece, side):
    blocks = ordered(spread(piece, "uly"), side)
    blocks = jnp.moveaxis(blocks, 0, -2)
    return blocks.reshape(piece.shape[:-1] + (-1,))


def window_by_swaps(qkv, out_weight, reach):
    frames, rows, cols, _, heads, size = qkv.shape
    lines, sides = lax.axis_size("blk"), lax.axis_size("uly")
    line, side = lax.axis_index("blk"), lax.axis_index("uly")
    group, share = heads // sides, heads // sides // lines
    got = swap([cut(qkv, (side ^ s) * group, group, 4) for s in range(sides)], "uly")
    grouped = jnp.stack(got, axis=3)
    grouped = jnp.transpose(grouped, (4, 5, 0, 1, 3, 2, 6))
    got = swap([cut(grouped, (line ^ t) * share, share, 1) for t in range(lines)], "blk")
    shared = ordered(got, line)
    shared = jnp.transpose(shared, (1, 2, 3, 0, 4, 5, 6, 7))
    flat = shared.reshape(3, share, -1, size)
    attended = attend(flat[0], flat[1], flat[2])
    attended = attended.reshape(share, frames, lines * rows, sides * cols, size)
    attended = jnp.transpose(attended, (1, 2, 3, 0, 4)).reshape(
        frames, lines * rows, sides * cols, share * size
    )
    padded = jnp.pad(attended, ((0, 0), (reach, reach), (0, 0), (0, 0)))
    got = swap([cut(padded, (line ^ t) * rows, rows + 2 * reach, 1) for t in range(lines)], "blk")
    partial = 0.0
    for t in range(lines):
        weight = cut(out_weight, ((side * lines) + (line ^ t)) * share * size, share * size, 0)
        partial = partial + jnp.einsum(
            "frcw,wp->frcp", got[t], weight, preferred_element_type=jnp.float32
        )
    partial = partial.astype(jnp.bfloat16)
    got = spread(partial, "uly")
    blocks = []
    for place in range(sides):
        total = 0.0
        for s in range(sides):
            at = (place ^ s) * cols
            total = total + got[s][:, :, at : at + cols].astype(jnp.float32)
        blocks.append(total.astype(jnp.bfloat16))
    patches = ordered(blocks, side)
    patches = jnp.transpose(patches, (1, 2, 0, 3, 4))
    return patches.reshape(frames, rows + 2 * reach, sides * cols, -1)


def window_by_gathers(qkv, out_weight, reach):
    frames, rows, cols, _, heads, size = qkv.shape
    grouped = lax.all_to_all(qkv, "blk", split_axis=4, concat_axis=1, tiled=True)
    flat = [
        lax.all_gather(grouped[:, :, :, which], "uly", axis=2, tiled=True) for which in (1, 2)
    ]
    flat = [grouped[:, :, :, 0]] + flat
    flat = [jnp.swapaxes(one.reshape(-1, one.shape[3], size), 0, 1) for one in flat]
    attended = jnp.swapaxes(attend(*flat), 0, 1)
    attended = attended.reshape(grouped.shape[:3] + grouped.shape[4:])
    restored = lax.all_to_all(attended, "blk", split_axis=1, concat_axis=3, tiled=True)
    patches = jnp.einsum(
        "frcw,wp->frcp",
        restored.reshape(frames, rows, cols, heads * size),
        out_weight,
        preferred_element_type=jnp.float32,
    ).astype(jnp.bfloat16)
    patches = lax.all_gather(patches, "uly", axis=2, tiled=True)
    patches = lax.all_gather(patches, "blk", axis=1, tiled=True)
    padded = jnp.pad(patches, ((0, 0), (reach, reach), (0, 0), (0, 0)))
    return cut(padded, lax.axis_index("blk") * rows, rows + 2 * reach, 1)


def unfold_patches(piece, latent_ch):
    frames, rows, cols = (piece.shape[0], piece.shape[1], piece.shape[2])
    parts = piece.reshape(frames, rows, cols, PATCH, PATCH, latent_ch)
    parts = jnp.transpose(parts, (0, 1, 3, 2, 4, 5))
    return parts.reshape(frames, rows * PATCH, cols * PATCH, latent_ch)


def convolve(current, kernels):
    return lax.conv_general_dilated(
        current,
        kernels,
        (1, 1),
        ((0, 0), (1, 1)),
        dimension_numbers=("NHWC", "HWOI", "NHWC"),
        preferred_element_type=jnp.float32,
    )


def activate(summed, first, height):
    rows = first + lax.broadcasted_iota(jnp.int32, summed.shape, 1)
    inside = (rows >= 0) & (rows < height)
    return jnp.where(inside, jax.nn.silu(summed), 0.0).astype(jnp.bfloat16)


def dot(left, right):
    return jnp.dot(left, right, preferred_element_type=jnp.float32)


def dot_rows(left, right):
    return lax.dot_general(
        left, right, (((1,), (1,)), ((), ())), preferred_element_type=jnp.float32
    )


def picked(source, count):
    rows = source.shape[0]
    places = lax.broadcasted_iota(jnp.int32, (rows, count), 1)
    return jnp.where(places == source, 1.0, 0.0).astype(jnp.bfloat16)


def line_of(rows):
    return lax.broadcasted_iota(jnp.int32, (rows, 1), 0)


def bits(number):
    return number.bit_length() - 1


def call(kernel, flops, inputs, outputs, scratch=(), far=()):
    near = pl.BlockSpec(memory_space=pltpu.VMEM)
    kept = pl.BlockSpec(memory_space=pltpu.HBM)
    moved = sum(one.size for one in inputs) + sum(math.prod(shape) for shape in outputs)
    return pl.pallas_call(
        kernel,
        out_shape=[jax.ShapeDtypeStruct(shape, jnp.bfloat16) for shape in outputs],
        in_specs=[kept if place in far else near for place in range(len(inputs))],
        out_specs=[near] * len(outputs),
        scratch_shapes=[
            pltpu.VMEM(one, jnp.bfloat16) if isinstance(one, tuple) else one for one in scratch
        ],
        compiler_params=pltpu.CompilerParams(vmem_limit_bytes=GRANT),
        cost_estimate=pl.CostEstimate(
            flops=flops, transcendentals=0, bytes_accessed=2 * moved
        ),
    )(*[
        pltpu.with_memory_space_constraint(one, pltpu.HBM) if place in far else one
        for place, one in enumerate(inputs)
    ])


def pack_kernel(sides, flat, lift, *refs):
    out, sems = refs[:sides], refs[sides]
    group, count = out[0].shape[1], flat.shape[0]
    side = lax.axis_index("uly")
    copies = []
    for s in reversed(range(sides)):
        heads = pl.ds(pl.multiple_of((side ^ s) * group, group), group)
        for place, source, target in (
            (s, flat.at[:, heads], out[s].at[pl.ds(0, count)]),
            (sides + s, lift, out[s].at[pl.ds(count, lift.shape[0])]),
        ):
            copies.append(pltpu.make_async_copy(source, target, sems.at[place]))
    for copy in copies:
        copy.start()
    for copy in copies:
        copy.wait()


def load_kernel(layers, kernels, *refs):
    out, sems = refs[:-1], refs[-1]
    sources = [kernels.at[layer] for layer in layers]
    if len(out) > len(layers):
        part = out[-1].shape[3]
        half = pl.ds(pl.multiple_of(lax.axis_index("grp") * part, part), part)
        sources.append(kernels.at[SHARED, :, :, :, half])
    copies = [
        pltpu.make_async_copy(sources[place], out[place], sems.at[place])
        for place in reversed(range(len(sources)))
    ]
    for copy in copies:
        copy.start()
    for copy in copies:
        copy.wait()


def regroup_kernel(sides, lines, tokens, *refs):
    pieces, out, held = refs[:sides], refs[sides : sides + lines], refs[-1]
    _, group, size = pieces[0].shape
    flat = jnp.concatenate(
        [
            piece[: 3 * tokens]
            .reshape(tokens, 3, group, size)[:, which]
            .astype(jnp.float32)
            .reshape(tokens * group, size)
            for piece in pieces
            for which in range(3)
        ],
        axis=1,
    ).astype(jnp.bfloat16)
    at = line_of(group * tokens)
    source = ((at & (tokens - 1)) << bits(group)) + (at >> bits(tokens))
    held[...] = dot(picked(source, tokens * group), flat).astype(jnp.bfloat16)
    line = lax.axis_index("blk")
    span = group * tokens // lines
    for t in range(lines):
        out[t][...] = held[pl.ds(pl.multiple_of((line ^ t) * span, span), span), :]


def attention_kernel(sides, lines, share, *refs):
    pieces, weights, kept, sent = refs[:lines], refs[lines], refs[-2], refs[-1]
    tokens = pieces[0].shape[0] // share
    size = pieces[0].shape[1] // (3 * sides)
    block = sides * tokens
    scale = 1.0 / size**0.5
    line, side = lax.axis_index("blk"), lax.axis_index("uly")
    mixed = []
    wide = [piece[...].astype(jnp.float32) for piece in pieces]
    for head in range(share):
        q, k, v = [
            jnp.concatenate(
                [
                    piece[
                        head * tokens : (head + 1) * tokens,
                        (s * 3 + which) * size : (s * 3 + which + 1) * size,
                    ]
                    for piece in wide
                    for s in range(sides)
                ],
                axis=0,
            ).astype(jnp.bfloat16)
            for which in range(3)
        ]
        scores = dot_rows(q, k) * scale
        powers = jnp.exp(scores - jnp.max(scores, axis=1, keepdims=True))
        totals = jnp.sum(powers, axis=1, keepdims=True)
        mixed.append((dot(powers.astype(jnp.bfloat16), v) / totals).astype(jnp.bfloat16))
    depth = share * size
    at = pl.multiple_of((side * lines + line) * depth, depth)
    summed = dot(jnp.concatenate(mixed, axis=1), weights[pl.ds(at, depth), :])
    for odd, out in enumerate((kept, sent)):
        rows = [
            summed[t * block + (s ^ odd) * tokens : t * block + ((s ^ odd) + 1) * tokens]
            for t in range(lines)
            for s in range(0, sides, 2)
        ]
        out[...] = jnp.concatenate(rows, axis=0).astype(jnp.bfloat16)


def window_kernel(lines, kept, got, *refs):
    out, held = refs[:lines], refs[-1]
    block = kept.shape[0] // lines
    line = lax.axis_index("blk")
    empty = jnp.zeros((block, held.shape[1]), jnp.bfloat16)
    held[:block] = empty
    held[held.shape[0] - block :] = empty
    total = (kept[...].astype(jnp.float32) + got[...].astype(jnp.float32)).astype(jnp.bfloat16)
    for t in range(lines):
        at = pl.multiple_of(((line ^ t) + 1) * block, block)
        held[pl.ds(at, block), :] = total[t * block : (t + 1) * block]
    for t in range(lines):
        at = pl.multiple_of((line ^ t) * block, block)
        out[t][...] = held[pl.ds(at, 3 * block), :]


def add_kernel(*refs):
    total = refs[0][...].astype(jnp.float32)
    for piece in refs[1:-1]:
        total = total + piece[...].astype(jnp.float32)
    refs[-1][...] = total.astype(jnp.bfloat16)


def fold_kernel(sides, skip, *refs):
    pieces, kernels, out, held = refs[:sides], refs[sides], refs[-2], refs[-1]
    latent, own = out.shape[0] // 9, out.shape[1]
    side = lax.axis_index("uly")
    for s in range(sides):
        lift = pieces[s][skip:].astype(jnp.float32).reshape(latent, own).astype(jnp.bfloat16)
        held[:, pl.ds(pl.multiple_of((side ^ s) * own, own), own)] = lift
    lift = held[...]
    for tap in range(9):
        product = dot_rows(lift, kernels[tap // 3, tap % 3])
        out[tap * latent : (tap + 1) * latent, :] = product.astype(jnp.bfloat16)


def activated(summed, first, width, height):
    row = first + (line_of(summed.shape[0]) >> bits(width))
    inside = (row >= 0) & (row < height)
    return jnp.where(inside, jax.nn.silu(summed), 0.0)


def shifted(summed, half, own):
    size = summed.shape[0]
    summed = summed.reshape(size // (2 * half), 2, half, 3 * own)

    def part(parity, tap):
        return summed[:, parity, :, tap * own : (tap + 1) * own].reshape(size // 2, own)

    column = line_of(size // 2) & (half - 1)
    before = jnp.where(column == 0, 0.0, pltpu.roll(part(1, 0), 1, 0))
    after = jnp.where(column == half - 1, 0.0, pltpu.roll(part(0, 2), size // 2 - 1, 0))
    even = before + part(0, 1) + part(1, 2)
    odd = part(0, 0) + part(1, 1) + after
    both = [one.reshape(size // (2 * half), 1, half, own) for one in (even, odd)]
    return jnp.concatenate(both, axis=1).reshape(size, own)


def convolved(current, kernels, mates, half):
    width = 2 * half
    own = kernels.shape[2]
    size = current.shape[0] - 2 * width

    def product(parts):
        summed = 0.0
        for above in range(3):
            for taps, lanes in parts:
                taps = taps[above].reshape(3 * own, taps.shape[3])
                summed = summed + dot_rows(current[above * width : above * width + size, lanes], taps)
        return shifted(summed, half, own)

    sums = [product([(kernels, slice(None))])]
    if mates:
        group = lax.axis_index("grp")
        part = mates[0].shape[3]
        starts = [pl.multiple_of(place * part, part) for place in (group, 1 - group)]
        sums.append(product([(m, pl.ds(start, part)) for m, start in zip(mates, starts)]))
    return sums


def taps_kernel(sides, *refs):
    folded, even_taps, odd_taps = refs[:sides], refs[-2], refs[-1]
    side = lax.axis_index("uly")
    latent = folded[0].shape[0] // 9
    own = folded[0].shape[1]
    empty = jnp.zeros((latent, sides * own), jnp.bfloat16)
    for above in range(3):
        even_taps[above, 2 * latent : 3 * latent, :] = empty
        odd_taps[above, 3 * latent :, :] = empty
        for s in range(sides):
            lanes = pl.ds(pl.multiple_of((side ^ s) * own, own), own)
            for beside in range(3):
                at = (above * 3 + beside) * latent
                taps = folded[s][at : at + latent, :]
                to = (3, 0, 1)[beside] * latent
                even_taps[above, to : to + latent, lanes] = taps
                odd_taps[above, beside * latent : (beside + 1) * latent, lanes] = taps


def first_kernel(sides, rows, cols, height, *refs):
    partials, (even_taps, odd_taps, kernels, out, held) = refs[:sides], refs[sides:]
    side, line = lax.axis_index("uly"), lax.axis_index("blk")
    half = sides * cols
    part = partials[0].shape[0]
    count = 2 * part
    latent = even_taps.shape[1] // 4
    own = kernels.shape[2]
    at = line_of(count)
    column = at & (cols - 1)
    group = (at >> bits(cols)) & (sides - 1)
    row = (at >> bits(half)) & (rows - 1)
    block = at >> bits(half * rows)
    total = 0.0
    for s in range(sides):
        place = group ^ side ^ s
        source = (((block << bits(sides // 2)) + (place >> 1)) << bits(rows)) + row
        source = (source << bits(cols)) + column
        source = jnp.where(place & 1 == 0, source, -1)
        total = total + dot(picked(source, part), partials[s][...])
    total = total.astype(jnp.bfloat16).astype(jnp.float32)
    wide = 2 * latent
    lines = [
        total[:, i * wide : (i + 1) * wide].reshape(count // half, 1, half, wide) for i in range(2)
    ]
    latents = jnp.concatenate(lines, axis=1).reshape(2 * count, wide)
    place = line_of(2 * count) & (half - 1)
    before = jnp.where(place == 0, 0.0, pltpu.roll(latents, 1, 0))
    after = jnp.where(place == half - 1, 0.0, pltpu.roll(latents, 2 * count - 1, 0))
    start = line * rows * PATCH - (LAYERS - 1)
    size = 2 * count - 2 * half
    for parity, (other, taps) in enumerate(((before, even_taps), (after, odd_taps))):
        current = jnp.concatenate([latents, other], axis=1).astype(jnp.bfloat16)
        summed = 0.0
        for above in range(3):
            summed = summed + dot(current[above * half : above * half + size], taps[above])
        summed = activated(summed, start, half, height).astype(jnp.bfloat16)
        for row in range(size // half):
            at = (2 * row + parity) * half
            held[at : at + half, :] = summed[row * half : (row + 1) * half]
    for place, summed in enumerate(convolved(held, kernels, (), half)):
        result = activated(summed, start + 1, 2 * half, height).astype(jnp.bfloat16)
        out[:, place * own : (place + 1) * own] = result


def layer_kernel(layer, pieces_in, sides, half, step, height, *refs):
    pieces, kernels, mates = refs[:pieces_in], refs[pieces_in], refs[pieces_in + 1 : -2]
    out, held = refs[-2:]
    side, line = lax.axis_index("uly"), lax.axis_index("blk")
    own = kernels.shape[2]
    for s in range(pieces_in):
        for place in range(pieces[s].shape[1] // own):
            to = side ^ s ^ (place * (sides // 2))
            lanes = pl.ds(pl.multiple_of(to * own, own), own)
            held[:, lanes] = pieces[s][:, place * own : (place + 1) * own]
    width = 2 * half
    first = line * step + layer + 1 - LAYERS
    for place, summed in enumerate(convolved(held, kernels, mates, half)):
        result = activated(summed, first, width, height).astype(jnp.bfloat16)
        if layer == LAYERS - 1:
            at = line_of(result.shape[0])
            column = at & (width - 1)
            source = (at - column) + ((column & 1) << bits(half)) + (column >> 1)
            result = dot(picked(source, result.shape[0]), result).astype(jnp.bfloat16)
        out[:, place * own : (place + 1) * own] = result


def fits_kernels(qkv, lift_weight, conv_weight):
    frames, rows, cols, _, heads, size = qkv.shape
    lines, sides = lax.axis_size("blk"), lax.axis_size("uly")
    powers = all(n & (n - 1) == 0 for n in (lines, sides, rows, cols, heads))
    return (
        powers
        and lax.axis_size("grp") == 2
        and sides >= 4
        and frames == 1
        and rows * PATCH == LAYERS
        and heads % (lines * sides) == 0
        and rows * cols % 8 == 0
        and rows * cols * heads // (lines * sides) % 16 == 0
        and rows * cols * sides % 32 == 0
        and sides * cols % 16 == 0
        and heads // sides % 8 == 0
        and size % 128 == 0
        and conv_weight.shape[3] % 128 == 0
        and lift_weight.size % (heads // sides * size) == 0
        and conv_weight.shape[3] == size
        and lift_weight.shape[0] * 2 % 128 == 0
    )


def body_by_kernels(qkv, out_weight, lift_weight, conv_weight):
    _, rows, cols, _, heads, size = qkv.shape
    lines, sides = lax.axis_size("blk"), lax.axis_size("uly")
    group, share = heads // sides, heads // sides // lines
    latent, own = lift_weight.shape
    tokens, half = rows * cols, sides * cols
    height = lines * rows * PATCH
    width, all_ch = 2 * half, sides * own
    pieces = call(
        functools.partial(pack_kernel, sides),
        0,
        [qkv.reshape(3 * tokens, heads, size), lift_weight.reshape(-1, group, size)],
        [(3 * tokens + lift_weight.size // (group * size), group, size)] * sides,
        [pltpu.SemaphoreType.DMA((2 * sides,))],
        far=(0, 1),
    )
    got = swap(pieces, "uly")

    def load(layers, extra):
        shapes = [conv_weight.shape[1:]] * len(layers) + extra
        return call(
            functools.partial(load_kernel, layers),
            10**8,
            [conv_weight],
            shapes,
            [pltpu.SemaphoreType.DMA((len(shapes),))],
            far=(0,),
        )

    kernels = {}
    kernels[0], part = load([0], [conv_weight.shape[1:4] + (all_ch // 2,)])
    (kernels[1],) = load([1], [])
    later = list(range(2, LAYERS))
    kernels.update(zip(later, load(later, [])))
    far = sides // 2
    across = [(i, i ^ far) for i in range(sides)]
    part = lax.ppermute(part, "uly", across)
    other = lax.ppermute(part, "grp", [(0, 1), (1, 0)])
    mates = {SHARED: [part, other]}
    span = (share * tokens, sides * 3 * size)
    shared = call(
        functools.partial(regroup_kernel, sides, lines, tokens),
        2 * (group * tokens) ** 2 * span[1],
        got,
        [span] * lines,
        [(group * tokens, span[1])],
    )
    (folded,) = call(
        functools.partial(fold_kernel, sides, 3 * tokens),
        2 * 9 * latent * all_ch * own,
        [*got, kernels[0]],
        [(9 * latent, own)],
        [(latent, all_ch)],
    )
    got = swap(shared, "blk")
    beyond = lax.ppermute(folded, "uly", across)
    folded = swap([folded] * far, "uly") + swap([beyond] * far, "uly")
    (*taps,) = call(
        functools.partial(taps_kernel, sides), 10**7, folded, [(3, 4 * latent, all_ch)] * 2
    )
    block, features = sides // 2 * tokens, out_weight.shape[1]
    kept, sent = call(
        functools.partial(attention_kernel, sides, lines, share),
        16 * share * size * (lines * block) ** 2,
        [*got, out_weight],
        [(lines * block, features)] * 2,
    )
    _, got = swap([sent] * 2, "uly")
    windows = call(
        functools.partial(window_kernel, lines),
        10**6,
        [kept, got],
        [(3 * block, features)] * lines,
        [((lines + 2) * block, features)],
    )
    got = swap(windows, "blk")
    (partial,) = call(add_kernel, 10**6, got, [(3 * block, features)])
    got = spread(partial, "uly")
    count = (rows + 2) * PATCH
    (current,) = call(
        functools.partial(first_kernel, sides, rows, cols, height),
        18 * count * width * all_ch * own,
        [*got, *taps, kernels[1]],
        [(count * width, own)],
        [((count + 2) * width, all_ch)],
    )
    for layer in range(2, LAYERS):
        whole = current.shape[1] == own
        got = swap([current] * (sides if whole else far), "uly")
        extra = mates.get(layer, [])
        kernel = functools.partial(
            layer_kernel, layer, len(got), sides, half, rows * PATCH, height
        )
        held = (count * width, all_ch)
        count -= 2
        (current,) = call(
            kernel,
            18 * count * width * all_ch * own * (2 if extra else 1),
            [*got, kernels[layer], *extra],
            [(count * width, own * (2 if extra else 1))],
            [held],
        )
    return current.reshape(1, count, width, own)


def body(qkv, out_weight, lift_weight, conv_weight):
    if fits_kernels(qkv, lift_weight, conv_weight):
        return body_by_kernels(qkv, out_weight, lift_weight, conv_weight)
    rows, heads = qkv.shape[1], qkv.shape[4]
    lines, sides = lax.axis_size("blk"), lax.axis_size("uly")
    side = lax.axis_index("uly")
    latent_ch = lift_weight.shape[0]
    own = conv_weight.shape[3]
    reach = -(-LAYERS // PATCH)
    lifts = gathered(lift_weight, side)
    folded = jnp.einsum(
        "abdc,ec->abde", conv_weight[0], lifts, preferred_element_type=jnp.float32
    )
    folded = ordered(spread(folded.astype(jnp.bfloat16), "uly"), side)
    folded = jnp.transpose(folded, (1, 2, 0, 3, 4)).reshape(3, 3, sides * own, latent_ch)
    powers = lines & (lines - 1) == 0 and sides & (sides - 1) == 0
    if powers and heads % (lines * sides) == 0:
        patches = window_by_swaps(qkv, out_weight, reach)
    else:
        patches = window_by_gathers(qkv, out_weight, reach)
    height = lines * rows * PATCH
    margin = LAYERS - 1
    start = lax.axis_index("blk") * rows * PATCH
    latent = unfold_patches(patches, latent_ch)
    spare = reach * PATCH - LAYERS
    latent = latent[:, spare : latent.shape[1] - spare]
    current = activate(convolve(latent, folded), start - margin, height)
    for layer in range(1, LAYERS):
        margin -= 1
        kernels = conv_weight[layer]
        if layer > 1:
            current = gathered(current, side)
        current = activate(convolve(current, kernels), start - margin, height)
    return current


def solution(mesh):
    in_specs = (
        P("grp", "blk", "uly", None, None, None),
        P(),
        P(None, "uly"),
        P(None, None, None, "uly", None),
    )
    out_specs = P("grp", "blk", None, "uly")
    return jax.shard_map(
        body, mesh=mesh, in_specs=in_specs, out_specs=out_specs, check_vma=False
    )
```

```python
import functools
import math

import jax
import jax.numpy as jnp
from jax import lax
from jax.experimental import pallas as pl
from jax.experimental.pallas import tpu as pltpu
from jax.sharding import PartitionSpec as P


PATCH = 2
LAYERS = 4
GRANT = 8 * 2**20
SHARED = 2


def swap(pieces, axis):
    count = lax.axis_size(axis)
    got = [pieces[0]]
    for step in range(1, len(pieces)):
        got.append(lax.ppermute(pieces[step], axis, [(i, i ^ step) for i in range(count)]))
    return got


def spread(piece, axis):
    return swap([piece] * lax.axis_size(axis), axis)


def cut(array, start, size, axis):
    return lax.dynamic_slice_in_dim(array, start, size, axis=axis)


def attend(queries, keys, values):
    scale = 1.0 / queries.shape[-1] ** 0.5
    scores = jnp.einsum("hqd,hkd->hqk", queries, keys, preferred_element_type=jnp.float32) * scale
    weights = jnp.exp(scores - jnp.max(scores, axis=2, keepdims=True))
    totals = jnp.sum(weights, axis=2)
    mixed = jnp.einsum(
        "hqk,hkd->hqd", weights.astype(jnp.bfloat16), values, preferred_element_type=jnp.float32
    )
    return (mixed / totals[:, :, None]).astype(jnp.bfloat16)


def ordered(blocks, me):
    stacked = jnp.stack(blocks)
    return jnp.concatenate(
        [cut(stacked, me ^ place, 1, 0) for place in range(len(blocks))], axis=0
    )


def gathered(piece, side):
    blocks = ordered(spread(piece, "uly"), side)
    blocks = jnp.moveaxis(blocks, 0, -2)
    return blocks.reshape(piece.shape[:-1] + (-1,))


def window_by_swaps(qkv, out_weight, reach):
    frames, rows, cols, _, heads, size = qkv.shape
    lines, sides = lax.axis_size("blk"), lax.axis_size("uly")
    line, side = lax.axis_index("blk"), lax.axis_index("uly")
    group, share = heads // sides, heads // sides // lines
    got = swap([cut(qkv, (side ^ s) * group, group, 4) for s in range(sides)], "uly")
    grouped = jnp.stack(got, axis=3)
    grouped = jnp.transpose(grouped, (4, 5, 0, 1, 3, 2, 6))
    got = swap([cut(grouped, (line ^ t) * share, share, 1) for t in range(lines)], "blk")
    shared = ordered(got, line)
    shared = jnp.transpose(shared, (1, 2, 3, 0, 4, 5, 6, 7))
    flat = shared.reshape(3, share, -1, size)
    attended = attend(flat[0], flat[1], flat[2])
    attended = attended.reshape(share, frames, lines * rows, sides * cols, size)
    attended = jnp.transpose(attended, (1, 2, 3, 0, 4)).reshape(
        frames, lines * rows, sides * cols, share * size
    )
    padded = jnp.pad(attended, ((0, 0), (reach, reach), (0, 0), (0, 0)))
    got = swap([cut(padded, (line ^ t) * rows, rows + 2 * reach, 1) for t in range(lines)], "blk")
    partial = 0.0
    for t in range(lines):
        weight = cut(out_weight, ((side * lines) + (line ^ t)) * share * size, share * size, 0)
        partial = partial + jnp.einsum(
            "frcw,wp->frcp", got[t], weight, preferred_element_type=jnp.float32
        )
    partial = partial.astype(jnp.bfloat16)
    got = spread(partial, "uly")
    blocks = []
    for place in range(sides):
        total = 0.0
        for s in range(sides):
            at = (place ^ s) * cols
            total = total + got[s][:, :, at : at + cols].astype(jnp.float32)
        blocks.append(total.astype(jnp.bfloat16))
    patches = ordered(blocks, side)
    patches = jnp.transpose(patches, (1, 2, 0, 3, 4))
    return patches.reshape(frames, rows + 2 * reach, sides * cols, -1)


def window_by_gathers(qkv, out_weight, reach):
    frames, rows, cols, _, heads, size = qkv.shape
    grouped = lax.all_to_all(qkv, "blk", split_axis=4, concat_axis=1, tiled=True)
    flat = [
        lax.all_gather(grouped[:, :, :, which], "uly", axis=2, tiled=True) for which in (1, 2)
    ]
    flat = [grouped[:, :, :, 0]] + flat
    flat = [jnp.swapaxes(one.reshape(-1, one.shape[3], size), 0, 1) for one in flat]
    attended = jnp.swapaxes(attend(*flat), 0, 1)
    attended = attended.reshape(grouped.shape[:3] + grouped.shape[4:])
    restored = lax.all_to_all(attended, "blk", split_axis=1, concat_axis=3, tiled=True)
    patches = jnp.einsum(
        "frcw,wp->frcp",
        restored.reshape(frames, rows, cols, heads * size),
        out_weight,
        preferred_element_type=jnp.float32,
    ).astype(jnp.bfloat16)
    patches = lax.all_gather(patches, "uly", axis=2, tiled=True)
    patches = lax.all_gather(patches, "blk", axis=1, tiled=True)
    padded = jnp.pad(patches, ((0, 0), (reach, reach), (0, 0), (0, 0)))
    return cut(padded, lax.axis_index("blk") * rows, rows + 2 * reach, 1)


def unfold_patches(piece, latent_ch):
    frames, rows, cols = (piece.shape[0], piece.shape[1], piece.shape[2])
    parts = piece.reshape(frames, rows, cols, PATCH, PATCH, latent_ch)
    parts = jnp.transpose(parts, (0, 1, 3, 2, 4, 5))
    return parts.reshape(frames, rows * PATCH, cols * PATCH, latent_ch)


def convolve(current, kernels):
    return lax.conv_general_dilated(
        current,
        kernels,
        (1, 1),
        ((0, 0), (1, 1)),
        dimension_numbers=("NHWC", "HWOI", "NHWC"),
        preferred_element_type=jnp.float32,
    )


def activate(summed, first, height):
    rows = first + lax.broadcasted_iota(jnp.int32, summed.shape, 1)
    inside = (rows >= 0) & (rows < height)
    return jnp.where(inside, jax.nn.silu(summed), 0.0).astype(jnp.bfloat16)


def dot(left, right):
    return jnp.dot(left, right, preferred_element_type=jnp.float32)


def dot_rows(left, right):
    return lax.dot_general(
        left, right, (((1,), (1,)), ((), ())), preferred_element_type=jnp.float32
    )


def picked(source, count):
    rows = source.shape[0]
    places = lax.broadcasted_iota(jnp.int32, (rows, count), 1)
    return jnp.where(places == source, 1.0, 0.0).astype(jnp.bfloat16)


def line_of(rows):
    return lax.broadcasted_iota(jnp.int32, (rows, 1), 0)


def bits(number):
    return number.bit_length() - 1


def call(kernel, flops, inputs, outputs, scratch=(), far=()):
    near = pl.BlockSpec(memory_space=pltpu.VMEM)
    kept = pl.BlockSpec(memory_space=pltpu.HBM)
    moved = sum(one.size for one in inputs) + sum(math.prod(shape) for shape in outputs)
    return pl.pallas_call(
        kernel,
        out_shape=[jax.ShapeDtypeStruct(shape, jnp.bfloat16) for shape in outputs],
        in_specs=[kept if place in far else near for place in range(len(inputs))],
        out_specs=[near] * len(outputs),
        scratch_shapes=[
            pltpu.VMEM(one, jnp.bfloat16) if isinstance(one, tuple) else one for one in scratch
        ],
        compiler_params=pltpu.CompilerParams(vmem_limit_bytes=GRANT),
        cost_estimate=pl.CostEstimate(
            flops=flops, transcendentals=0, bytes_accessed=2 * moved
        ),
    )(*[
        pltpu.with_memory_space_constraint(one, pltpu.HBM) if place in far else one
        for place, one in enumerate(inputs)
    ])


def pack_kernel(sides, flat, lift, *refs):
    out, sems = refs[:sides], refs[sides]
    group, count = out[0].shape[1], flat.shape[0]
    side = lax.axis_index("uly")
    copies = []
    for s in reversed(range(sides)):
        heads = pl.ds(pl.multiple_of((side ^ s) * group, group), group)
        for place, source, target in (
            (s, flat.at[:, heads], out[s].at[pl.ds(0, count)]),
            (sides + s, lift, out[s].at[pl.ds(count, lift.shape[0])]),
        ):
            copies.append(pltpu.make_async_copy(source, target, sems.at[place]))
    for copy in copies:
        copy.start()
    for copy in copies:
        copy.wait()


def load_kernel(layers, kernels, *refs):
    out, sems = refs[:-1], refs[-1]
    sources = [kernels.at[layer] for layer in layers]
    parts = len(out) - len(layers)
    for place in range(parts):
        part = out[-1].shape[3]
        at = (lax.axis_index("grp") * parts + place) * part
        sources.append(kernels.at[SHARED, :, :, :, pl.ds(pl.multiple_of(at, part), part)])
    copies = [
        pltpu.make_async_copy(sources[place], out[place], sems.at[place])
        for place in reversed(range(len(sources)))
    ]
    for copy in copies:
        copy.start()
    for copy in copies:
        copy.wait()


def join_kernel(*refs):
    parts, out = refs[:-1], refs[-1]
    size, each = parts[0].shape[3], len(parts) // 2
    group = lax.axis_index("grp")
    for place, part in enumerate(parts):
        owner = group if place < each else 1 - group
        at = pl.multiple_of((owner * each + place % each) * size, size)
        out[:, :, :, pl.ds(at, size)] = part[...]


def regroup_kernel(sides, lines, tokens, *refs):
    pieces, out, held = refs[:sides], refs[sides : sides + lines], refs[-1]
    _, group, size = pieces[0].shape
    flat = jnp.concatenate(
        [
            piece[: 3 * tokens]
            .reshape(tokens, 3, group, size)[:, which]
            .astype(jnp.float32)
            .reshape(tokens * group, size)
            for piece in pieces
            for which in range(3)
        ],
        axis=1,
    ).astype(jnp.bfloat16)
    at = line_of(group * tokens)
    source = ((at & (tokens - 1)) << bits(group)) + (at >> bits(tokens))
    held[...] = dot(picked(source, tokens * group), flat).astype(jnp.bfloat16)
    line = lax.axis_index("blk")
    span = group * tokens // lines
    for t in range(lines):
        out[t][...] = held[pl.ds(pl.multiple_of((line ^ t) * span, span), span), :]


def attention_kernel(sides, lines, share, *refs):
    pieces, weights, kept, sent = refs[:lines], refs[lines], refs[-2], refs[-1]
    tokens = pieces[0].shape[0] // share
    size = pieces[0].shape[1] // (3 * sides)
    block = sides * tokens
    scale = 1.0 / size**0.5
    line, side = lax.axis_index("blk"), lax.axis_index("uly")
    mixed = []
    wide = [piece[...].astype(jnp.float32) for piece in pieces]
    for head in range(share):
        q, k, v = [
            jnp.concatenate(
                [
                    piece[
                        head * tokens : (head + 1) * tokens,
                        (s * 3 + which) * size : (s * 3 + which + 1) * size,
                    ]
                    for piece in wide
                    for s in range(sides)
                ],
                axis=0,
            ).astype(jnp.bfloat16)
            for which in range(3)
        ]
        scores = dot_rows(q, k) * scale
        powers = jnp.exp(scores - jnp.max(scores, axis=1, keepdims=True))
        totals = jnp.sum(powers, axis=1, keepdims=True)
        mixed.append((dot(powers.astype(jnp.bfloat16), v) / totals).astype(jnp.bfloat16))
    depth = share * size
    at = pl.multiple_of((side * lines + line) * depth, depth)
    summed = dot(jnp.concatenate(mixed, axis=1), weights[pl.ds(at, depth), :])
    for odd, out in enumerate((kept, sent)):
        rows = [
            summed[t * block + (s ^ odd) * tokens : t * block + ((s ^ odd) + 1) * tokens]
            for t in range(lines)
            for s in range(0, sides, 2)
        ]
        out[...] = jnp.concatenate(rows, axis=0).astype(jnp.bfloat16)


def window_kernel(lines, kept, got, *refs):
    out, held = refs[:lines], refs[-1]
    block = kept.shape[0] // lines
    line = lax.axis_index("blk")
    empty = jnp.zeros((block, held.shape[1]), jnp.bfloat16)
    held[:block] = empty
    held[held.shape[0] - block :] = empty
    total = (kept[...].astype(jnp.float32) + got[...].astype(jnp.float32)).astype(jnp.bfloat16)
    for t in range(lines):
        at = pl.multiple_of(((line ^ t) + 1) * block, block)
        held[pl.ds(at, block), :] = total[t * block : (t + 1) * block]
    for t in range(lines):
        at = pl.multiple_of((line ^ t) * block, block)
        out[t][...] = held[pl.ds(at, 3 * block), :]


def add_kernel(*refs):
    total = refs[0][...].astype(jnp.float32)
    for piece in refs[1:-1]:
        total = total + piece[...].astype(jnp.float32)
    refs[-1][...] = total.astype(jnp.bfloat16)


def fold_kernel(sides, skip, *refs):
    pieces, kernels, out, held = refs[:sides], refs[sides], refs[-2], refs[-1]
    latent, own = out.shape[0] // 9, out.shape[1]
    side = lax.axis_index("uly")
    for s in range(sides):
        lift = pieces[s][skip:].astype(jnp.float32).reshape(latent, own).astype(jnp.bfloat16)
        held[:, pl.ds(pl.multiple_of((side ^ s) * own, own), own)] = lift
    lift = held[...]
    for tap in range(9):
        product = dot_rows(lift, kernels[tap // 3, tap % 3])
        out[tap * latent : (tap + 1) * latent, :] = product.astype(jnp.bfloat16)


def activated(summed, first, width, height):
    row = first + (line_of(summed.shape[0]) >> bits(width))
    inside = (row >= 0) & (row < height)
    return jnp.where(inside, jax.nn.silu(summed), 0.0)


def shifted(summed, half, own):
    size = summed.shape[0]
    summed = summed.reshape(size // (2 * half), 2, half, 3 * own)

    def part(parity, tap):
        return summed[:, parity, :, tap * own : (tap + 1) * own].reshape(size // 2, own)

    column = line_of(size // 2) & (half - 1)
    before = jnp.where(column == 0, 0.0, pltpu.roll(part(1, 0), 1, 0))
    after = jnp.where(column == half - 1, 0.0, pltpu.roll(part(0, 2), size // 2 - 1, 0))
    even = before + part(0, 1) + part(1, 2)
    odd = part(0, 0) + part(1, 1) + after
    both = [one.reshape(size // (2 * half), 1, half, own) for one in (even, odd)]
    return jnp.concatenate(both, axis=1).reshape(size, own)


def convolved(current, kernels, half):
    width = 2 * half
    own = kernels.shape[2]
    size = current.shape[0] - 2 * width
    summed = 0.0
    for above in range(3):
        taps = kernels[above].reshape(3 * own, kernels.shape[3])
        summed = summed + dot_rows(current[above * width : above * width + size], taps)
    return shifted(summed, half, own)


def taps_kernel(sides, *refs):
    folded, even_taps, odd_taps = refs[:sides], refs[-2], refs[-1]
    side = lax.axis_index("uly")
    latent = folded[0].shape[0] // 9
    own = folded[0].shape[1]
    empty = jnp.zeros((latent, sides * own), jnp.bfloat16)
    for above in range(3):
        even_taps[above, 2 * latent : 3 * latent, :] = empty
        odd_taps[above, 3 * latent :, :] = empty
        for s in range(sides):
            lanes = pl.ds(pl.multiple_of((side ^ s) * own, own), own)
            for beside in range(3):
                at = (above * 3 + beside) * latent
                taps = folded[s][at : at + latent, :]
                to = (3, 0, 1)[beside] * latent
                even_taps[above, to : to + latent, lanes] = taps
                odd_taps[above, beside * latent : (beside + 1) * latent, lanes] = taps


def first_kernel(sides, rows, cols, height, *refs):
    partials, (even_taps, odd_taps, kernels, out, held) = refs[:sides], refs[sides:]
    side, line = lax.axis_index("uly"), lax.axis_index("blk")
    half = sides * cols
    part = partials[0].shape[0]
    count = 2 * part
    latent = even_taps.shape[1] // 4
    at = line_of(count)
    column = at & (cols - 1)
    group = (at >> bits(cols)) & (sides - 1)
    row = (at >> bits(half)) & (rows - 1)
    block = at >> bits(half * rows)
    total = 0.0
    for s in range(sides):
        place = group ^ side ^ s
        source = (((block << bits(sides // 2)) + (place >> 1)) << bits(rows)) + row
        source = (source << bits(cols)) + column
        source = jnp.where(place & 1 == 0, source, -1)
        total = total + dot(picked(source, part), partials[s][...])
    total = total.astype(jnp.bfloat16).astype(jnp.float32)
    wide = 2 * latent
    lines = [
        total[:, i * wide : (i + 1) * wide].reshape(count // half, 1, half, wide) for i in range(2)
    ]
    latents = jnp.concatenate(lines, axis=1).reshape(2 * count, wide)
    place = line_of(2 * count) & (half - 1)
    before = jnp.where(place == 0, 0.0, pltpu.roll(latents, 1, 0))
    after = jnp.where(place == half - 1, 0.0, pltpu.roll(latents, 2 * count - 1, 0))
    start = line * rows * PATCH - (LAYERS - 1)
    size = 2 * count - 2 * half
    for parity, (other, taps) in enumerate(((before, even_taps), (after, odd_taps))):
        current = jnp.concatenate([latents, other], axis=1).astype(jnp.bfloat16)
        summed = 0.0
        for above in range(3):
            summed = summed + dot(current[above * half : above * half + size], taps[above])
        summed = activated(summed, start, half, height).astype(jnp.bfloat16)
        for row in range(size // half):
            at = (2 * row + parity) * half
            held[at : at + half, :] = summed[row * half : (row + 1) * half]
    summed = convolved(held, kernels, half)
    out[...] = activated(summed, start + 1, 2 * half, height).astype(jnp.bfloat16)


def layer_kernel(layer, pieces_in, sides, half, step, height, *refs):
    pieces, kernels = refs[:pieces_in], refs[pieces_in:-2]
    out, held = refs[-2:]
    side, line = lax.axis_index("uly"), lax.axis_index("blk")
    own = kernels[0].shape[2]
    for s in range(pieces_in):
        for place in range(pieces[s].shape[1] // own):
            to = side ^ s ^ (place * (sides // 2))
            lanes = pl.ds(pl.multiple_of(to * own, own), own)
            held[:, lanes] = pieces[s][:, place * own : (place + 1) * own]
    width = 2 * half
    first = line * step + layer + 1 - LAYERS
    for place, taps in enumerate(kernels):
        summed = convolved(held, taps, half)
        result = activated(summed, first, width, height).astype(jnp.bfloat16)
        if layer == LAYERS - 1:
            at = line_of(result.shape[0])
            column = at & (width - 1)
            source = (at - column) + ((column & 1) << bits(half)) + (column >> 1)
            result = dot(picked(source, result.shape[0]), result).astype(jnp.bfloat16)
        out[:, place * own : (place + 1) * own] = result


def fits_kernels(qkv, lift_weight, conv_weight):
    frames, rows, cols, _, heads, size = qkv.shape
    lines, sides = lax.axis_size("blk"), lax.axis_size("uly")
    powers = all(n & (n - 1) == 0 for n in (lines, sides, rows, cols, heads))
    return (
        powers
        and lax.axis_size("grp") == 2
        and sides >= 4
        and frames == 1
        and rows * PATCH == LAYERS
        and heads % (lines * sides) == 0
        and rows * cols % 8 == 0
        and rows * cols * heads // (lines * sides) % 16 == 0
        and rows * cols * sides % 32 == 0
        and sides * cols % 16 == 0
        and heads // sides % 8 == 0
        and size % 128 == 0
        and conv_weight.shape[3] % 128 == 0
        and lift_weight.size % (heads // sides * size) == 0
        and conv_weight.shape[3] == size
        and lift_weight.shape[0] * 2 % 128 == 0
    )


def body_by_kernels(qkv, out_weight, lift_weight, conv_weight):
    _, rows, cols, _, heads, size = qkv.shape
    lines, sides = lax.axis_size("blk"), lax.axis_size("uly")
    group, share = heads // sides, heads // sides // lines
    latent, own = lift_weight.shape
    tokens, half = rows * cols, sides * cols
    height = lines * rows * PATCH
    width, all_ch = 2 * half, sides * own
    pieces = call(
        functools.partial(pack_kernel, sides),
        0,
        [qkv.reshape(3 * tokens, heads, size), lift_weight.reshape(-1, group, size)],
        [(3 * tokens + lift_weight.size // (group * size), group, size)] * sides,
        [pltpu.SemaphoreType.DMA((2 * sides,))],
        far=(0, 1),
    )
    got = swap(pieces, "uly")

    def load(layers, extra):
        shapes = [conv_weight.shape[1:]] * len(layers) + extra
        return call(
            functools.partial(load_kernel, layers),
            10**8,
            [conv_weight],
            shapes,
            [pltpu.SemaphoreType.DMA((len(shapes),))],
            far=(0,),
        )

    far = sides // 2
    across = [(i, i ^ far) for i in range(sides)]
    kernels = {}
    quarter = conv_weight.shape[1:4] + (all_ch // 4,)
    kernels[0], kernels[1], *parts = load([0, 1], [quarter] * 2)
    later = list(range(2, LAYERS))
    kernels.update(zip(later, load(later, [])))
    others = []
    for place in range(2):
        parts[place] = lax.ppermute(parts[place], "uly", across)
        others.append(lax.ppermute(parts[place], "grp", [(0, 1), (1, 0)]))
    (mate,) = call(join_kernel, 10**7, parts + others, [conv_weight.shape[1:]])
    mates = {SHARED: [mate]}
    span = (share * tokens, sides * 3 * size)
    shared = call(
        functools.partial(regroup_kernel, sides, lines, tokens),
        2 * (group * tokens) ** 2 * span[1],
        got,
        [span] * lines,
        [(group * tokens, span[1])],
    )
    (folded,) = call(
        functools.partial(fold_kernel, sides, 3 * tokens),
        2 * 9 * latent * all_ch * own,
        [*got, kernels[0]],
        [(9 * latent, own)],
        [(latent, all_ch)],
    )
    got = swap(shared, "blk")
    beyond = lax.ppermute(folded, "uly", across)
    folded = swap([folded] * far, "uly") + swap([beyond] * far, "uly")
    (*taps,) = call(
        functools.partial(taps_kernel, sides), 10**7, folded, [(3, 4 * latent, all_ch)] * 2
    )
    block, features = sides // 2 * tokens, out_weight.shape[1]
    kept, sent = call(
        functools.partial(attention_kernel, sides, lines, share),
        16 * share * size * (lines * block) ** 2,
        [*got, out_weight],
        [(lines * block, features)] * 2,
    )
    _, got = swap([sent] * 2, "uly")
    windows = call(
        functools.partial(window_kernel, lines),
        10**6,
        [kept, got],
        [(3 * block, features)] * lines,
        [((lines + 2) * block, features)],
    )
    got = swap(windows, "blk")
    (partial,) = call(add_kernel, 10**6, got, [(3 * block, features)])
    got = spread(partial, "uly")
    count = (rows + 2) * PATCH
    (current,) = call(
        functools.partial(first_kernel, sides, rows, cols, height),
        18 * count * width * all_ch * own,
        [*got, *taps, kernels[1]],
        [(count * width, own)],
        [((count + 2) * width, all_ch)],
    )
    for layer in range(2, LAYERS):
        whole = current.shape[1] == own
        got = swap([current] * (sides if whole else far), "uly")
        extra = mates.get(layer, [])
        kernel = functools.partial(
            layer_kernel, layer, len(got), sides, half, rows * PATCH, height
        )
        held = (count * width, all_ch)
        count -= 2
        (current,) = call(
            kernel,
            18 * count * width * all_ch * own * (2 if extra else 1),
            [*got, kernels[layer], *extra],
            [(count * width, own * (2 if extra else 1))],
            [held],
        )
    return current.reshape(1, count, width, own)


def body(qkv, out_weight, lift_weight, conv_weight):
    if fits_kernels(qkv, lift_weight, conv_weight):
        return body_by_kernels(qkv, out_weight, lift_weight, conv_weight)
    rows, heads = qkv.shape[1], qkv.shape[4]
    lines, sides = lax.axis_size("blk"), lax.axis_size("uly")
    side = lax.axis_index("uly")
    latent_ch = lift_weight.shape[0]
    own = conv_weight.shape[3]
    reach = -(-LAYERS // PATCH)
    lifts = gathered(lift_weight, side)
    folded = jnp.einsum(
        "abdc,ec->abde", conv_weight[0], lifts, preferred_element_type=jnp.float32
    )
    folded = ordered(spread(folded.astype(jnp.bfloat16), "uly"), side)
    folded = jnp.transpose(folded, (1, 2, 0, 3, 4)).reshape(3, 3, sides * own, latent_ch)
    powers = lines & (lines - 1) == 0 and sides & (sides - 1) == 0
    if powers and heads % (lines * sides) == 0:
        patches = window_by_swaps(qkv, out_weight, reach)
    else:
        patches = window_by_gathers(qkv, out_weight, reach)
    height = lines * rows * PATCH
    margin = LAYERS - 1
    start = lax.axis_index("blk") * rows * PATCH
    latent = unfold_patches(patches, latent_ch)
    spare = reach * PATCH - LAYERS
    latent = latent[:, spare : latent.shape[1] - spare]
    current = activate(convolve(latent, folded), start - margin, height)
    for layer in range(1, LAYERS):
        margin -= 1
        kernels = conv_weight[layer]
        if layer > 1:
            current = gathered(current, side)
        current = activate(convolve(current, kernels), start - margin, height)
    return current


def solution(mesh):
    in_specs = (
        P("grp", "blk", "uly", None, None, None),
        P(),
        P(None, "uly"),
        P(None, None, None, "uly", None),
    )
    out_specs = P("grp", "blk", None, "uly")
    return jax.shard_map(
        body, mesh=mesh, in_specs=in_specs, out_specs=out_specs, check_vma=False
    )
```

```python
import functools
import math

import jax
import jax.numpy as jnp
from jax import lax
from jax.experimental import pallas as pl
from jax.experimental.pallas import tpu as pltpu
from jax.sharding import PartitionSpec as P


PATCH = 2
LAYERS = 4
GRANT = 8 * 2**20
SHARED = 2


def swap(pieces, axis):
    count = lax.axis_size(axis)
    got = [pieces[0]]
    for step in range(1, len(pieces)):
        got.append(lax.ppermute(pieces[step], axis, [(i, i ^ step) for i in range(count)]))
    return got


def spread(piece, axis):
    return swap([piece] * lax.axis_size(axis), axis)


def cut(array, start, size, axis):
    return lax.dynamic_slice_in_dim(array, start, size, axis=axis)


def attend(queries, keys, values):
    scale = 1.0 / queries.shape[-1] ** 0.5
    scores = jnp.einsum("hqd,hkd->hqk", queries, keys, preferred_element_type=jnp.float32) * scale
    weights = jnp.exp(scores - jnp.max(scores, axis=2, keepdims=True))
    totals = jnp.sum(weights, axis=2)
    mixed = jnp.einsum(
        "hqk,hkd->hqd", weights.astype(jnp.bfloat16), values, preferred_element_type=jnp.float32
    )
    return (mixed / totals[:, :, None]).astype(jnp.bfloat16)


def ordered(blocks, me):
    stacked = jnp.stack(blocks)
    return jnp.concatenate(
        [cut(stacked, me ^ place, 1, 0) for place in range(len(blocks))], axis=0
    )


def gathered(piece, side):
    blocks = ordered(spread(piece, "uly"), side)
    blocks = jnp.moveaxis(blocks, 0, -2)
    return blocks.reshape(piece.shape[:-1] + (-1,))


def window_by_swaps(qkv, out_weight, reach):
    frames, rows, cols, _, heads, size = qkv.shape
    lines, sides = lax.axis_size("blk"), lax.axis_size("uly")
    line, side = lax.axis_index("blk"), lax.axis_index("uly")
    group, share = heads // sides, heads // sides // lines
    got = swap([cut(qkv, (side ^ s) * group, group, 4) for s in range(sides)], "uly")
    grouped = jnp.stack(got, axis=3)
    grouped = jnp.transpose(grouped, (4, 5, 0, 1, 3, 2, 6))
    got = swap([cut(grouped, (line ^ t) * share, share, 1) for t in range(lines)], "blk")
    shared = ordered(got, line)
    shared = jnp.transpose(shared, (1, 2, 3, 0, 4, 5, 6, 7))
    flat = shared.reshape(3, share, -1, size)
    attended = attend(flat[0], flat[1], flat[2])
    attended = attended.reshape(share, frames, lines * rows, sides * cols, size)
    attended = jnp.transpose(attended, (1, 2, 3, 0, 4)).reshape(
        frames, lines * rows, sides * cols, share * size
    )
    padded = jnp.pad(attended, ((0, 0), (reach, reach), (0, 0), (0, 0)))
    got = swap([cut(padded, (line ^ t) * rows, rows + 2 * reach, 1) for t in range(lines)], "blk")
    partial = 0.0
    for t in range(lines):
        weight = cut(out_weight, ((side * lines) + (line ^ t)) * share * size, share * size, 0)
        partial = partial + jnp.einsum(
            "frcw,wp->frcp", got[t], weight, preferred_element_type=jnp.float32
        )
    partial = partial.astype(jnp.bfloat16)
    got = spread(partial, "uly")
    blocks = []
    for place in range(sides):
        total = 0.0
        for s in range(sides):
            at = (place ^ s) * cols
            total = total + got[s][:, :, at : at + cols].astype(jnp.float32)
        blocks.append(total.astype(jnp.bfloat16))
    patches = ordered(blocks, side)
    patches = jnp.transpose(patches, (1, 2, 0, 3, 4))
    return patches.reshape(frames, rows + 2 * reach, sides * cols, -1)


def window_by_gathers(qkv, out_weight, reach):
    frames, rows, cols, _, heads, size = qkv.shape
    grouped = lax.all_to_all(qkv, "blk", split_axis=4, concat_axis=1, tiled=True)
    flat = [
        lax.all_gather(grouped[:, :, :, which], "uly", axis=2, tiled=True) for which in (1, 2)
    ]
    flat = [grouped[:, :, :, 0]] + flat
    flat = [jnp.swapaxes(one.reshape(-1, one.shape[3], size), 0, 1) for one in flat]
    attended = jnp.swapaxes(attend(*flat), 0, 1)
    attended = attended.reshape(grouped.shape[:3] + grouped.shape[4:])
    restored = lax.all_to_all(attended, "blk", split_axis=1, concat_axis=3, tiled=True)
    patches = jnp.einsum(
        "frcw,wp->frcp",
        restored.reshape(frames, rows, cols, heads * size),
        out_weight,
        preferred_element_type=jnp.float32,
    ).astype(jnp.bfloat16)
    patches = lax.all_gather(patches, "uly", axis=2, tiled=True)
    patches = lax.all_gather(patches, "blk", axis=1, tiled=True)
    padded = jnp.pad(patches, ((0, 0), (reach, reach), (0, 0), (0, 0)))
    return cut(padded, lax.axis_index("blk") * rows, rows + 2 * reach, 1)


def unfold_patches(piece, latent_ch):
    frames, rows, cols = (piece.shape[0], piece.shape[1], piece.shape[2])
    parts = piece.reshape(frames, rows, cols, PATCH, PATCH, latent_ch)
    parts = jnp.transpose(parts, (0, 1, 3, 2, 4, 5))
    return parts.reshape(frames, rows * PATCH, cols * PATCH, latent_ch)


def convolve(current, kernels):
    return lax.conv_general_dilated(
        current,
        kernels,
        (1, 1),
        ((0, 0), (1, 1)),
        dimension_numbers=("NHWC", "HWOI", "NHWC"),
        preferred_element_type=jnp.float32,
    )


def activate(summed, first, height):
    rows = first + lax.broadcasted_iota(jnp.int32, summed.shape, 1)
    inside = (rows >= 0) & (rows < height)
    return jnp.where(inside, jax.nn.silu(summed), 0.0).astype(jnp.bfloat16)


def dot(left, right):
    return jnp.dot(left, right, preferred_element_type=jnp.float32)


def dot_rows(left, right):
    return lax.dot_general(
        left, right, (((1,), (1,)), ((), ())), preferred_element_type=jnp.float32
    )


def picked(source, count):
    rows = source.shape[0]
    places = lax.broadcasted_iota(jnp.int32, (rows, count), 1)
    return jnp.where(places == source, 1.0, 0.0).astype(jnp.bfloat16)


def line_of(rows):
    return lax.broadcasted_iota(jnp.int32, (rows, 1), 0)


def bits(number):
    return number.bit_length() - 1


def call(kernel, flops, inputs, outputs, scratch=(), far=()):
    near = pl.BlockSpec(memory_space=pltpu.VMEM)
    kept = pl.BlockSpec(memory_space=pltpu.HBM)
    moved = sum(one.size for one in inputs) + sum(math.prod(shape) for shape in outputs)
    return pl.pallas_call(
        kernel,
        out_shape=[jax.ShapeDtypeStruct(shape, jnp.bfloat16) for shape in outputs],
        in_specs=[kept if place in far else near for place in range(len(inputs))],
        out_specs=[near] * len(outputs),
        scratch_shapes=[
            pltpu.VMEM(one, jnp.bfloat16) if isinstance(one, tuple) else one for one in scratch
        ],
        compiler_params=pltpu.CompilerParams(vmem_limit_bytes=GRANT),
        cost_estimate=pl.CostEstimate(
            flops=flops, transcendentals=0, bytes_accessed=2 * moved
        ),
    )(*[
        pltpu.with_memory_space_constraint(one, pltpu.HBM) if place in far else one
        for place, one in enumerate(inputs)
    ])


def pack_kernel(sides, flat, lift, *refs):
    out, sems = refs[:sides], refs[sides]
    group, count = out[0].shape[1], flat.shape[0]
    side = lax.axis_index("uly")
    copies = []
    for s in reversed(range(sides)):
        heads = pl.ds(pl.multiple_of((side ^ s) * group, group), group)
        for place, source, target in (
            (s, flat.at[:, heads], out[s].at[pl.ds(0, count)]),
            (sides + s, lift, out[s].at[pl.ds(count, lift.shape[0])]),
        ):
            copies.append(pltpu.make_async_copy(source, target, sems.at[place]))
    for copy in copies:
        copy.start()
    for copy in copies:
        copy.wait()


def load_kernel(layers, kernels, *refs):
    out, sems = refs[:-1], refs[-1]
    sources = [kernels.at[layer] for layer in layers]
    parts = len(out) - len(layers)
    for place in range(parts):
        part = out[-1].shape[3]
        at = (lax.axis_index("grp") * parts + place) * part
        sources.append(kernels.at[SHARED, :, :, :, pl.ds(pl.multiple_of(at, part), part)])
    copies = [
        pltpu.make_async_copy(sources[place], out[place], sems.at[place])
        for place in reversed(range(len(sources)))
    ]
    for copy in copies:
        copy.start()
    for copy in copies:
        copy.wait()


def join_kernel(*refs):
    parts, out = refs[:-1], refs[-1]
    size, each = parts[0].shape[3], len(parts) // 2
    group = lax.axis_index("grp")
    for place, part in enumerate(parts):
        owner = group if place < each else 1 - group
        at = pl.multiple_of((owner * each + place % each) * size, size)
        out[:, :, :, pl.ds(at, size)] = part[...]


def regroup_kernel(sides, lines, tokens, *refs):
    pieces, out, held = refs[:sides], refs[sides : sides + lines], refs[-1]
    _, group, size = pieces[0].shape
    flat = jnp.concatenate(
        [
            piece[: 3 * tokens]
            .reshape(tokens, 3, group, size)[:, which]
            .astype(jnp.float32)
            .reshape(tokens * group, size)
            for piece in pieces
            for which in range(3)
        ],
        axis=1,
    ).astype(jnp.bfloat16)
    at = line_of(group * tokens)
    source = ((at & (tokens - 1)) << bits(group)) + (at >> bits(tokens))
    held[...] = dot(picked(source, tokens * group), flat).astype(jnp.bfloat16)
    line = lax.axis_index("blk")
    span = group * tokens // lines
    for t in range(lines):
        out[t][...] = held[pl.ds(pl.multiple_of((line ^ t) * span, span), span), :]


def attention_kernel(sides, lines, share, *refs):
    pieces, out, held = refs[:lines], refs[lines : 2 * lines], refs[-1]
    tokens = pieces[0].shape[0] // share
    size = pieces[0].shape[1] // (3 * sides)
    block = sides * tokens
    scale = 1.0 / size**0.5
    line = lax.axis_index("blk")
    empty = jnp.zeros((block, held.shape[1]), jnp.bfloat16)
    held[:block] = empty
    held[held.shape[0] - block :] = empty
    wide = [piece[...].astype(jnp.float32) for piece in pieces]
    for head in range(share):
        q, k, v = [
            jnp.concatenate(
                [
                    piece[
                        head * tokens : (head + 1) * tokens,
                        (s * 3 + which) * size : (s * 3 + which + 1) * size,
                    ]
                    for piece in wide
                    for s in range(sides)
                ],
                axis=0,
            ).astype(jnp.bfloat16)
            for which in range(3)
        ]
        scores = dot_rows(q, k) * scale
        weights = jnp.exp(scores - jnp.max(scores, axis=1, keepdims=True))
        totals = jnp.sum(weights, axis=1, keepdims=True)
        mixed = (dot(weights.astype(jnp.bfloat16), v) / totals).astype(jnp.bfloat16)
        for t in range(lines):
            at = pl.multiple_of(((line ^ t) + 1) * block, block)
            held[pl.ds(at, block), head * size : (head + 1) * size] = mixed[
                t * block : (t + 1) * block
            ]
    for t in range(lines):
        at = pl.multiple_of((line ^ t) * block, block)
        out[t][...] = held[pl.ds(at, 3 * block), :]


def project_kernel(lines, *refs):
    pieces, weights, out = refs[:lines], refs[lines], refs[-1]
    line, side = lax.axis_index("blk"), lax.axis_index("uly")
    depth = pieces[0].shape[1]
    summed = 0.0
    for t in range(lines):
        at = pl.multiple_of((side * lines + (line ^ t)) * depth, depth)
        summed = summed + dot(pieces[t][...], weights[pl.ds(at, depth), :])
    out[...] = summed.astype(jnp.bfloat16)


def fold_kernel(sides, skip, *refs):
    pieces, kernels, out, held = refs[:sides], refs[sides], refs[-2], refs[-1]
    latent, own = out.shape[0] // 9, out.shape[1]
    side = lax.axis_index("uly")
    for s in range(sides):
        lift = pieces[s][skip:].astype(jnp.float32).reshape(latent, own).astype(jnp.bfloat16)
        held[:, pl.ds(pl.multiple_of((side ^ s) * own, own), own)] = lift
    lift = held[...]
    for tap in range(9):
        product = dot_rows(lift, kernels[tap // 3, tap % 3])
        out[tap * latent : (tap + 1) * latent, :] = product.astype(jnp.bfloat16)


def activated(summed, first, width, height):
    row = first + (line_of(summed.shape[0]) >> bits(width))
    inside = (row >= 0) & (row < height)
    return jnp.where(inside, jax.nn.silu(summed), 0.0)


def shifted(summed, half, own):
    size = summed.shape[0]
    summed = summed.reshape(size // (2 * half), 2, half, 3 * own)

    def part(parity, tap):
        return summed[:, parity, :, tap * own : (tap + 1) * own].reshape(size // 2, own)

    column = line_of(size // 2) & (half - 1)
    before = jnp.where(column == 0, 0.0, pltpu.roll(part(1, 0), 1, 0))
    after = jnp.where(column == half - 1, 0.0, pltpu.roll(part(0, 2), size // 2 - 1, 0))
    even = before + part(0, 1) + part(1, 2)
    odd = part(0, 0) + part(1, 1) + after
    both = [one.reshape(size // (2 * half), 1, half, own) for one in (even, odd)]
    return jnp.concatenate(both, axis=1).reshape(size, own)


def convolved(current, kernels, half):
    width = 2 * half
    own = kernels.shape[2]
    size = current.shape[0] - 2 * width
    summed = 0.0
    for above in range(3):
        taps = kernels[above].reshape(3 * own, kernels.shape[3])
        summed = summed + dot_rows(current[above * width : above * width + size], taps)
    return shifted(summed, half, own)


def taps_kernel(sides, *refs):
    folded, even_taps, odd_taps = refs[:sides], refs[-2], refs[-1]
    side = lax.axis_index("uly")
    latent = folded[0].shape[0] // 9
    own = folded[0].shape[1]
    empty = jnp.zeros((latent, sides * own), jnp.bfloat16)
    for above in range(3):
        even_taps[above, 2 * latent : 3 * latent, :] = empty
        odd_taps[above, 3 * latent :, :] = empty
        for s in range(sides):
            lanes = pl.ds(pl.multiple_of((side ^ s) * own, own), own)
            for beside in range(3):
                at = (above * 3 + beside) * latent
                taps = folded[s][at : at + latent, :]
                to = (3, 0, 1)[beside] * latent
                even_taps[above, to : to + latent, lanes] = taps
                odd_taps[above, beside * latent : (beside + 1) * latent, lanes] = taps


def first_kernel(sides, rows, cols, height, *refs):
    partials, (even_taps, odd_taps, kernels, out, held) = refs[:sides], refs[sides:]
    kernels = kernels.at[1]
    side, line = lax.axis_index("uly"), lax.axis_index("blk")
    half = sides * cols
    count = partials[0].shape[0]
    latent = even_taps.shape[1] // 4
    at = line_of(count)
    column = at & (cols - 1)
    group = (at >> bits(cols)) & (sides - 1)
    row = (at >> bits(half)) & (rows - 1)
    block = at >> bits(half * rows)
    total = 0.0
    for s in range(sides):
        source = (((block << bits(sides)) + (group ^ side ^ s)) << bits(rows)) + row
        source = (source << bits(cols)) + column
        total = total + dot(picked(source, count), partials[s][...])
    total = total.astype(jnp.bfloat16).astype(jnp.float32)
    wide = 2 * latent
    lines = [
        total[:, i * wide : (i + 1) * wide].reshape(count // half, 1, half, wide) for i in range(2)
    ]
    latents = jnp.concatenate(lines, axis=1).reshape(2 * count, wide)
    place = line_of(2 * count) & (half - 1)
    before = jnp.where(place == 0, 0.0, pltpu.roll(latents, 1, 0))
    after = jnp.where(place == half - 1, 0.0, pltpu.roll(latents, 2 * count - 1, 0))
    start = line * rows * PATCH - (LAYERS - 1)
    size = 2 * count - 2 * half
    for parity, (other, taps) in enumerate(((before, even_taps), (after, odd_taps))):
        current = jnp.concatenate([latents, other], axis=1).astype(jnp.bfloat16)
        summed = 0.0
        for above in range(3):
            summed = summed + dot(current[above * half : above * half + size], taps[above])
        summed = activated(summed, start, half, height).astype(jnp.bfloat16)
        for row in range(size // half):
            at = (2 * row + parity) * half
            held[at : at + half, :] = summed[row * half : (row + 1) * half]
    summed = convolved(held, kernels, half)
    out[...] = activated(summed, start + 1, 2 * half, height).astype(jnp.bfloat16)


def layer_kernel(layer, pieces_in, sides, half, step, height, *refs):
    pieces = refs[:pieces_in]
    kernels = [refs[pieces_in].at[layer], *refs[pieces_in + 1 : -2]]
    out, held = refs[-2:]
    side, line = lax.axis_index("uly"), lax.axis_index("blk")
    own = kernels[0].shape[2]
    for s in range(pieces_in):
        for place in range(pieces[s].shape[1] // own):
            to = side ^ s ^ (place * (sides // 2))
            lanes = pl.ds(pl.multiple_of(to * own, own), own)
            held[:, lanes] = pieces[s][:, place * own : (place + 1) * own]
    width = 2 * half
    first = line * step + layer + 1 - LAYERS
    for place, taps in enumerate(kernels):
        summed = convolved(held, taps, half)
        result = activated(summed, first, width, height).astype(jnp.bfloat16)
        if layer == LAYERS - 1:
            at = line_of(result.shape[0])
            column = at & (width - 1)
            source = (at - column) + ((column & 1) << bits(half)) + (column >> 1)
            result = dot(picked(source, result.shape[0]), result).astype(jnp.bfloat16)
        out[:, place * own : (place + 1) * own] = result


def fits_kernels(qkv, lift_weight, conv_weight):
    frames, rows, cols, _, heads, size = qkv.shape
    lines, sides = lax.axis_size("blk"), lax.axis_size("uly")
    powers = all(n & (n - 1) == 0 for n in (lines, sides, rows, cols, heads))
    return (
        powers
        and lax.axis_size("grp") == 2
        and sides >= 4
        and frames == 1
        and rows * PATCH == LAYERS
        and heads % (lines * sides) == 0
        and rows * cols % 8 == 0
        and rows * cols * heads // (lines * sides) % 16 == 0
        and rows * cols * sides % 32 == 0
        and sides * cols % 16 == 0
        and heads // sides % 8 == 0
        and size % 128 == 0
        and conv_weight.shape[3] % 128 == 0
        and lift_weight.size % (heads // sides * size) == 0
        and conv_weight.shape[3] == size
        and lift_weight.shape[0] * 2 % 128 == 0
    )


def body_by_kernels(qkv, out_weight, lift_weight, conv_weight):
    _, rows, cols, _, heads, size = qkv.shape
    lines, sides = lax.axis_size("blk"), lax.axis_size("uly")
    group, share = heads // sides, heads // sides // lines
    latent, own = lift_weight.shape
    tokens, half = rows * cols, sides * cols
    height = lines * rows * PATCH
    width, all_ch = 2 * half, sides * own
    pieces = call(
        functools.partial(pack_kernel, sides),
        0,
        [qkv.reshape(3 * tokens, heads, size), lift_weight.reshape(-1, group, size)],
        [(3 * tokens + lift_weight.size // (group * size), group, size)] * sides,
        [pltpu.SemaphoreType.DMA((2 * sides,))],
        far=(0, 1),
    )
    got = swap(pieces, "uly")

    def load(layers, extra):
        shapes = [conv_weight.shape[1:]] * len(layers) + extra
        return call(
            functools.partial(load_kernel, layers),
            10**8,
            [conv_weight],
            shapes,
            [pltpu.SemaphoreType.DMA((len(shapes),))],
            far=(0,),
        )

    far = sides // 2
    across = [(i, i ^ far) for i in range(sides)]
    kernels = {}
    quarter = conv_weight.shape[1:4] + (all_ch // 4,)
    kernels[0], *parts = load([0], [quarter] * 2)
    others = []
    for place in range(2):
        parts[place] = lax.ppermute(parts[place], "uly", across)
        others.append(lax.ppermute(parts[place], "grp", [(0, 1), (1, 0)]))
    (mate,) = call(join_kernel, 10**7, parts + others, [conv_weight.shape[1:]])
    mates = {SHARED: [mate]}
    span = (share * tokens, sides * 3 * size)
    shared = call(
        functools.partial(regroup_kernel, sides, lines, tokens),
        2 * (group * tokens) ** 2 * span[1],
        got,
        [span] * lines,
        [(group * tokens, span[1])],
    )
    (folded,) = call(
        functools.partial(fold_kernel, sides, 3 * tokens),
        2 * 9 * latent * all_ch * own,
        [*got, kernels[0]],
        [(9 * latent, own)],
        [(latent, all_ch)],
    )
    got = swap(shared, "blk")
    beyond = lax.ppermute(folded, "uly", across)
    folded = swap([folded] * far, "uly") + swap([beyond] * far, "uly")
    (*taps,) = call(
        functools.partial(taps_kernel, sides), 10**7, folded, [(3, 4 * latent, all_ch)] * 2
    )
    block = sides * tokens
    windows = call(
        functools.partial(attention_kernel, sides, lines, share),
        4 * share * size * (lines * block) ** 2,
        got,
        [(3 * block, share * size)] * lines,
        [((lines + 2) * block, share * size)],
    )
    got = swap(windows, "blk")
    (partial,) = call(
        functools.partial(project_kernel, lines),
        2 * 3 * block * lines * share * size * out_weight.shape[1],
        [*got, out_weight],
        [(3 * block, out_weight.shape[1])],
    )
    got = spread(partial, "uly")
    count = (rows + 2) * PATCH
    (current,) = call(
        functools.partial(first_kernel, sides, rows, cols, height),
        18 * count * width * all_ch * own,
        [*got, *taps, conv_weight],
        [(count * width, own)],
        [((count + 2) * width, all_ch)],
    )
    for layer in range(2, LAYERS):
        whole = current.shape[1] == own
        got = swap([current] * (sides if whole else far), "uly")
        extra = mates.get(layer, [])
        kernel = functools.partial(
            layer_kernel, layer, len(got), sides, half, rows * PATCH, height
        )
        held = (count * width, all_ch)
        count -= 2
        (current,) = call(
            kernel,
            18 * count * width * all_ch * own * (2 if extra else 1),
            [*got, conv_weight, *extra],
            [(count * width, own * (2 if extra else 1))],
            [held],
        )
    return current.reshape(1, count, width, own)


def body(qkv, out_weight, lift_weight, conv_weight):
    if fits_kernels(qkv, lift_weight, conv_weight):
        return body_by_kernels(qkv, out_weight, lift_weight, conv_weight)
    rows, heads = qkv.shape[1], qkv.shape[4]
    lines, sides = lax.axis_size("blk"), lax.axis_size("uly")
    side = lax.axis_index("uly")
    latent_ch = lift_weight.shape[0]
    own = conv_weight.shape[3]
    reach = -(-LAYERS // PATCH)
    lifts = gathered(lift_weight, side)
    folded = jnp.einsum(
        "abdc,ec->abde", conv_weight[0], lifts, preferred_element_type=jnp.float32
    )
    folded = ordered(spread(folded.astype(jnp.bfloat16), "uly"), side)
    folded = jnp.transpose(folded, (1, 2, 0, 3, 4)).reshape(3, 3, sides * own, latent_ch)
    powers = lines & (lines - 1) == 0 and sides & (sides - 1) == 0
    if powers and heads % (lines * sides) == 0:
        patches = window_by_swaps(qkv, out_weight, reach)
    else:
        patches = window_by_gathers(qkv, out_weight, reach)
    height = lines * rows * PATCH
    margin = LAYERS - 1
    start = lax.axis_index("blk") * rows * PATCH
    latent = unfold_patches(patches, latent_ch)
    spare = reach * PATCH - LAYERS
    latent = latent[:, spare : latent.shape[1] - spare]
    current = activate(convolve(latent, folded), start - margin, height)
    for layer in range(1, LAYERS):
        margin -= 1
        kernels = conv_weight[layer]
        if layer > 1:
            current = gathered(current, side)
        current = activate(convolve(current, kernels), start - margin, height)
    return current


def solution(mesh):
    in_specs = (
        P("grp", "blk", "uly", None, None, None),
        P(),
        P(None, "uly"),
        P(None, None, None, "uly", None),
    )
    out_specs = P("grp", "blk", None, "uly")
    return jax.shard_map(
        body, mesh=mesh, in_specs=in_specs, out_specs=out_specs, check_vma=False
    )
```

```python
import functools
import math

import jax
import jax.numpy as jnp
from jax import lax
from jax.experimental import pallas as pl
from jax.experimental.pallas import tpu as pltpu
from jax.sharding import PartitionSpec as P


PATCH = 2
LAYERS = 4
GRANT = 8 * 2**20
SHARED = 2


def swap(pieces, axis):
    count = lax.axis_size(axis)
    got = [pieces[0]]
    for step in range(1, len(pieces)):
        got.append(lax.ppermute(pieces[step], axis, [(i, i ^ step) for i in range(count)]))
    return got


def spread(piece, axis):
    return swap([piece] * lax.axis_size(axis), axis)


def cut(array, start, size, axis):
    return lax.dynamic_slice_in_dim(array, start, size, axis=axis)


def attend(queries, keys, values):
    scale = 1.0 / queries.shape[-1] ** 0.5
    scores = jnp.einsum("hqd,hkd->hqk", queries, keys, preferred_element_type=jnp.float32) * scale
    weights = jnp.exp(scores - jnp.max(scores, axis=2, keepdims=True))
    totals = jnp.sum(weights, axis=2)
    mixed = jnp.einsum(
        "hqk,hkd->hqd", weights.astype(jnp.bfloat16), values, preferred_element_type=jnp.float32
    )
    return (mixed / totals[:, :, None]).astype(jnp.bfloat16)


def ordered(blocks, me):
    stacked = jnp.stack(blocks)
    return jnp.concatenate(
        [cut(stacked, me ^ place, 1, 0) for place in range(len(blocks))], axis=0
    )


def gathered(piece, side):
    blocks = ordered(spread(piece, "uly"), side)
    blocks = jnp.moveaxis(blocks, 0, -2)
    return blocks.reshape(piece.shape[:-1] + (-1,))


def window_by_swaps(qkv, out_weight, reach):
    frames, rows, cols, _, heads, size = qkv.shape
    lines, sides = lax.axis_size("blk"), lax.axis_size("uly")
    line, side = lax.axis_index("blk"), lax.axis_index("uly")
    group, share = heads // sides, heads // sides // lines
    got = swap([cut(qkv, (side ^ s) * group, group, 4) for s in range(sides)], "uly")
    grouped = jnp.stack(got, axis=3)
    grouped = jnp.transpose(grouped, (4, 5, 0, 1, 3, 2, 6))
    got = swap([cut(grouped, (line ^ t) * share, share, 1) for t in range(lines)], "blk")
    shared = ordered(got, line)
    shared = jnp.transpose(shared, (1, 2, 3, 0, 4, 5, 6, 7))
    flat = shared.reshape(3, share, -1, size)
    attended = attend(flat[0], flat[1], flat[2])
    attended = attended.reshape(share, frames, lines * rows, sides * cols, size)
    attended = jnp.transpose(attended, (1, 2, 3, 0, 4)).reshape(
        frames, lines * rows, sides * cols, share * size
    )
    padded = jnp.pad(attended, ((0, 0), (reach, reach), (0, 0), (0, 0)))
    got = swap([cut(padded, (line ^ t) * rows, rows + 2 * reach, 1) for t in range(lines)], "blk")
    partial = 0.0
    for t in range(lines):
        weight = cut(out_weight, ((side * lines) + (line ^ t)) * share * size, share * size, 0)
        partial = partial + jnp.einsum(
            "frcw,wp->frcp", got[t], weight, preferred_element_type=jnp.float32
        )
    partial = partial.astype(jnp.bfloat16)
    got = spread(partial, "uly")
    blocks = []
    for place in range(sides):
        total = 0.0
        for s in range(sides):
            at = (place ^ s) * cols
            total = total + got[s][:, :, at : at + cols].astype(jnp.float32)
        blocks.append(total.astype(jnp.bfloat16))
    patches = ordered(blocks, side)
    patches = jnp.transpose(patches, (1, 2, 0, 3, 4))
    return patches.reshape(frames, rows + 2 * reach, sides * cols, -1)


def window_by_gathers(qkv, out_weight, reach):
    frames, rows, cols, _, heads, size = qkv.shape
    grouped = lax.all_to_all(qkv, "blk", split_axis=4, concat_axis=1, tiled=True)
    flat = [
        lax.all_gather(grouped[:, :, :, which], "uly", axis=2, tiled=True) for which in (1, 2)
    ]
    flat = [grouped[:, :, :, 0]] + flat
    flat = [jnp.swapaxes(one.reshape(-1, one.shape[3], size), 0, 1) for one in flat]
    attended = jnp.swapaxes(attend(*flat), 0, 1)
    attended = attended.reshape(grouped.shape[:3] + grouped.shape[4:])
    restored = lax.all_to_all(attended, "blk", split_axis=1, concat_axis=3, tiled=True)
    patches = jnp.einsum(
        "frcw,wp->frcp",
        restored.reshape(frames, rows, cols, heads * size),
        out_weight,
        preferred_element_type=jnp.float32,
    ).astype(jnp.bfloat16)
    patches = lax.all_gather(patches, "uly", axis=2, tiled=True)
    patches = lax.all_gather(patches, "blk", axis=1, tiled=True)
    padded = jnp.pad(patches, ((0, 0), (reach, reach), (0, 0), (0, 0)))
    return cut(padded, lax.axis_index("blk") * rows, rows + 2 * reach, 1)


def unfold_patches(piece, latent_ch):
    frames, rows, cols = (piece.shape[0], piece.shape[1], piece.shape[2])
    parts = piece.reshape(frames, rows, cols, PATCH, PATCH, latent_ch)
    parts = jnp.transpose(parts, (0, 1, 3, 2, 4, 5))
    return parts.reshape(frames, rows * PATCH, cols * PATCH, latent_ch)


def convolve(current, kernels):
    return lax.conv_general_dilated(
        current,
        kernels,
        (1, 1),
        ((0, 0), (1, 1)),
        dimension_numbers=("NHWC", "HWOI", "NHWC"),
        preferred_element_type=jnp.float32,
    )


def activate(summed, first, height):
    rows = first + lax.broadcasted_iota(jnp.int32, summed.shape, 1)
    inside = (rows >= 0) & (rows < height)
    return jnp.where(inside, jax.nn.silu(summed), 0.0).astype(jnp.bfloat16)


def dot(left, right):
    return jnp.dot(left, right, preferred_element_type=jnp.float32)


def dot_rows(left, right):
    return lax.dot_general(
        left, right, (((1,), (1,)), ((), ())), preferred_element_type=jnp.float32
    )


def picked(source, count):
    rows = source.shape[0]
    places = lax.broadcasted_iota(jnp.int32, (rows, count), 1)
    return jnp.where(places == source, 1.0, 0.0).astype(jnp.bfloat16)


def line_of(rows):
    return lax.broadcasted_iota(jnp.int32, (rows, 1), 0)


def bits(number):
    return number.bit_length() - 1


def call(kernel, flops, inputs, outputs, scratch=(), far=(), sums=()):
    near = pl.BlockSpec(memory_space=pltpu.VMEM)
    kept = pl.BlockSpec(memory_space=pltpu.HBM)
    moved = sum(one.size for one in inputs) + sum(math.prod(shape) for shape in outputs)
    return pl.pallas_call(
        kernel,
        out_shape=[
            jax.ShapeDtypeStruct(shape, jnp.float32 if place in sums else jnp.bfloat16)
            for place, shape in enumerate(outputs)
        ],
        in_specs=[kept if place in far else near for place in range(len(inputs))],
        out_specs=[near] * len(outputs),
        scratch_shapes=[
            pltpu.VMEM(one, jnp.bfloat16) if isinstance(one, tuple) else one for one in scratch
        ],
        compiler_params=pltpu.CompilerParams(vmem_limit_bytes=GRANT),
        cost_estimate=pl.CostEstimate(
            flops=flops, transcendentals=0, bytes_accessed=2 * moved
        ),
    )(*[
        pltpu.with_memory_space_constraint(one, pltpu.HBM) if place in far else one
        for place, one in enumerate(inputs)
    ])


def pack_kernel(sides, flat, lift, *refs):
    out, sems = refs[:sides], refs[sides]
    group, count = out[0].shape[1], flat.shape[0]
    side = lax.axis_index("uly")
    copies = []
    for s in reversed(range(sides)):
        heads = pl.ds(pl.multiple_of((side ^ s) * group, group), group)
        for place, source, target in (
            (s, flat.at[:, heads], out[s].at[pl.ds(0, count)]),
            (sides + s, lift, out[s].at[pl.ds(count, lift.shape[0])]),
        ):
            copies.append(pltpu.make_async_copy(source, target, sems.at[place]))
    for copy in copies:
        copy.start()
    for copy in copies:
        copy.wait()


def load_kernel(layers, kernels, *refs):
    out, sems = refs[:-1], refs[-1]
    sources = [kernels.at[layer] for layer in layers]
    parts = len(out) - len(layers)
    for place in range(parts):
        part = out[-1].shape[3]
        at = (lax.axis_index("grp") * parts + place) * part
        sources.append(kernels.at[SHARED, :, :, :, pl.ds(pl.multiple_of(at, part), part)])
    copies = [
        pltpu.make_async_copy(sources[place], out[place], sems.at[place])
        for place in reversed(range(len(sources)))
    ]
    for copy in copies:
        copy.start()
    for copy in copies:
        copy.wait()


def join_kernel(*refs):
    parts, out = refs[:-1], refs[-1]
    size, each = parts[0].shape[3], len(parts) // 2
    group = lax.axis_index("grp")
    for place, part in enumerate(parts):
        owner = group if place < each else 1 - group
        at = pl.multiple_of((owner * each + place % each) * size, size)
        out[:, :, :, pl.ds(at, size)] = part[...]


def regroup_kernel(sides, lines, tokens, *refs):
    pieces, out, held = refs[:sides], refs[sides : sides + lines], refs[-1]
    _, group, size = pieces[0].shape
    flat = jnp.concatenate(
        [
            piece[: 3 * tokens]
            .reshape(tokens, 3, group, size)[:, which]
            .astype(jnp.float32)
            .reshape(tokens * group, size)
            for piece in pieces
            for which in range(3)
        ],
        axis=1,
    ).astype(jnp.bfloat16)
    at = line_of(group * tokens)
    source = ((at & (tokens - 1)) << bits(group)) + (at >> bits(tokens))
    held[...] = dot(picked(source, tokens * group), flat).astype(jnp.bfloat16)
    line = lax.axis_index("blk")
    span = group * tokens // lines
    for t in range(lines):
        out[t][...] = held[pl.ds(pl.multiple_of((line ^ t) * span, span), span), :]


def attention_kernel(sides, lines, share, *refs):
    pieces, out, held = refs[:lines], refs[lines : 2 * lines], refs[-1]
    tokens = pieces[0].shape[0] // share
    size = pieces[0].shape[1] // (3 * sides)
    block = sides * tokens
    scale = 1.0 / size**0.5
    line = lax.axis_index("blk")
    empty = jnp.zeros((block, held.shape[1]), jnp.bfloat16)
    held[:block] = empty
    held[held.shape[0] - block :] = empty
    wide = [piece[...].astype(jnp.float32) for piece in pieces]
    for head in range(share):
        q, k, v = [
            jnp.concatenate(
                [
                    piece[
                        head * tokens : (head + 1) * tokens,
                        (s * 3 + which) * size : (s * 3 + which + 1) * size,
                    ]
                    for piece in wide
                    for s in range(sides)
                ],
                axis=0,
            ).astype(jnp.bfloat16)
            for which in range(3)
        ]
        scores = dot_rows(q, k) * scale
        weights = jnp.exp(scores - jnp.max(scores, axis=1, keepdims=True))
        totals = jnp.sum(weights, axis=1, keepdims=True)
        mixed = (dot(weights.astype(jnp.bfloat16), v) / totals).astype(jnp.bfloat16)
        for t in range(lines):
            at = pl.multiple_of(((line ^ t) + 1) * block, block)
            held[pl.ds(at, block), head * size : (head + 1) * size] = mixed[
                t * block : (t + 1) * block
            ]
    for t in range(lines):
        at = pl.multiple_of((line ^ t) * block, block)
        out[t][...] = held[pl.ds(at, 3 * block), :]


def project_kernel(lines, *refs):
    pieces, weights, out = refs[:lines], refs[lines], refs[-1]
    line, side = lax.axis_index("blk"), lax.axis_index("uly")
    depth = pieces[0].shape[1]
    summed = 0.0
    for t in range(lines):
        at = pl.multiple_of((side * lines + (line ^ t)) * depth, depth)
        summed = summed + dot(pieces[t][...], weights[pl.ds(at, depth), :])
    out[...] = summed.astype(jnp.bfloat16)


def fold_kernel(sides, skip, *refs):
    pieces, kernels, out, held = refs[:sides], refs[sides], refs[-2], refs[-1]
    latent, own = out.shape[0] // 9, out.shape[1]
    side = lax.axis_index("uly")
    for s in range(sides):
        lift = pieces[s][skip:].astype(jnp.float32).reshape(latent, own).astype(jnp.bfloat16)
        held[:, pl.ds(pl.multiple_of((side ^ s) * own, own), own)] = lift
    lift = held[...]
    for tap in range(9):
        product = dot_rows(lift, kernels[tap // 3, tap % 3])
        out[tap * latent : (tap + 1) * latent, :] = product.astype(jnp.bfloat16)


def activated(summed, first, width, height):
    row = first + (line_of(summed.shape[0]) >> bits(width))
    inside = (row >= 0) & (row < height)
    return jnp.where(inside, jax.nn.silu(summed), 0.0)


def shifted(summed, half, own):
    size = summed.shape[0]
    summed = summed.reshape(size // (2 * half), 2, half, 3 * own)

    def part(parity, tap):
        return summed[:, parity, :, tap * own : (tap + 1) * own].reshape(size // 2, own)

    column = line_of(size // 2) & (half - 1)
    before = jnp.where(column == 0, 0.0, pltpu.roll(part(1, 0), 1, 0))
    after = jnp.where(column == half - 1, 0.0, pltpu.roll(part(0, 2), size // 2 - 1, 0))
    even = before + part(0, 1) + part(1, 2)
    odd = part(0, 0) + part(1, 1) + after
    both = [one.reshape(size // (2 * half), 1, half, own) for one in (even, odd)]
    return jnp.concatenate(both, axis=1).reshape(size, own)


def convolved(current, kernels, half):
    width = 2 * half
    size = current.shape[0] - 2 * width
    summed = 0.0
    for above in range(3):
        taps = kernels[above]
        taps = taps.reshape(-1, taps.shape[-1])
        summed = summed + dot_rows(current[above * width : above * width + size, :], taps)
    return summed


def taps_kernel(sides, *refs):
    folded, even_taps, odd_taps = refs[:sides], refs[-2], refs[-1]
    side = lax.axis_index("uly")
    latent = folded[0].shape[0] // 9
    own = folded[0].shape[1]
    empty = jnp.zeros((latent, sides * own), jnp.bfloat16)
    for above in range(3):
        even_taps[above, 2 * latent : 3 * latent, :] = empty
        odd_taps[above, 3 * latent :, :] = empty
        for s in range(sides):
            lanes = pl.ds(pl.multiple_of((side ^ s) * own, own), own)
            for beside in range(3):
                at = (above * 3 + beside) * latent
                taps = folded[s][at : at + latent, :]
                to = (3, 0, 1)[beside] * latent
                even_taps[above, to : to + latent, lanes] = taps
                odd_taps[above, beside * latent : (beside + 1) * latent, lanes] = taps


def first_kernel(sides, rows, cols, height, *refs):
    partials, (even_taps, odd_taps, kernels, out, held) = refs[:sides], refs[sides:]
    kernels = kernels.at[1]
    side, line = lax.axis_index("uly"), lax.axis_index("blk")
    half = sides * cols
    count = partials[0].shape[0]
    latent = even_taps.shape[1] // 4
    own = kernels.shape[2]
    at = line_of(count)
    column = at & (cols - 1)
    group = (at >> bits(cols)) & (sides - 1)
    row = (at >> bits(half)) & (rows - 1)
    block = at >> bits(half * rows)
    total = 0.0
    for s in range(sides):
        source = (((block << bits(sides)) + (group ^ side ^ s)) << bits(rows)) + row
        source = (source << bits(cols)) + column
        total = total + dot(picked(source, count), partials[s][...])
    total = total.astype(jnp.bfloat16).astype(jnp.float32)
    wide = 2 * latent
    lines = [
        total[:, i * wide : (i + 1) * wide].reshape(count // half, 1, half, wide) for i in range(2)
    ]
    latents = jnp.concatenate(lines, axis=1).reshape(2 * count, wide)
    place = line_of(2 * count) & (half - 1)
    before = jnp.where(place == 0, 0.0, pltpu.roll(latents, 1, 0))
    after = jnp.where(place == half - 1, 0.0, pltpu.roll(latents, 2 * count - 1, 0))
    start = line * rows * PATCH - (LAYERS - 1)
    size = 2 * count - 2 * half
    for parity, (other, taps) in enumerate(((before, even_taps), (after, odd_taps))):
        current = jnp.concatenate([latents, other], axis=1).astype(jnp.bfloat16)
        summed = 0.0
        for above in range(3):
            summed = summed + dot(current[above * half : above * half + size], taps[above])
        summed = activated(summed, start, half, height).astype(jnp.bfloat16)
        for row in range(size // half):
            at = (2 * row + parity) * half
            held[at : at + half, :] = summed[row * half : (row + 1) * half]
    summed = shifted(convolved(held, kernels, half), half, own)
    out[...] = activated(summed, start + 1, 2 * half, height).astype(jnp.bfloat16)


def layer_kernel(layer, pieces_in, half, step, height, *refs):
    pieces = refs[:pieces_in]
    kernels = [refs[pieces_in].at[layer], *refs[pieces_in + 1 : -2]]
    out, held = refs[-2:]
    side, line = lax.axis_index("uly"), lax.axis_index("blk")
    own = kernels[0].shape[2]
    for s in range(pieces_in):
        lanes = pl.ds(pl.multiple_of((side ^ s) * own, own), own)
        held[:, lanes] = pieces[s][...]
    first = line * step + layer + 1 - LAYERS
    for place, taps in enumerate(kernels):
        summed = shifted(convolved(held, taps, half), half, own)
        result = activated(summed, first, 2 * half, height).astype(jnp.bfloat16)
        out[:, place * own : (place + 1) * own] = result


def early_kernel(layer, sides, half, *refs):
    piece, kernels, total, later = refs[0], refs[1].at[layer], refs[2], refs[3:]
    side = lax.axis_index("uly")
    own = kernels.shape[2]

    def met(above, s):
        places = [side ^ s, side ^ s ^ (sides // 2)]
        lanes = [pl.ds(pl.multiple_of(place * own, own), own) for place in places]
        taps = [kernels[above, :, :, lane].reshape(3 * own, own) for lane in lanes]
        return jnp.concatenate(taps, axis=1)

    total[...] = convolved(piece, [met(above, 0) for above in range(3)], half)
    for s, out in enumerate(later, 1):
        for above in range(3):
            out[above] = met(above, s)


def last_kernel(layer, half, step, height, *refs):
    count = (len(refs) - 2) // 2
    total, pieces, kernels, out = refs[0], refs[1 : 1 + count], refs[1 + count : -1], refs[-1]
    summed = total[...]
    for piece, taps in zip(pieces, kernels):
        summed = summed + convolved(piece, taps, half)
    width = 2 * half
    first = lax.axis_index("blk") * step + layer + 1 - LAYERS
    summed = shifted(summed, half, summed.shape[1] // 3)
    result = activated(summed, first, width, height).astype(jnp.bfloat16)
    at = line_of(result.shape[0])
    column = at & (width - 1)
    source = (at - column) + ((column & 1) << bits(half)) + (column >> 1)
    out[...] = dot(picked(source, result.shape[0]), result).astype(jnp.bfloat16)


def fits_kernels(qkv, lift_weight, conv_weight):
    frames, rows, cols, _, heads, size = qkv.shape
    lines, sides = lax.axis_size("blk"), lax.axis_size("uly")
    powers = all(n & (n - 1) == 0 for n in (lines, sides, rows, cols, heads))
    return (
        powers
        and lax.axis_size("grp") == 2
        and sides >= 4
        and frames == 1
        and LAYERS == SHARED + 2
        and rows * PATCH == LAYERS
        and heads % (lines * sides) == 0
        and rows * cols % 8 == 0
        and rows * cols * heads // (lines * sides) % 16 == 0
        and rows * cols * sides % 32 == 0
        and sides * cols % 16 == 0
        and heads // sides % 8 == 0
        and size % 128 == 0
        and conv_weight.shape[3] % 128 == 0
        and lift_weight.size % (heads // sides * size) == 0
        and conv_weight.shape[3] == size
        and lift_weight.shape[0] * 2 % 128 == 0
    )


def body_by_kernels(qkv, out_weight, lift_weight, conv_weight):
    _, rows, cols, _, heads, size = qkv.shape
    lines, sides = lax.axis_size("blk"), lax.axis_size("uly")
    group, share = heads // sides, heads // sides // lines
    latent, own = lift_weight.shape
    tokens, half = rows * cols, sides * cols
    height = lines * rows * PATCH
    width, all_ch = 2 * half, sides * own
    pieces = call(
        functools.partial(pack_kernel, sides),
        0,
        [qkv.reshape(3 * tokens, heads, size), lift_weight.reshape(-1, group, size)],
        [(3 * tokens + lift_weight.size // (group * size), group, size)] * sides,
        [pltpu.SemaphoreType.DMA((2 * sides,))],
        far=(0, 1),
    )
    got = swap(pieces, "uly")

    def load(layers, extra):
        shapes = [conv_weight.shape[1:]] * len(layers) + extra
        return call(
            functools.partial(load_kernel, layers),
            10**8,
            [conv_weight],
            shapes,
            [pltpu.SemaphoreType.DMA((len(shapes),))],
            far=(0,),
        )

    far = sides // 2
    across = [(i, i ^ far) for i in range(sides)]
    kernels = {}
    quarter = conv_weight.shape[1:4] + (all_ch // 4,)
    kernels[0], *parts = load([0], [quarter] * 2)
    others = []
    for place in range(2):
        parts[place] = lax.ppermute(parts[place], "uly", across)
        others.append(lax.ppermute(parts[place], "grp", [(0, 1), (1, 0)]))
    (mate,) = call(join_kernel, 10**7, parts + others, [conv_weight.shape[1:]])
    span = (share * tokens, sides * 3 * size)
    shared = call(
        functools.partial(regroup_kernel, sides, lines, tokens),
        2 * (group * tokens) ** 2 * span[1],
        got,
        [span] * lines,
        [(group * tokens, span[1])],
    )
    (folded,) = call(
        functools.partial(fold_kernel, sides, 3 * tokens),
        2 * 9 * latent * all_ch * own,
        [*got, kernels[0]],
        [(9 * latent, own)],
        [(latent, all_ch)],
    )
    got = swap(shared, "blk")
    beyond = lax.ppermute(folded, "uly", across)
    folded = swap([folded] * far, "uly") + swap([beyond] * far, "uly")
    (*taps,) = call(
        functools.partial(taps_kernel, sides), 10**7, folded, [(3, 4 * latent, all_ch)] * 2
    )
    block = sides * tokens
    windows = call(
        functools.partial(attention_kernel, sides, lines, share),
        4 * share * size * (lines * block) ** 2,
        got,
        [(3 * block, share * size)] * lines,
        [((lines + 2) * block, share * size)],
    )
    got = swap(windows, "blk")
    (partial,) = call(
        functools.partial(project_kernel, lines),
        2 * 3 * block * lines * share * size * out_weight.shape[1],
        [*got, out_weight],
        [(3 * block, out_weight.shape[1])],
    )
    got = spread(partial, "uly")
    count = (rows + 2) * PATCH
    (current,) = call(
        functools.partial(first_kernel, sides, rows, cols, height),
        18 * count * width * all_ch * own,
        [*got, *taps, conv_weight],
        [(count * width, own)],
        [((count + 2) * width, all_ch)],
    )
    layer, last = SHARED, SHARED + 1
    (current,) = call(
        functools.partial(layer_kernel, layer, sides, half, rows * PATCH, height),
        36 * count * width * all_ch * own,
        [*spread(current, "uly"), conv_weight, mate],
        [((count - 2) * width, 2 * own)],
        [(count * width, all_ch)],
    )
    count -= 4
    _, *got = swap([current] * far, "uly")
    total, *later = call(
        functools.partial(early_kernel, last, sides, half),
        9 * count * width * all_ch * own,
        [current, conv_weight],
        [(count * width, 3 * own)] + [(3, 3 * own, 2 * own)] * len(got),
        sums=(0,),
    )
    (current,) = call(
        functools.partial(last_kernel, last, half, rows * PATCH, height),
        9 * count * width * all_ch * own,
        [total, *got, *later],
        [(count * width, own)],
    )
    return current.reshape(1, count, width, own)


def body(qkv, out_weight, lift_weight, conv_weight):
    if fits_kernels(qkv, lift_weight, conv_weight):
        return body_by_kernels(qkv, out_weight, lift_weight, conv_weight)
    rows, heads = qkv.shape[1], qkv.shape[4]
    lines, sides = lax.axis_size("blk"), lax.axis_size("uly")
    side = lax.axis_index("uly")
    latent_ch = lift_weight.shape[0]
    own = conv_weight.shape[3]
    reach = -(-LAYERS // PATCH)
    lifts = gathered(lift_weight, side)
    folded = jnp.einsum(
        "abdc,ec->abde", conv_weight[0], lifts, preferred_element_type=jnp.float32
    )
    folded = ordered(spread(folded.astype(jnp.bfloat16), "uly"), side)
    folded = jnp.transpose(folded, (1, 2, 0, 3, 4)).reshape(3, 3, sides * own, latent_ch)
    powers = lines & (lines - 1) == 0 and sides & (sides - 1) == 0
    if powers and heads % (lines * sides) == 0:
        patches = window_by_swaps(qkv, out_weight, reach)
    else:
        patches = window_by_gathers(qkv, out_weight, reach)
    height = lines * rows * PATCH
    margin = LAYERS - 1
    start = lax.axis_index("blk") * rows * PATCH
    latent = unfold_patches(patches, latent_ch)
    spare = reach * PATCH - LAYERS
    latent = latent[:, spare : latent.shape[1] - spare]
    current = activate(convolve(latent, folded), start - margin, height)
    for layer in range(1, LAYERS):
        margin -= 1
        kernels = conv_weight[layer]
        if layer > 1:
            current = gathered(current, side)
        current = activate(convolve(current, kernels), start - margin, height)
    return current


def solution(mesh):
    in_specs = (
        P("grp", "blk", "uly", None, None, None),
        P(),
        P(None, "uly"),
        P(None, None, None, "uly", None),
    )
    out_specs = P("grp", "blk", None, "uly")
    return jax.shard_map(
        body, mesh=mesh, in_specs=in_specs, out_specs=out_specs, check_vma=False
    )
```

```python
import functools
import math

import jax
import jax.numpy as jnp
from jax import lax
from jax.experimental import pallas as pl
from jax.experimental.pallas import tpu as pltpu
from jax.sharding import PartitionSpec as P


PATCH = 2
LAYERS = 4
GRANT = 8 * 2**20
SHARED = 2


def swap(pieces, axis):
    count = lax.axis_size(axis)
    got = [pieces[0]]
    for step in range(1, len(pieces)):
        got.append(lax.ppermute(pieces[step], axis, [(i, i ^ step) for i in range(count)]))
    return got


def spread(piece, axis):
    return swap([piece] * lax.axis_size(axis), axis)


def cut(array, start, size, axis):
    return lax.dynamic_slice_in_dim(array, start, size, axis=axis)


def attend(queries, keys, values):
    scale = 1.0 / queries.shape[-1] ** 0.5
    scores = jnp.einsum("hqd,hkd->hqk", queries, keys, preferred_element_type=jnp.float32) * scale
    weights = jnp.exp(scores - jnp.max(scores, axis=2, keepdims=True))
    totals = jnp.sum(weights, axis=2)
    mixed = jnp.einsum(
        "hqk,hkd->hqd", weights.astype(jnp.bfloat16), values, preferred_element_type=jnp.float32
    )
    return (mixed / totals[:, :, None]).astype(jnp.bfloat16)


def ordered(blocks, me):
    stacked = jnp.stack(blocks)
    return jnp.concatenate(
        [cut(stacked, me ^ place, 1, 0) for place in range(len(blocks))], axis=0
    )


def gathered(piece, side):
    blocks = ordered(spread(piece, "uly"), side)
    blocks = jnp.moveaxis(blocks, 0, -2)
    return blocks.reshape(piece.shape[:-1] + (-1,))


def window_by_swaps(qkv, out_weight, reach):
    frames, rows, cols, _, heads, size = qkv.shape
    lines, sides = lax.axis_size("blk"), lax.axis_size("uly")
    line, side = lax.axis_index("blk"), lax.axis_index("uly")
    group, share = heads // sides, heads // sides // lines
    got = swap([cut(qkv, (side ^ s) * group, group, 4) for s in range(sides)], "uly")
    grouped = jnp.stack(got, axis=3)
    grouped = jnp.transpose(grouped, (4, 5, 0, 1, 3, 2, 6))
    got = swap([cut(grouped, (line ^ t) * share, share, 1) for t in range(lines)], "blk")
    shared = ordered(got, line)
    shared = jnp.transpose(shared, (1, 2, 3, 0, 4, 5, 6, 7))
    flat = shared.reshape(3, share, -1, size)
    attended = attend(flat[0], flat[1], flat[2])
    attended = attended.reshape(share, frames, lines * rows, sides * cols, size)
    attended = jnp.transpose(attended, (1, 2, 3, 0, 4)).reshape(
        frames, lines * rows, sides * cols, share * size
    )
    padded = jnp.pad(attended, ((0, 0), (reach, reach), (0, 0), (0, 0)))
    got = swap([cut(padded, (line ^ t) * rows, rows + 2 * reach, 1) for t in range(lines)], "blk")
    partial = 0.0
    for t in range(lines):
        weight = cut(out_weight, ((side * lines) + (line ^ t)) * share * size, share * size, 0)
        partial = partial + jnp.einsum(
            "frcw,wp->frcp", got[t], weight, preferred_element_type=jnp.float32
        )
    partial = partial.astype(jnp.bfloat16)
    got = spread(partial, "uly")
    blocks = []
    for place in range(sides):
        total = 0.0
        for s in range(sides):
            at = (place ^ s) * cols
            total = total + got[s][:, :, at : at + cols].astype(jnp.float32)
        blocks.append(total.astype(jnp.bfloat16))
    patches = ordered(blocks, side)
    patches = jnp.transpose(patches, (1, 2, 0, 3, 4))
    return patches.reshape(frames, rows + 2 * reach, sides * cols, -1)


def window_by_gathers(qkv, out_weight, reach):
    frames, rows, cols, _, heads, size = qkv.shape
    grouped = lax.all_to_all(qkv, "blk", split_axis=4, concat_axis=1, tiled=True)
    flat = [
        lax.all_gather(grouped[:, :, :, which], "uly", axis=2, tiled=True) for which in (1, 2)
    ]
    flat = [grouped[:, :, :, 0]] + flat
    flat = [jnp.swapaxes(one.reshape(-1, one.shape[3], size), 0, 1) for one in flat]
    attended = jnp.swapaxes(attend(*flat), 0, 1)
    attended = attended.reshape(grouped.shape[:3] + grouped.shape[4:])
    restored = lax.all_to_all(attended, "blk", split_axis=1, concat_axis=3, tiled=True)
    patches = jnp.einsum(
        "frcw,wp->frcp",
        restored.reshape(frames, rows, cols, heads * size),
        out_weight,
        preferred_element_type=jnp.float32,
    ).astype(jnp.bfloat16)
    patches = lax.all_gather(patches, "uly", axis=2, tiled=True)
    patches = lax.all_gather(patches, "blk", axis=1, tiled=True)
    padded = jnp.pad(patches, ((0, 0), (reach, reach), (0, 0), (0, 0)))
    return cut(padded, lax.axis_index("blk") * rows, rows + 2 * reach, 1)


def unfold_patches(piece, latent_ch):
    frames, rows, cols = (piece.shape[0], piece.shape[1], piece.shape[2])
    parts = piece.reshape(frames, rows, cols, PATCH, PATCH, latent_ch)
    parts = jnp.transpose(parts, (0, 1, 3, 2, 4, 5))
    return parts.reshape(frames, rows * PATCH, cols * PATCH, latent_ch)


def convolve(current, kernels):
    return lax.conv_general_dilated(
        current,
        kernels,
        (1, 1),
        ((0, 0), (1, 1)),
        dimension_numbers=("NHWC", "HWOI", "NHWC"),
        preferred_element_type=jnp.float32,
    )


def activate(summed, first, height):
    rows = first + lax.broadcasted_iota(jnp.int32, summed.shape, 1)
    inside = (rows >= 0) & (rows < height)
    return jnp.where(inside, jax.nn.silu(summed), 0.0).astype(jnp.bfloat16)


def dot(left, right):
    return jnp.dot(left, right, preferred_element_type=jnp.float32)


def dot_rows(left, right):
    return lax.dot_general(
        left, right, (((1,), (1,)), ((), ())), preferred_element_type=jnp.float32
    )


def picked(source, count):
    rows = source.shape[0]
    places = lax.broadcasted_iota(jnp.int32, (rows, count), 1)
    return jnp.where(places == source, 1.0, 0.0).astype(jnp.bfloat16)


def line_of(rows):
    return lax.broadcasted_iota(jnp.int32, (rows, 1), 0)


def bits(number):
    return number.bit_length() - 1


def call(kernel, flops, inputs, outputs, scratch=(), far=(), sums=()):
    near = pl.BlockSpec(memory_space=pltpu.VMEM)
    kept = pl.BlockSpec(memory_space=pltpu.HBM)
    moved = sum(one.size for one in inputs) + sum(math.prod(shape) for shape in outputs)
    return pl.pallas_call(
        kernel,
        out_shape=[
            jax.ShapeDtypeStruct(shape, jnp.float32 if place in sums else jnp.bfloat16)
            for place, shape in enumerate(outputs)
        ],
        in_specs=[kept if place in far else near for place in range(len(inputs))],
        out_specs=[near] * len(outputs),
        scratch_shapes=[
            pltpu.VMEM(one, jnp.bfloat16) if isinstance(one, tuple) else one for one in scratch
        ],
        compiler_params=pltpu.CompilerParams(vmem_limit_bytes=GRANT),
        cost_estimate=pl.CostEstimate(
            flops=flops, transcendentals=0, bytes_accessed=2 * moved
        ),
    )(*[
        pltpu.with_memory_space_constraint(one, pltpu.HBM) if place in far else one
        for place, one in enumerate(inputs)
    ])


def pack_kernel(sides, flat, lift, *refs):
    out, sems = refs[:sides], refs[sides]
    group, count = out[0].shape[1], flat.shape[0]
    side = lax.axis_index("uly")
    copies = []
    for s in reversed(range(sides)):
        heads = pl.ds(pl.multiple_of((side ^ s) * group, group), group)
        for place, source, target in (
            (s, flat.at[:, heads], out[s].at[pl.ds(0, count)]),
            (sides + s, lift, out[s].at[pl.ds(count, lift.shape[0])]),
        ):
            copies.append(pltpu.make_async_copy(source, target, sems.at[place]))
    for copy in copies:
        copy.start()
    for copy in copies:
        copy.wait()


def load_kernel(layers, kernels, *refs):
    out, sems = refs[:-1], refs[-1]
    sources = [kernels.at[layer] for layer in layers]
    parts = len(out) - len(layers)
    for place in range(parts):
        part = out[-1].shape[3]
        at = (lax.axis_index("grp") * parts + place) * part
        sources.append(kernels.at[SHARED, :, :, :, pl.ds(pl.multiple_of(at, part), part)])
    copies = [
        pltpu.make_async_copy(sources[place], out[place], sems.at[place])
        for place in reversed(range(len(sources)))
    ]
    for copy in copies:
        copy.start()
    for copy in copies:
        copy.wait()


def join_kernel(*refs):
    parts, out = refs[:-1], refs[-1]
    size, each = parts[0].shape[3], len(parts) // 2
    group = lax.axis_index("grp")
    for place, part in enumerate(parts):
        owner = group if place < each else 1 - group
        at = pl.multiple_of((owner * each + place % each) * size, size)
        out[:, :, :, pl.ds(at, size)] = part[...]


def regroup_kernel(sides, lines, tokens, *refs):
    pieces, out, held = refs[:sides], refs[sides : sides + lines], refs[-1]
    _, group, size = pieces[0].shape
    flat = jnp.concatenate(
        [
            piece[: 3 * tokens]
            .reshape(tokens, 3, group, size)[:, which]
            .astype(jnp.float32)
            .reshape(tokens * group, size)
            for piece in pieces
            for which in range(3)
        ],
        axis=1,
    ).astype(jnp.bfloat16)
    at = line_of(group * tokens)
    source = ((at & (tokens - 1)) << bits(group)) + (at >> bits(tokens))
    held[...] = dot(picked(source, tokens * group), flat).astype(jnp.bfloat16)
    line = lax.axis_index("blk")
    span = group * tokens // lines
    for t in range(lines):
        out[t][...] = held[pl.ds(pl.multiple_of((line ^ t) * span, span), span), :]


def attention_kernel(sides, lines, share, *refs):
    pieces, out, held = refs[:lines], refs[lines : 2 * lines], refs[-1]
    tokens = pieces[0].shape[0] // share
    size = pieces[0].shape[1] // (3 * sides)
    block = sides * tokens
    scale = 1.0 / size**0.5
    line = lax.axis_index("blk")
    empty = jnp.zeros((block, held.shape[1]), jnp.bfloat16)
    held[:block] = empty
    held[held.shape[0] - block :] = empty
    wide = [piece[...].astype(jnp.float32) for piece in pieces]
    for head in range(share):
        q, k, v = [
            jnp.concatenate(
                [
                    piece[
                        head * tokens : (head + 1) * tokens,
                        (s * 3 + which) * size : (s * 3 + which + 1) * size,
                    ]
                    for piece in wide
                    for s in range(sides)
                ],
                axis=0,
            ).astype(jnp.bfloat16)
            for which in range(3)
        ]
        scores = dot_rows(q, k) * scale
        weights = jnp.exp(scores - jnp.max(scores, axis=1, keepdims=True))
        totals = jnp.sum(weights, axis=1, keepdims=True)
        mixed = (dot(weights.astype(jnp.bfloat16), v) / totals).astype(jnp.bfloat16)
        for t in range(lines):
            at = pl.multiple_of(((line ^ t) + 1) * block, block)
            held[pl.ds(at, block), head * size : (head + 1) * size] = mixed[
                t * block : (t + 1) * block
            ]
    for t in range(lines):
        at = pl.multiple_of((line ^ t) * block, block)
        out[t][...] = held[pl.ds(at, 3 * block), :]


def project_kernel(lines, *refs):
    pieces, weights, out = refs[:lines], refs[lines], refs[-1]
    line, side = lax.axis_index("blk"), lax.axis_index("uly")
    depth = pieces[0].shape[1]
    summed = 0.0
    for t in range(lines):
        at = pl.multiple_of((side * lines + (line ^ t)) * depth, depth)
        summed = summed + dot(pieces[t][...], weights[pl.ds(at, depth), :])
    out[...] = summed.astype(jnp.bfloat16)


def fold_kernel(sides, skip, *refs):
    pieces, kernels, out, held = refs[:sides], refs[sides], refs[-2], refs[-1]
    latent, own = out.shape[0] // 9, out.shape[1]
    side = lax.axis_index("uly")
    for s in range(sides):
        lift = pieces[s][skip:].astype(jnp.float32).reshape(latent, own).astype(jnp.bfloat16)
        held[:, pl.ds(pl.multiple_of((side ^ s) * own, own), own)] = lift
    lift = held[...]
    for tap in range(9):
        product = dot_rows(lift, kernels[tap // 3, tap % 3])
        out[tap * latent : (tap + 1) * latent, :] = product.astype(jnp.bfloat16)


def activated(summed, first, width, height):
    row = first + (line_of(summed.shape[0]) >> bits(width))
    inside = (row >= 0) & (row < height)
    return jnp.where(inside, jax.nn.silu(summed), 0.0)


def shifted(summed, half, own):
    size = summed.shape[0]
    summed = summed.reshape(size // (2 * half), 2, half, 3 * own)

    def part(parity, tap):
        return summed[:, parity, :, tap * own : (tap + 1) * own].reshape(size // 2, own)

    column = line_of(size // 2) & (half - 1)
    before = jnp.where(column == 0, 0.0, pltpu.roll(part(1, 0), 1, 0))
    after = jnp.where(column == half - 1, 0.0, pltpu.roll(part(0, 2), size // 2 - 1, 0))
    even = before + part(0, 1) + part(1, 2)
    odd = part(0, 0) + part(1, 1) + after
    both = [one.reshape(size // (2 * half), 1, half, own) for one in (even, odd)]
    return jnp.concatenate(both, axis=1).reshape(size, own)


def convolved(current, kernels, half):
    width = 2 * half
    size = current.shape[0] - 2 * width
    summed = 0.0
    for above in range(3):
        taps = kernels[above]
        taps = taps.reshape(-1, taps.shape[-1])
        summed = summed + dot_rows(current[above * width : above * width + size, :], taps)
    return summed


def taps_kernel(sides, *refs):
    folded, even_taps, odd_taps = refs[:sides], refs[-2], refs[-1]
    side = lax.axis_index("uly")
    latent = folded[0].shape[0] // 9
    own = folded[0].shape[1]
    empty = jnp.zeros((latent, sides * own), jnp.bfloat16)
    for above in range(3):
        even_taps[above, 2 * latent : 3 * latent, :] = empty
        odd_taps[above, 3 * latent :, :] = empty
        for s in range(sides):
            lanes = pl.ds(pl.multiple_of((side ^ s) * own, own), own)
            for beside in range(3):
                at = (above * 3 + beside) * latent
                taps = folded[s][at : at + latent, :]
                to = (3, 0, 1)[beside] * latent
                even_taps[above, to : to + latent, lanes] = taps
                odd_taps[above, beside * latent : (beside + 1) * latent, lanes] = taps


def first_kernel(sides, rows, cols, height, *refs):
    partials, (even_taps, odd_taps, kernels, out, held) = refs[:sides], refs[sides:]
    kernels = kernels.at[1]
    side, line = lax.axis_index("uly"), lax.axis_index("blk")
    half = sides * cols
    count = partials[0].shape[0]
    latent = even_taps.shape[1] // 4
    own = kernels.shape[2]
    at = line_of(count)
    column = at & (cols - 1)
    group = (at >> bits(cols)) & (sides - 1)
    row = (at >> bits(half)) & (rows - 1)
    block = at >> bits(half * rows)
    picks = []
    for s in range(sides):
        source = (((block << bits(sides)) + (group ^ side ^ s)) << bits(rows)) + row
        picks.append((source << bits(cols)) + column)
    places = lax.broadcasted_iota(jnp.int32, (count, sides * count), 1)
    hits = places == picks[0]
    for s in range(1, sides):
        hits = hits | (places == picks[s] + s * count)
    picks = jnp.where(hits, 1.0, 0.0).astype(jnp.bfloat16)
    total = dot(picks, jnp.concatenate([piece[...] for piece in partials], axis=0))
    total = total.astype(jnp.bfloat16).astype(jnp.float32)
    wide = 2 * latent
    lines = [
        total[:, i * wide : (i + 1) * wide].reshape(count // half, 1, half, wide) for i in range(2)
    ]
    latents = jnp.concatenate(lines, axis=1).reshape(2 * count, wide)
    place = line_of(2 * count) & (half - 1)
    before = jnp.where(place == 0, 0.0, pltpu.roll(latents, 1, 0))
    after = jnp.where(place == half - 1, 0.0, pltpu.roll(latents, 2 * count - 1, 0))
    start = line * rows * PATCH - (LAYERS - 1)
    size = 2 * count - 2 * half
    for parity, (other, taps) in enumerate(((before, even_taps), (after, odd_taps))):
        current = jnp.concatenate([latents, other], axis=1).astype(jnp.bfloat16)
        summed = 0.0
        for above in range(3):
            summed = summed + dot(current[above * half : above * half + size], taps[above])
        summed = activated(summed, start, half, height).astype(jnp.bfloat16)
        for row in range(size // half):
            at = (2 * row + parity) * half
            held[at : at + half, :] = summed[row * half : (row + 1) * half]
    summed = shifted(convolved(held, kernels, half), half, own)
    out[...] = activated(summed, start + 1, 2 * half, height).astype(jnp.bfloat16)


def layer_kernel(layer, pieces_in, half, step, height, *refs):
    pieces = refs[:pieces_in]
    kernels = [refs[pieces_in].at[layer], *refs[pieces_in + 1 : -2]]
    out, held = refs[-2:]
    side, line = lax.axis_index("uly"), lax.axis_index("blk")
    own = kernels[0].shape[2]
    for s in range(pieces_in):
        lanes = pl.ds(pl.multiple_of((side ^ s) * own, own), own)
        held[:, lanes] = pieces[s][...]
    first = line * step + layer + 1 - LAYERS
    for place, taps in enumerate(kernels):
        summed = shifted(convolved(held, taps, half), half, own)
        result = activated(summed, first, 2 * half, height).astype(jnp.bfloat16)
        out[:, place * own : (place + 1) * own] = result


def early_kernel(layer, sides, half, *refs):
    piece, kernels, total, later = refs[0], refs[1].at[layer], refs[2], refs[3:]
    side = lax.axis_index("uly")
    own = kernels.shape[2]

    def met(above, s):
        places = [side ^ s, side ^ s ^ (sides // 2)]
        lanes = [pl.ds(pl.multiple_of(place * own, own), own) for place in places]
        taps = [kernels[above, :, :, lane].reshape(3 * own, own) for lane in lanes]
        return jnp.concatenate(taps, axis=1)

    total[...] = convolved(piece, [met(above, 0) for above in range(3)], half)
    for s, out in enumerate(later, 1):
        for above in range(3):
            out[above] = met(above, s)


def last_kernel(layer, half, step, height, *refs):
    count = (len(refs) - 2) // 2
    total, pieces, kernels, out = refs[0], refs[1 : 1 + count], refs[1 + count : -1], refs[-1]
    summed = total[...]
    for piece, taps in zip(pieces, kernels):
        summed = summed + convolved(piece, taps, half)
    width = 2 * half
    first = lax.axis_index("blk") * step + layer + 1 - LAYERS
    summed = shifted(summed, half, summed.shape[1] // 3)
    result = activated(summed, first, width, height).astype(jnp.bfloat16)
    at = line_of(result.shape[0])
    column = at & (width - 1)
    source = (at - column) + ((column & 1) << bits(half)) + (column >> 1)
    out[...] = dot(picked(source, result.shape[0]), result).astype(jnp.bfloat16)


def fits_kernels(qkv, lift_weight, conv_weight):
    frames, rows, cols, _, heads, size = qkv.shape
    lines, sides = lax.axis_size("blk"), lax.axis_size("uly")
    powers = all(n & (n - 1) == 0 for n in (lines, sides, rows, cols, heads))
    return (
        powers
        and lax.axis_size("grp") == 2
        and sides >= 4
        and frames == 1
        and LAYERS == SHARED + 2
        and rows * PATCH == LAYERS
        and heads % (lines * sides) == 0
        and rows * cols % 8 == 0
        and rows * cols * heads // (lines * sides) % 16 == 0
        and rows * cols * sides % 32 == 0
        and sides * cols % 16 == 0
        and heads // sides % 8 == 0
        and size % 128 == 0
        and conv_weight.shape[3] % 128 == 0
        and lift_weight.size % (heads // sides * size) == 0
        and conv_weight.shape[3] == size
        and lift_weight.shape[0] * 2 % 128 == 0
    )


def body_by_kernels(qkv, out_weight, lift_weight, conv_weight):
    _, rows, cols, _, heads, size = qkv.shape
    lines, sides = lax.axis_size("blk"), lax.axis_size("uly")
    group, share = heads // sides, heads // sides // lines
    latent, own = lift_weight.shape
    tokens, half = rows * cols, sides * cols
    height = lines * rows * PATCH
    width, all_ch = 2 * half, sides * own
    pieces = call(
        functools.partial(pack_kernel, sides),
        0,
        [qkv.reshape(3 * tokens, heads, size), lift_weight.reshape(-1, group, size)],
        [(3 * tokens + lift_weight.size // (group * size), group, size)] * sides,
        [pltpu.SemaphoreType.DMA((2 * sides,))],
        far=(0, 1),
    )
    got = swap(pieces, "uly")

    def load(layers, extra):
        shapes = [conv_weight.shape[1:]] * len(layers) + extra
        return call(
            functools.partial(load_kernel, layers),
            10**8,
            [conv_weight],
            shapes,
            [pltpu.SemaphoreType.DMA((len(shapes),))],
            far=(0,),
        )

    far = sides // 2
    across = [(i, i ^ far) for i in range(sides)]
    kernels = {}
    quarter = conv_weight.shape[1:4] + (all_ch // 4,)
    kernels[0], *parts = load([0], [quarter] * 2)
    others = []
    for place in range(2):
        parts[place] = lax.ppermute(parts[place], "uly", across)
        others.append(lax.ppermute(parts[place], "grp", [(0, 1), (1, 0)]))
    (mate,) = call(join_kernel, 10**7, parts + others, [conv_weight.shape[1:]])
    span = (share * tokens, sides * 3 * size)
    shared = call(
        functools.partial(regroup_kernel, sides, lines, tokens),
        2 * (group * tokens) ** 2 * span[1],
        got,
        [span] * lines,
        [(group * tokens, span[1])],
    )
    (folded,) = call(
        functools.partial(fold_kernel, sides, 3 * tokens),
        2 * 9 * latent * all_ch * own,
        [*got, kernels[0]],
        [(9 * latent, own)],
        [(latent, all_ch)],
    )
    got = swap(shared, "blk")
    beyond = lax.ppermute(folded, "uly", across)
    folded = swap([folded] * far, "uly") + swap([beyond] * far, "uly")
    (*taps,) = call(
        functools.partial(taps_kernel, sides), 10**7, folded, [(3, 4 * latent, all_ch)] * 2
    )
    block = sides * tokens
    windows = call(
        functools.partial(attention_kernel, sides, lines, share),
        4 * share * size * (lines * block) ** 2,
        got,
        [(3 * block, share * size)] * lines,
        [((lines + 2) * block, share * size)],
    )
    got = swap(windows, "blk")
    (partial,) = call(
        functools.partial(project_kernel, lines),
        2 * 3 * block * lines * share * size * out_weight.shape[1],
        [*got, out_weight],
        [(3 * block, out_weight.shape[1])],
    )
    got = spread(partial, "uly")
    count = (rows + 2) * PATCH
    (current,) = call(
        functools.partial(first_kernel, sides, rows, cols, height),
        18 * count * width * all_ch * own,
        [*got, *taps, conv_weight],
        [(count * width, own)],
        [((count + 2) * width, all_ch)],
    )
    layer, last = SHARED, SHARED + 1
    (current,) = call(
        functools.partial(layer_kernel, layer, sides, half, rows * PATCH, height),
        36 * count * width * all_ch * own,
        [*spread(current, "uly"), conv_weight, mate],
        [((count - 2) * width, 2 * own)],
        [(count * width, all_ch)],
    )
    count -= 4
    _, *got = swap([current] * far, "uly")
    total, *later = call(
        functools.partial(early_kernel, last, sides, half),
        9 * count * width * all_ch * own,
        [current, conv_weight],
        [(count * width, 3 * own)] + [(3, 3 * own, 2 * own)] * len(got),
        sums=(0,),
    )
    (current,) = call(
        functools.partial(last_kernel, last, half, rows * PATCH, height),
        9 * count * width * all_ch * own,
        [total, *got, *later],
        [(count * width, own)],
    )
    return current.reshape(1, count, width, own)


def body(qkv, out_weight, lift_weight, conv_weight):
    if fits_kernels(qkv, lift_weight, conv_weight):
        return body_by_kernels(qkv, out_weight, lift_weight, conv_weight)
    rows, heads = qkv.shape[1], qkv.shape[4]
    lines, sides = lax.axis_size("blk"), lax.axis_size("uly")
    side = lax.axis_index("uly")
    latent_ch = lift_weight.shape[0]
    own = conv_weight.shape[3]
    reach = -(-LAYERS // PATCH)
    lifts = gathered(lift_weight, side)
    folded = jnp.einsum(
        "abdc,ec->abde", conv_weight[0], lifts, preferred_element_type=jnp.float32
    )
    folded = ordered(spread(folded.astype(jnp.bfloat16), "uly"), side)
    folded = jnp.transpose(folded, (1, 2, 0, 3, 4)).reshape(3, 3, sides * own, latent_ch)
    powers = lines & (lines - 1) == 0 and sides & (sides - 1) == 0
    if powers and heads % (lines * sides) == 0:
        patches = window_by_swaps(qkv, out_weight, reach)
    else:
        patches = window_by_gathers(qkv, out_weight, reach)
    height = lines * rows * PATCH
    margin = LAYERS - 1
    start = lax.axis_index("blk") * rows * PATCH
    latent = unfold_patches(patches, latent_ch)
    spare = reach * PATCH - LAYERS
    latent = latent[:, spare : latent.shape[1] - spare]
    current = activate(convolve(latent, folded), start - margin, height)
    for layer in range(1, LAYERS):
        margin -= 1
        kernels = conv_weight[layer]
        if layer > 1:
            current = gathered(current, side)
        current = activate(convolve(current, kernels), start - margin, height)
    return current


def solution(mesh):
    in_specs = (
        P("grp", "blk", "uly", None, None, None),
        P(),
        P(None, "uly"),
        P(None, None, None, "uly", None),
    )
    out_specs = P("grp", "blk", None, "uly")
    return jax.shard_map(
        body, mesh=mesh, in_specs=in_specs, out_specs=out_specs, check_vma=False
    )
```

```python
import functools
import math

import jax
import jax.numpy as jnp
from jax import lax
from jax.experimental import pallas as pl
from jax.experimental.pallas import tpu as pltpu
from jax.sharding import PartitionSpec as P


PATCH = 2
LAYERS = 4
GRANT = 8 * 2**20
SHARED = 2


def swap(pieces, axis):
    count = lax.axis_size(axis)
    got = [pieces[0]]
    for step in range(1, len(pieces)):
        got.append(lax.ppermute(pieces[step], axis, [(i, i ^ step) for i in range(count)]))
    return got


def spread(piece, axis):
    return swap([piece] * lax.axis_size(axis), axis)


def cut(array, start, size, axis):
    return lax.dynamic_slice_in_dim(array, start, size, axis=axis)


def attend(queries, keys, values):
    scale = 1.0 / queries.shape[-1] ** 0.5
    scores = jnp.einsum("hqd,hkd->hqk", queries, keys, preferred_element_type=jnp.float32) * scale
    weights = jnp.exp(scores - jnp.max(scores, axis=2, keepdims=True))
    totals = jnp.sum(weights, axis=2)
    mixed = jnp.einsum(
        "hqk,hkd->hqd", weights.astype(jnp.bfloat16), values, preferred_element_type=jnp.float32
    )
    return (mixed / totals[:, :, None]).astype(jnp.bfloat16)


def ordered(blocks, me):
    stacked = jnp.stack(blocks)
    return jnp.concatenate(
        [cut(stacked, me ^ place, 1, 0) for place in range(len(blocks))], axis=0
    )


def gathered(piece, side):
    blocks = ordered(spread(piece, "uly"), side)
    blocks = jnp.moveaxis(blocks, 0, -2)
    return blocks.reshape(piece.shape[:-1] + (-1,))


def window_by_swaps(qkv, out_weight, reach):
    frames, rows, cols, _, heads, size = qkv.shape
    lines, sides = lax.axis_size("blk"), lax.axis_size("uly")
    line, side = lax.axis_index("blk"), lax.axis_index("uly")
    group, share = heads // sides, heads // sides // lines
    got = swap([cut(qkv, (side ^ s) * group, group, 4) for s in range(sides)], "uly")
    grouped = jnp.stack(got, axis=3)
    grouped = jnp.transpose(grouped, (4, 5, 0, 1, 3, 2, 6))
    got = swap([cut(grouped, (line ^ t) * share, share, 1) for t in range(lines)], "blk")
    shared = ordered(got, line)
    shared = jnp.transpose(shared, (1, 2, 3, 0, 4, 5, 6, 7))
    flat = shared.reshape(3, share, -1, size)
    attended = attend(flat[0], flat[1], flat[2])
    attended = attended.reshape(share, frames, lines * rows, sides * cols, size)
    attended = jnp.transpose(attended, (1, 2, 3, 0, 4)).reshape(
        frames, lines * rows, sides * cols, share * size
    )
    padded = jnp.pad(attended, ((0, 0), (reach, reach), (0, 0), (0, 0)))
    got = swap([cut(padded, (line ^ t) * rows, rows + 2 * reach, 1) for t in range(lines)], "blk")
    partial = 0.0
    for t in range(lines):
        weight = cut(out_weight, ((side * lines) + (line ^ t)) * share * size, share * size, 0)
        partial = partial + jnp.einsum(
            "frcw,wp->frcp", got[t], weight, preferred_element_type=jnp.float32
        )
    partial = partial.astype(jnp.bfloat16)
    got = spread(partial, "uly")
    blocks = []
    for place in range(sides):
        total = 0.0
        for s in range(sides):
            at = (place ^ s) * cols
            total = total + got[s][:, :, at : at + cols].astype(jnp.float32)
        blocks.append(total.astype(jnp.bfloat16))
    patches = ordered(blocks, side)
    patches = jnp.transpose(patches, (1, 2, 0, 3, 4))
    return patches.reshape(frames, rows + 2 * reach, sides * cols, -1)


def window_by_gathers(qkv, out_weight, reach):
    frames, rows, cols, _, heads, size = qkv.shape
    grouped = lax.all_to_all(qkv, "blk", split_axis=4, concat_axis=1, tiled=True)
    flat = [
        lax.all_gather(grouped[:, :, :, which], "uly", axis=2, tiled=True) for which in (1, 2)
    ]
    flat = [grouped[:, :, :, 0]] + flat
    flat = [jnp.swapaxes(one.reshape(-1, one.shape[3], size), 0, 1) for one in flat]
    attended = jnp.swapaxes(attend(*flat), 0, 1)
    attended = attended.reshape(grouped.shape[:3] + grouped.shape[4:])
    restored = lax.all_to_all(attended, "blk", split_axis=1, concat_axis=3, tiled=True)
    patches = jnp.einsum(
        "frcw,wp->frcp",
        restored.reshape(frames, rows, cols, heads * size),
        out_weight,
        preferred_element_type=jnp.float32,
    ).astype(jnp.bfloat16)
    patches = lax.all_gather(patches, "uly", axis=2, tiled=True)
    patches = lax.all_gather(patches, "blk", axis=1, tiled=True)
    padded = jnp.pad(patches, ((0, 0), (reach, reach), (0, 0), (0, 0)))
    return cut(padded, lax.axis_index("blk") * rows, rows + 2 * reach, 1)


def unfold_patches(piece, latent_ch):
    frames, rows, cols = (piece.shape[0], piece.shape[1], piece.shape[2])
    parts = piece.reshape(frames, rows, cols, PATCH, PATCH, latent_ch)
    parts = jnp.transpose(parts, (0, 1, 3, 2, 4, 5))
    return parts.reshape(frames, rows * PATCH, cols * PATCH, latent_ch)


def convolve(current, kernels):
    return lax.conv_general_dilated(
        current,
        kernels,
        (1, 1),
        ((0, 0), (1, 1)),
        dimension_numbers=("NHWC", "HWOI", "NHWC"),
        preferred_element_type=jnp.float32,
    )


def activate(summed, first, height):
    rows = first + lax.broadcasted_iota(jnp.int32, summed.shape, 1)
    inside = (rows >= 0) & (rows < height)
    return jnp.where(inside, jax.nn.silu(summed), 0.0).astype(jnp.bfloat16)


def dot(left, right):
    return jnp.dot(left, right, preferred_element_type=jnp.float32)


def dot_rows(left, right):
    return lax.dot_general(
        left, right, (((1,), (1,)), ((), ())), preferred_element_type=jnp.float32
    )


def picked(source, count):
    rows = source.shape[0]
    places = lax.broadcasted_iota(jnp.int32, (rows, count), 1)
    return jnp.where(places == source, 1.0, 0.0).astype(jnp.bfloat16)


def line_of(rows):
    return lax.broadcasted_iota(jnp.int32, (rows, 1), 0)


def bits(number):
    return number.bit_length() - 1


def call(kernel, flops, inputs, outputs, scratch=(), far=(), sums=()):
    near = pl.BlockSpec(memory_space=pltpu.VMEM)
    kept = pl.BlockSpec(memory_space=pltpu.HBM)
    moved = sum(one.size for one in inputs) + sum(math.prod(shape) for shape in outputs)
    return pl.pallas_call(
        kernel,
        out_shape=[
            jax.ShapeDtypeStruct(shape, jnp.float32 if place in sums else jnp.bfloat16)
            for place, shape in enumerate(outputs)
        ],
        in_specs=[kept if place in far else near for place in range(len(inputs))],
        out_specs=[near] * len(outputs),
        scratch_shapes=[
            pltpu.VMEM(one, jnp.bfloat16) if isinstance(one, tuple) else one for one in scratch
        ],
        compiler_params=pltpu.CompilerParams(vmem_limit_bytes=GRANT),
        cost_estimate=pl.CostEstimate(
            flops=flops, transcendentals=0, bytes_accessed=2 * moved
        ),
    )(*[
        pltpu.with_memory_space_constraint(one, pltpu.HBM) if place in far else one
        for place, one in enumerate(inputs)
    ])


def pack_kernel(sides, flat, lift, *refs):
    out, sems = refs[:sides], refs[sides]
    group, count = out[0].shape[1], flat.shape[0]
    side = lax.axis_index("uly")
    copies = []
    for s in reversed(range(sides)):
        heads = pl.ds(pl.multiple_of((side ^ s) * group, group), group)
        for place, source, target in (
            (s, flat.at[:, heads], out[s].at[pl.ds(0, count)]),
            (sides + s, lift, out[s].at[pl.ds(count, lift.shape[0])]),
        ):
            copies.append(pltpu.make_async_copy(source, target, sems.at[place]))
    for copy in copies:
        copy.start()
    for copy in copies:
        copy.wait()


def load_kernel(layers, kernels, *refs):
    out, sems = refs[:-1], refs[-1]
    sources = [kernels.at[layer] for layer in layers]
    parts = len(out) - len(layers)
    for place in range(parts):
        part = out[-1].shape[3]
        at = (lax.axis_index("grp") * parts + place) * part
        sources.append(kernels.at[SHARED, :, :, :, pl.ds(pl.multiple_of(at, part), part)])
    copies = [
        pltpu.make_async_copy(sources[place], out[place], sems.at[place])
        for place in reversed(range(len(sources)))
    ]
    for copy in copies:
        copy.start()
    for copy in copies:
        copy.wait()


def join_kernel(*refs):
    parts, out = refs[:-1], refs[-1]
    size, each = parts[0].shape[3], len(parts) // 2
    group = lax.axis_index("grp")
    for place, part in enumerate(parts):
        owner = group if place < each else 1 - group
        at = pl.multiple_of((owner * each + place % each) * size, size)
        out[:, :, :, pl.ds(at, size)] = part[...]


def regroup_kernel(sides, lines, tokens, *refs):
    pieces, out, held = refs[:sides], refs[sides : sides + lines], refs[-1]
    _, group, size = pieces[0].shape
    flat = jnp.concatenate(
        [
            piece[: 3 * tokens]
            .reshape(tokens, 3, group, size)[:, which]
            .astype(jnp.float32)
            .reshape(tokens * group, size)
            for piece in pieces
            for which in range(3)
        ],
        axis=1,
    ).astype(jnp.bfloat16)
    at = line_of(group * tokens)
    source = ((at & (tokens - 1)) << bits(group)) + (at >> bits(tokens))
    held[...] = dot(picked(source, tokens * group), flat).astype(jnp.bfloat16)
    line = lax.axis_index("blk")
    span = group * tokens // lines
    for t in range(lines):
        out[t][...] = held[pl.ds(pl.multiple_of((line ^ t) * span, span), span), :]


def attention_kernel(sides, lines, share, *refs):
    pieces, out, held = refs[:lines], refs[lines : 2 * lines], refs[-1]
    tokens = pieces[0].shape[0] // share
    size = pieces[0].shape[1] // (3 * sides)
    block = sides * tokens
    scale = 1.0 / size**0.5
    line = lax.axis_index("blk")
    empty = jnp.zeros((block, held.shape[1]), jnp.bfloat16)
    held[:block] = empty
    held[held.shape[0] - block :] = empty
    wide = [piece[...].astype(jnp.float32) for piece in pieces]
    for head in range(share):
        q, k, v = [
            jnp.concatenate(
                [
                    piece[
                        head * tokens : (head + 1) * tokens,
                        (s * 3 + which) * size : (s * 3 + which + 1) * size,
                    ]
                    for piece in wide
                    for s in range(sides)
                ],
                axis=0,
            ).astype(jnp.bfloat16)
            for which in range(3)
        ]
        scores = dot_rows(q, k) * scale
        weights = jnp.exp(scores - jnp.max(scores, axis=1, keepdims=True))
        totals = jnp.sum(weights, axis=1, keepdims=True)
        mixed = (dot(weights.astype(jnp.bfloat16), v) / totals).astype(jnp.bfloat16)
        for t in range(lines):
            at = pl.multiple_of(((line ^ t) + 1) * block, block)
            held[pl.ds(at, block), head * size : (head + 1) * size] = mixed[
                t * block : (t + 1) * block
            ]
    for t in range(lines):
        at = pl.multiple_of((line ^ t) * block, block)
        out[t][...] = held[pl.ds(at, 3 * block), :]


def project_kernel(lines, *refs):
    pieces, weights, out = refs[:lines], refs[lines], refs[-1]
    line, side = lax.axis_index("blk"), lax.axis_index("uly")
    depth = pieces[0].shape[1]
    summed = 0.0
    for t in range(lines):
        at = pl.multiple_of((side * lines + (line ^ t)) * depth, depth)
        summed = summed + dot(pieces[t][...], weights[pl.ds(at, depth), :])
    out[...] = summed.astype(jnp.bfloat16)


def fold_kernel(sides, skip, *refs):
    pieces, kernels, out, held = refs[:sides], refs[sides], refs[-2], refs[-1]
    latent, own = out.shape[0] // 9, out.shape[1]
    side = lax.axis_index("uly")
    for s in range(sides):
        lift = pieces[s][skip:].astype(jnp.float32).reshape(latent, own).astype(jnp.bfloat16)
        held[:, pl.ds(pl.multiple_of((side ^ s) * own, own), own)] = lift
    lift = held[...]
    for tap in range(9):
        product = dot_rows(lift, kernels[tap // 3, tap % 3])
        out[tap * latent : (tap + 1) * latent, :] = product.astype(jnp.bfloat16)


def activated(summed, first, width, height):
    row = first + (line_of(summed.shape[0]) >> bits(width))
    inside = (row >= 0) & (row < height)
    return jnp.where(inside, jax.nn.silu(summed), 0.0)


def shifted(summed, half, own):
    size = summed.shape[0]
    summed = summed.reshape(size // (2 * half), 2, half, 3 * own)

    def part(parity, tap):
        return summed[:, parity, :, tap * own : (tap + 1) * own].reshape(size // 2, own)

    column = line_of(size // 2) & (half - 1)
    before = jnp.where(column == 0, 0.0, pltpu.roll(part(1, 0), 1, 0))
    after = jnp.where(column == half - 1, 0.0, pltpu.roll(part(0, 2), size // 2 - 1, 0))
    even = before + part(0, 1) + part(1, 2)
    odd = part(0, 0) + part(1, 1) + after
    both = [one.reshape(size // (2 * half), 1, half, own) for one in (even, odd)]
    return jnp.concatenate(both, axis=1).reshape(size, own)


def convolved(current, kernels, half):
    width = 2 * half
    size = current.shape[0] - 2 * width
    summed = 0.0
    for above in range(3):
        taps = kernels[above]
        taps = taps.reshape(-1, taps.shape[-1])
        summed = summed + dot_rows(current[above * width : above * width + size, :], taps)
    return summed


def taps_kernel(sides, *refs):
    folded, even_taps, odd_taps = refs[:sides], refs[-2], refs[-1]
    side = lax.axis_index("uly")
    latent = folded[0].shape[0] // 9
    own = folded[0].shape[1]
    empty = jnp.zeros((latent, sides * own), jnp.bfloat16)
    for above in range(3):
        even_taps[above, 2 * latent : 3 * latent, :] = empty
        odd_taps[above, 3 * latent :, :] = empty
        for s in range(sides):
            lanes = pl.ds(pl.multiple_of((side ^ s) * own, own), own)
            for beside in range(3):
                at = (above * 3 + beside) * latent
                taps = folded[s][at : at + latent, :]
                to = (3, 0, 1)[beside] * latent
                even_taps[above, to : to + latent, lanes] = taps
                odd_taps[above, beside * latent : (beside + 1) * latent, lanes] = taps


def first_kernel(sides, rows, cols, height, *refs):
    partials, (even_taps, odd_taps, kernels, out, held) = refs[:sides], refs[sides:]
    kernels = kernels.at[1]
    side, line = lax.axis_index("uly"), lax.axis_index("blk")
    half = sides * cols
    count = partials[0].shape[0]
    latent = even_taps.shape[1] // 4
    own = kernels.shape[2]
    at = line_of(count)
    column = at & (cols - 1)
    group = (at >> bits(cols)) & (sides - 1)
    row = (at >> bits(half)) & (rows - 1)
    block = at >> bits(half * rows)
    picks = []
    for s in range(sides):
        source = (((block << bits(sides)) + (group ^ side ^ s)) << bits(rows)) + row
        picks.append((source << bits(cols)) + column)
    places = lax.broadcasted_iota(jnp.int32, (count, sides * count), 1)
    hits = places == picks[0]
    for s in range(1, sides):
        hits = hits | (places == picks[s] + s * count)
    picks = jnp.where(hits, 1.0, 0.0).astype(jnp.bfloat16)
    total = dot(picks, jnp.concatenate([piece[...] for piece in partials], axis=0))
    total = total.astype(jnp.bfloat16).astype(jnp.float32)
    wide = 2 * latent
    lines = [
        total[:, i * wide : (i + 1) * wide].reshape(count // half, 1, half, wide) for i in range(2)
    ]
    latents = jnp.concatenate(lines, axis=1).reshape(2 * count, wide)
    place = line_of(2 * count) & (half - 1)
    before = jnp.where(place == 0, 0.0, pltpu.roll(latents, 1, 0))
    after = jnp.where(place == half - 1, 0.0, pltpu.roll(latents, 2 * count - 1, 0))
    start = line * rows * PATCH - (LAYERS - 1)
    size = 2 * count - 2 * half
    for parity, (other, taps) in enumerate(((before, even_taps), (after, odd_taps))):
        current = jnp.concatenate([latents, other], axis=1).astype(jnp.bfloat16)
        summed = 0.0
        for above in range(3):
            summed = summed + dot(current[above * half : above * half + size], taps[above])
        summed = activated(summed, start, half, height).astype(jnp.bfloat16)
        for row in range(size // half):
            at = (2 * row + parity) * half
            held[at : at + half, :] = summed[row * half : (row + 1) * half]
    summed = shifted(convolved(held, kernels, half), half, own)
    out[...] = activated(summed, start + 1, 2 * half, height).astype(jnp.bfloat16)


def met(kernels, above, places):
    own = kernels.shape[2]
    lanes = [pl.ds(pl.multiple_of(place * own, own), own) for place in places]
    taps = [kernels[above, :, :, lane].reshape(3 * own, own) for lane in lanes]
    return jnp.concatenate(taps, axis=1)


def near_kernel(layer, sides, half, *refs):
    near = sides // 2
    pieces, kernels, total, later = refs[:near], refs[near].at[layer], refs[-2], refs[-1]
    side = lax.axis_index("uly")
    current = jnp.concatenate([piece[...] for piece in pieces], axis=1)
    taps = [met(kernels, above, [side ^ s for s in range(near)]) for above in range(3)]
    total[...] = convolved(current, taps, half)
    for above in range(3):
        later[above] = met(kernels, above, [side ^ s for s in range(near, sides)])


def layer_kernel(layer, sides, half, step, height, *refs):
    total, pieces, (later, mate, out, held) = refs[0], refs[1 : 1 + sides], refs[1 + sides :]
    side, line = lax.axis_index("uly"), lax.axis_index("blk")
    own = mate.shape[2]
    for s in range(sides):
        lanes = pl.ds(pl.multiple_of((side ^ s) * own, own), own)
        held[:, lanes] = pieces[s][...]
    first = line * step + layer + 1 - LAYERS
    rest = jnp.concatenate([piece[...] for piece in pieces[sides // 2 :]], axis=1)
    sums = (total[...] + convolved(rest, later, half), convolved(held, mate, half))
    for place, summed in enumerate(sums):
        summed = shifted(summed, half, own)
        result = activated(summed, first, 2 * half, height).astype(jnp.bfloat16)
        out[:, place * own : (place + 1) * own] = result


def early_kernel(layer, sides, half, *refs):
    piece, kernels, total, later = refs[0], refs[1].at[layer], refs[2], refs[3:]
    side = lax.axis_index("uly")
    own = kernels.shape[2]

    def met(above, s):
        places = [side ^ s, side ^ s ^ (sides // 2)]
        lanes = [pl.ds(pl.multiple_of(place * own, own), own) for place in places]
        taps = [kernels[above, :, :, lane].reshape(3 * own, own) for lane in lanes]
        return jnp.concatenate(taps, axis=1)

    total[...] = convolved(piece, [met(above, 0) for above in range(3)], half)
    for s, out in enumerate(later, 1):
        for above in range(3):
            out[above] = met(above, s)


def last_kernel(layer, half, step, height, *refs):
    count = (len(refs) - 2) // 2
    total, pieces, kernels, out = refs[0], refs[1 : 1 + count], refs[1 + count : -1], refs[-1]
    summed = total[...]
    for piece, taps in zip(pieces, kernels):
        summed = summed + convolved(piece, taps, half)
    width = 2 * half
    first = lax.axis_index("blk") * step + layer + 1 - LAYERS
    summed = shifted(summed, half, summed.shape[1] // 3)
    result = activated(summed, first, width, height).astype(jnp.bfloat16)
    at = line_of(result.shape[0])
    column = at & (width - 1)
    source = (at - column) + ((column & 1) << bits(half)) + (column >> 1)
    out[...] = dot(picked(source, result.shape[0]), result).astype(jnp.bfloat16)


def fits_kernels(qkv, lift_weight, conv_weight):
    frames, rows, cols, _, heads, size = qkv.shape
    lines, sides = lax.axis_size("blk"), lax.axis_size("uly")
    powers = all(n & (n - 1) == 0 for n in (lines, sides, rows, cols, heads))
    return (
        powers
        and lax.axis_size("grp") == 2
        and sides >= 4
        and frames == 1
        and LAYERS == SHARED + 2
        and rows * PATCH == LAYERS
        and heads % (lines * sides) == 0
        and rows * cols % 8 == 0
        and rows * cols * heads // (lines * sides) % 16 == 0
        and rows * cols * sides % 32 == 0
        and sides * cols % 16 == 0
        and heads // sides % 8 == 0
        and size % 128 == 0
        and conv_weight.shape[3] % 128 == 0
        and lift_weight.size % (heads // sides * size) == 0
        and conv_weight.shape[3] == size
        and lift_weight.shape[0] * 2 % 128 == 0
    )


def body_by_kernels(qkv, out_weight, lift_weight, conv_weight):
    _, rows, cols, _, heads, size = qkv.shape
    lines, sides = lax.axis_size("blk"), lax.axis_size("uly")
    group, share = heads // sides, heads // sides // lines
    latent, own = lift_weight.shape
    tokens, half = rows * cols, sides * cols
    height = lines * rows * PATCH
    width, all_ch = 2 * half, sides * own
    pieces = call(
        functools.partial(pack_kernel, sides),
        0,
        [qkv.reshape(3 * tokens, heads, size), lift_weight.reshape(-1, group, size)],
        [(3 * tokens + lift_weight.size // (group * size), group, size)] * sides,
        [pltpu.SemaphoreType.DMA((2 * sides,))],
        far=(0, 1),
    )
    got = swap(pieces, "uly")

    def load(layers, extra):
        shapes = [conv_weight.shape[1:]] * len(layers) + extra
        return call(
            functools.partial(load_kernel, layers),
            10**8,
            [conv_weight],
            shapes,
            [pltpu.SemaphoreType.DMA((len(shapes),))],
            far=(0,),
        )

    far = sides // 2
    across = [(i, i ^ far) for i in range(sides)]
    kernels = {}
    quarter = conv_weight.shape[1:4] + (all_ch // 4,)
    kernels[0], *parts = load([0], [quarter] * 2)
    others = []
    for place in range(2):
        parts[place] = lax.ppermute(parts[place], "uly", across)
        others.append(lax.ppermute(parts[place], "grp", [(0, 1), (1, 0)]))
    (mate,) = call(join_kernel, 10**7, parts + others, [conv_weight.shape[1:]])
    span = (share * tokens, sides * 3 * size)
    shared = call(
        functools.partial(regroup_kernel, sides, lines, tokens),
        2 * (group * tokens) ** 2 * span[1],
        got,
        [span] * lines,
        [(group * tokens, span[1])],
    )
    (folded,) = call(
        functools.partial(fold_kernel, sides, 3 * tokens),
        2 * 9 * latent * all_ch * own,
        [*got, kernels[0]],
        [(9 * latent, own)],
        [(latent, all_ch)],
    )
    got = swap(shared, "blk")
    beyond = lax.ppermute(folded, "uly", across)
    folded = swap([folded] * far, "uly") + swap([beyond] * far, "uly")
    (*taps,) = call(
        functools.partial(taps_kernel, sides), 10**7, folded, [(3, 4 * latent, all_ch)] * 2
    )
    block = sides * tokens
    windows = call(
        functools.partial(attention_kernel, sides, lines, share),
        4 * share * size * (lines * block) ** 2,
        got,
        [(3 * block, share * size)] * lines,
        [((lines + 2) * block, share * size)],
    )
    got = swap(windows, "blk")
    (partial,) = call(
        functools.partial(project_kernel, lines),
        2 * 3 * block * lines * share * size * out_weight.shape[1],
        [*got, out_weight],
        [(3 * block, out_weight.shape[1])],
    )
    got = spread(partial, "uly")
    count = (rows + 2) * PATCH
    (current,) = call(
        functools.partial(first_kernel, sides, rows, cols, height),
        18 * count * width * all_ch * own,
        [*got, *taps, conv_weight],
        [(count * width, own)],
        [((count + 2) * width, all_ch)],
    )
    layer, last = SHARED, SHARED + 1
    got = spread(current, "uly")
    total, later = call(
        functools.partial(near_kernel, layer, sides, half),
        9 * count * width * all_ch * own,
        [*got[:far], conv_weight],
        [((count - 2) * width, 3 * own), (3, 3 * own, far * own)],
        sums=(0,),
    )
    (current,) = call(
        functools.partial(layer_kernel, layer, sides, half, rows * PATCH, height),
        36 * count * width * all_ch * own,
        [total, *got, later, mate],
        [((count - 2) * width, 2 * own)],
        [(count * width, all_ch)],
    )
    count -= 4
    _, *got = swap([current] * far, "uly")
    total, *later = call(
        functools.partial(early_kernel, last, sides, half),
        9 * count * width * all_ch * own,
        [current, conv_weight],
        [(count * width, 3 * own)] + [(3, 3 * own, 2 * own)] * len(got),
        sums=(0,),
    )
    (current,) = call(
        functools.partial(last_kernel, last, half, rows * PATCH, height),
        9 * count * width * all_ch * own,
        [total, *got, *later],
        [(count * width, own)],
    )
    return current.reshape(1, count, width, own)


def body(qkv, out_weight, lift_weight, conv_weight):
    if fits_kernels(qkv, lift_weight, conv_weight):
        return body_by_kernels(qkv, out_weight, lift_weight, conv_weight)
    rows, heads = qkv.shape[1], qkv.shape[4]
    lines, sides = lax.axis_size("blk"), lax.axis_size("uly")
    side = lax.axis_index("uly")
    latent_ch = lift_weight.shape[0]
    own = conv_weight.shape[3]
    reach = -(-LAYERS // PATCH)
    lifts = gathered(lift_weight, side)
    folded = jnp.einsum(
        "abdc,ec->abde", conv_weight[0], lifts, preferred_element_type=jnp.float32
    )
    folded = ordered(spread(folded.astype(jnp.bfloat16), "uly"), side)
    folded = jnp.transpose(folded, (1, 2, 0, 3, 4)).reshape(3, 3, sides * own, latent_ch)
    powers = lines & (lines - 1) == 0 and sides & (sides - 1) == 0
    if powers and heads % (lines * sides) == 0:
        patches = window_by_swaps(qkv, out_weight, reach)
    else:
        patches = window_by_gathers(qkv, out_weight, reach)
    height = lines * rows * PATCH
    margin = LAYERS - 1
    start = lax.axis_index("blk") * rows * PATCH
    latent = unfold_patches(patches, latent_ch)
    spare = reach * PATCH - LAYERS
    latent = latent[:, spare : latent.shape[1] - spare]
    current = activate(convolve(latent, folded), start - margin, height)
    for layer in range(1, LAYERS):
        margin -= 1
        kernels = conv_weight[layer]
        if layer > 1:
            current = gathered(current, side)
        current = activate(convolve(current, kernels), start - margin, height)
    return current


def solution(mesh):
    in_specs = (
        P("grp", "blk", "uly", None, None, None),
        P(),
        P(None, "uly"),
        P(None, None, None, "uly", None),
    )
    out_specs = P("grp", "blk", None, "uly")
    return jax.shard_map(
        body, mesh=mesh, in_specs=in_specs, out_specs=out_specs, check_vma=False
    )
```

```python
import functools
import math

import jax
import jax.numpy as jnp
from jax import lax
from jax.experimental import pallas as pl
from jax.experimental.pallas import tpu as pltpu
from jax.sharding import PartitionSpec as P


PATCH = 2
LAYERS = 4
GRANT = 8 * 2**20
SHARED = 2


def swap(pieces, axis):
    count = lax.axis_size(axis)
    got = [pieces[0]]
    for step in range(1, len(pieces)):
        got.append(lax.ppermute(pieces[step], axis, [(i, i ^ step) for i in range(count)]))
    return got


def spread(piece, axis):
    return swap([piece] * lax.axis_size(axis), axis)


def cut(array, start, size, axis):
    return lax.dynamic_slice_in_dim(array, start, size, axis=axis)


def attend(queries, keys, values):
    scale = 1.0 / queries.shape[-1] ** 0.5
    scores = jnp.einsum("hqd,hkd->hqk", queries, keys, preferred_element_type=jnp.float32) * scale
    weights = jnp.exp(scores - jnp.max(scores, axis=2, keepdims=True))
    totals = jnp.sum(weights, axis=2)
    mixed = jnp.einsum(
        "hqk,hkd->hqd", weights.astype(jnp.bfloat16), values, preferred_element_type=jnp.float32
    )
    return (mixed / totals[:, :, None]).astype(jnp.bfloat16)


def ordered(blocks, me):
    stacked = jnp.stack(blocks)
    return jnp.concatenate(
        [cut(stacked, me ^ place, 1, 0) for place in range(len(blocks))], axis=0
    )


def gathered(piece, side):
    blocks = ordered(spread(piece, "uly"), side)
    blocks = jnp.moveaxis(blocks, 0, -2)
    return blocks.reshape(piece.shape[:-1] + (-1,))


def window_by_swaps(qkv, out_weight, reach):
    frames, rows, cols, _, heads, size = qkv.shape
    lines, sides = lax.axis_size("blk"), lax.axis_size("uly")
    line, side = lax.axis_index("blk"), lax.axis_index("uly")
    group, share = heads // sides, heads // sides // lines
    got = swap([cut(qkv, (side ^ s) * group, group, 4) for s in range(sides)], "uly")
    grouped = jnp.stack(got, axis=3)
    grouped = jnp.transpose(grouped, (4, 5, 0, 1, 3, 2, 6))
    got = swap([cut(grouped, (line ^ t) * share, share, 1) for t in range(lines)], "blk")
    shared = ordered(got, line)
    shared = jnp.transpose(shared, (1, 2, 3, 0, 4, 5, 6, 7))
    flat = shared.reshape(3, share, -1, size)
    attended = attend(flat[0], flat[1], flat[2])
    attended = attended.reshape(share, frames, lines * rows, sides * cols, size)
    attended = jnp.transpose(attended, (1, 2, 3, 0, 4)).reshape(
        frames, lines * rows, sides * cols, share * size
    )
    padded = jnp.pad(attended, ((0, 0), (reach, reach), (0, 0), (0, 0)))
    got = swap([cut(padded, (line ^ t) * rows, rows + 2 * reach, 1) for t in range(lines)], "blk")
    partial = 0.0
    for t in range(lines):
        weight = cut(out_weight, ((side * lines) + (line ^ t)) * share * size, share * size, 0)
        partial = partial + jnp.einsum(
            "frcw,wp->frcp", got[t], weight, preferred_element_type=jnp.float32
        )
    partial = partial.astype(jnp.bfloat16)
    got = spread(partial, "uly")
    blocks = []
    for place in range(sides):
        total = 0.0
        for s in range(sides):
            at = (place ^ s) * cols
            total = total + got[s][:, :, at : at + cols].astype(jnp.float32)
        blocks.append(total.astype(jnp.bfloat16))
    patches = ordered(blocks, side)
    patches = jnp.transpose(patches, (1, 2, 0, 3, 4))
    return patches.reshape(frames, rows + 2 * reach, sides * cols, -1)


def window_by_gathers(qkv, out_weight, reach):
    frames, rows, cols, _, heads, size = qkv.shape
    grouped = lax.all_to_all(qkv, "blk", split_axis=4, concat_axis=1, tiled=True)
    flat = [
        lax.all_gather(grouped[:, :, :, which], "uly", axis=2, tiled=True) for which in (1, 2)
    ]
    flat = [grouped[:, :, :, 0]] + flat
    flat = [jnp.swapaxes(one.reshape(-1, one.shape[3], size), 0, 1) for one in flat]
    attended = jnp.swapaxes(attend(*flat), 0, 1)
    attended = attended.reshape(grouped.shape[:3] + grouped.shape[4:])
    restored = lax.all_to_all(attended, "blk", split_axis=1, concat_axis=3, tiled=True)
    patches = jnp.einsum(
        "frcw,wp->frcp",
        restored.reshape(frames, rows, cols, heads * size),
        out_weight,
        preferred_element_type=jnp.float32,
    ).astype(jnp.bfloat16)
    patches = lax.all_gather(patches, "uly", axis=2, tiled=True)
    patches = lax.all_gather(patches, "blk", axis=1, tiled=True)
    padded = jnp.pad(patches, ((0, 0), (reach, reach), (0, 0), (0, 0)))
    return cut(padded, lax.axis_index("blk") * rows, rows + 2 * reach, 1)


def unfold_patches(piece, latent_ch):
    frames, rows, cols = (piece.shape[0], piece.shape[1], piece.shape[2])
    parts = piece.reshape(frames, rows, cols, PATCH, PATCH, latent_ch)
    parts = jnp.transpose(parts, (0, 1, 3, 2, 4, 5))
    return parts.reshape(frames, rows * PATCH, cols * PATCH, latent_ch)


def convolve(current, kernels):
    return lax.conv_general_dilated(
        current,
        kernels,
        (1, 1),
        ((0, 0), (1, 1)),
        dimension_numbers=("NHWC", "HWOI", "NHWC"),
        preferred_element_type=jnp.float32,
    )


def activate(summed, first, height):
    rows = first + lax.broadcasted_iota(jnp.int32, summed.shape, 1)
    inside = (rows >= 0) & (rows < height)
    return jnp.where(inside, jax.nn.silu(summed), 0.0).astype(jnp.bfloat16)


def dot(left, right):
    return jnp.dot(left, right, preferred_element_type=jnp.float32)


def dot_rows(left, right):
    return lax.dot_general(
        left, right, (((1,), (1,)), ((), ())), preferred_element_type=jnp.float32
    )


def picked(source, count):
    rows = source.shape[0]
    places = lax.broadcasted_iota(jnp.int32, (rows, count), 1)
    return jnp.where(places == source, 1.0, 0.0).astype(jnp.bfloat16)


def line_of(rows):
    return lax.broadcasted_iota(jnp.int32, (rows, 1), 0)


def bits(number):
    return number.bit_length() - 1


def call(kernel, flops, inputs, outputs, scratch=(), far=(), sums=()):
    near = pl.BlockSpec(memory_space=pltpu.VMEM)
    kept = pl.BlockSpec(memory_space=pltpu.HBM)
    moved = sum(one.size for one in inputs) + sum(math.prod(shape) for shape in outputs)
    return pl.pallas_call(
        kernel,
        out_shape=[
            jax.ShapeDtypeStruct(shape, jnp.float32 if place in sums else jnp.bfloat16)
            for place, shape in enumerate(outputs)
        ],
        in_specs=[kept if place in far else near for place in range(len(inputs))],
        out_specs=[near] * len(outputs),
        scratch_shapes=[
            pltpu.VMEM(one, jnp.bfloat16) if isinstance(one, tuple) else one for one in scratch
        ],
        compiler_params=pltpu.CompilerParams(vmem_limit_bytes=GRANT),
        cost_estimate=pl.CostEstimate(
            flops=flops, transcendentals=0, bytes_accessed=2 * moved
        ),
    )(*[
        pltpu.with_memory_space_constraint(one, pltpu.HBM) if place in far else one
        for place, one in enumerate(inputs)
    ])


def pack_kernel(sides, flat, lift, *refs):
    out, sems = refs[:sides], refs[sides]
    group, count = out[0].shape[1], flat.shape[0]
    side = lax.axis_index("uly")
    copies = []
    for s in reversed(range(sides)):
        heads = pl.ds(pl.multiple_of((side ^ s) * group, group), group)
        for place, source, target in (
            (s, flat.at[:, heads], out[s].at[pl.ds(0, count)]),
            (sides + s, lift, out[s].at[pl.ds(count, lift.shape[0])]),
        ):
            copies.append(pltpu.make_async_copy(source, target, sems.at[place]))
    for copy in copies:
        copy.start()
    for copy in copies:
        copy.wait()


def load_kernel(layers, kernels, *refs):
    out, sems = refs[:-1], refs[-1]
    sources = [kernels.at[layer] for layer in layers]
    parts = len(out) - len(layers)
    for place in range(parts):
        part = out[-1].shape[3]
        at = (lax.axis_index("grp") * parts + place) * part
        sources.append(kernels.at[SHARED, :, :, :, pl.ds(pl.multiple_of(at, part), part)])
    copies = [
        pltpu.make_async_copy(sources[place], out[place], sems.at[place])
        for place in reversed(range(len(sources)))
    ]
    for copy in copies:
        copy.start()
    for copy in copies:
        copy.wait()


def join_kernel(*refs):
    parts, out = refs[:-1], refs[-1]
    size, each = parts[0].shape[3], len(parts) // 2
    group = lax.axis_index("grp")
    for place, part in enumerate(parts):
        owner = group if place < each else 1 - group
        place = (owner * each + place % each) ^ lax.axis_index("uly")
        at = pl.multiple_of(place * size, size)
        out[:, :, :, pl.ds(at, size)] = part[...]


def regroup_kernel(sides, lines, tokens, *refs):
    pieces, out, held = refs[:sides], refs[sides : sides + lines], refs[-1]
    _, group, size = pieces[0].shape
    flat = jnp.concatenate(
        [
            piece[: 3 * tokens]
            .reshape(tokens, 3, group, size)[:, which]
            .astype(jnp.float32)
            .reshape(tokens * group, size)
            for piece in pieces
            for which in range(3)
        ],
        axis=1,
    ).astype(jnp.bfloat16)
    at = line_of(group * tokens)
    source = ((at & (tokens - 1)) << bits(group)) + (at >> bits(tokens))
    held[...] = dot(picked(source, tokens * group), flat).astype(jnp.bfloat16)
    line = lax.axis_index("blk")
    span = group * tokens // lines
    for t in range(lines):
        out[t][...] = held[pl.ds(pl.multiple_of((line ^ t) * span, span), span), :]


def attention_kernel(sides, lines, share, *refs):
    pieces, out, held = refs[:lines], refs[lines : 2 * lines], refs[-1]
    tokens = pieces[0].shape[0] // share
    size = pieces[0].shape[1] // (3 * sides)
    block = sides * tokens
    scale = 1.0 / size**0.5
    line = lax.axis_index("blk")
    empty = jnp.zeros((block, held.shape[1]), jnp.bfloat16)
    held[:block] = empty
    held[held.shape[0] - block :] = empty
    wide = [piece[...].astype(jnp.float32) for piece in pieces]
    for head in range(share):
        q, k, v = [
            jnp.concatenate(
                [
                    piece[
                        head * tokens : (head + 1) * tokens,
                        (s * 3 + which) * size : (s * 3 + which + 1) * size,
                    ]
                    for piece in wide
                    for s in range(sides)
                ],
                axis=0,
            ).astype(jnp.bfloat16)
            for which in range(3)
        ]
        scores = dot_rows(q, k) * scale
        weights = jnp.exp(scores - jnp.max(scores, axis=1, keepdims=True))
        totals = jnp.sum(weights, axis=1, keepdims=True)
        mixed = (dot(weights.astype(jnp.bfloat16), v) / totals).astype(jnp.bfloat16)
        for t in range(lines):
            at = pl.multiple_of(((line ^ t) + 1) * block, block)
            held[pl.ds(at, block), head * size : (head + 1) * size] = mixed[
                t * block : (t + 1) * block
            ]
    for t in range(lines):
        at = pl.multiple_of((line ^ t) * block, block)
        out[t][...] = held[pl.ds(at, 3 * block), :]


def project_kernel(lines, *refs):
    pieces, weights, out = refs[:lines], refs[lines], refs[-1]
    line, side = lax.axis_index("blk"), lax.axis_index("uly")
    depth = pieces[0].shape[1]
    summed = 0.0
    for t in range(lines):
        at = pl.multiple_of((side * lines + (line ^ t)) * depth, depth)
        summed = summed + dot(pieces[t][...], weights[pl.ds(at, depth), :])
    out[...] = summed.astype(jnp.bfloat16)


def fold_kernel(sides, skip, *refs):
    pieces, kernels, out, held = refs[:sides], refs[sides], refs[-2], refs[-1]
    latent, own = out.shape[0] // 9, out.shape[1]
    side = lax.axis_index("uly")
    for s in range(sides):
        lift = pieces[s][skip:].astype(jnp.float32).reshape(latent, own).astype(jnp.bfloat16)
        held[:, pl.ds(pl.multiple_of((side ^ s) * own, own), own)] = lift
    lift = held[...]
    for tap in range(9):
        product = dot_rows(lift, kernels[tap // 3, tap % 3])
        out[tap * latent : (tap + 1) * latent, :] = product.astype(jnp.bfloat16)


def activated(summed, first, width, height):
    row = first + (line_of(summed.shape[0]) >> bits(width))
    inside = (row >= 0) & (row < height)
    return jnp.where(inside, jax.nn.silu(summed), 0.0)


def shifted(summed, half, own):
    size = summed.shape[0]
    summed = summed.reshape(size // (2 * half), 2, half, 3 * own)

    def part(parity, tap):
        return summed[:, parity, :, tap * own : (tap + 1) * own].reshape(size // 2, own)

    column = line_of(size // 2) & (half - 1)
    before = jnp.where(column == 0, 0.0, pltpu.roll(part(1, 0), 1, 0))
    after = jnp.where(column == half - 1, 0.0, pltpu.roll(part(0, 2), size // 2 - 1, 0))
    even = before + part(0, 1) + part(1, 2)
    odd = part(0, 0) + part(1, 1) + after
    both = [one.reshape(size // (2 * half), 1, half, own) for one in (even, odd)]
    return jnp.concatenate(both, axis=1).reshape(size, own)


def convolved(current, kernels, half):
    width = 2 * half
    size = current.shape[0] - 2 * width
    summed = 0.0
    for above in range(3):
        taps = kernels[above]
        taps = taps.reshape(-1, taps.shape[-1])
        summed = summed + dot_rows(current[above * width : above * width + size, :], taps)
    return summed


def taps_kernel(sides, *refs):
    folded, even_taps, odd_taps = refs[:sides], refs[-2], refs[-1]
    side = lax.axis_index("uly")
    latent = folded[0].shape[0] // 9
    own = folded[0].shape[1]
    empty = jnp.zeros((latent, sides * own), jnp.bfloat16)
    for above in range(3):
        even_taps[above, 2 * latent : 3 * latent, :] = empty
        odd_taps[above, 3 * latent :, :] = empty
        for s in range(sides):
            lanes = pl.ds(pl.multiple_of((side ^ s) * own, own), own)
            for beside in range(3):
                at = (above * 3 + beside) * latent
                taps = folded[s][at : at + latent, :]
                to = (3, 0, 1)[beside] * latent
                even_taps[above, to : to + latent, lanes] = taps
                odd_taps[above, beside * latent : (beside + 1) * latent, lanes] = taps


def first_kernel(sides, rows, cols, height, *refs):
    partials, (even_taps, odd_taps, kernels, out, held) = refs[:sides], refs[sides:]
    kernels = kernels.at[1]
    side, line = lax.axis_index("uly"), lax.axis_index("blk")
    half = sides * cols
    count = partials[0].shape[0]
    latent = even_taps.shape[1] // 4
    own = kernels.shape[2]
    at = line_of(count)
    column = at & (cols - 1)
    group = (at >> bits(cols)) & (sides - 1)
    row = (at >> bits(half)) & (rows - 1)
    block = at >> bits(half * rows)
    picks = []
    for s in range(sides):
        source = (((block << bits(sides)) + (group ^ side ^ s)) << bits(rows)) + row
        picks.append((source << bits(cols)) + column)
    places = lax.broadcasted_iota(jnp.int32, (count, sides * count), 1)
    hits = places == picks[0]
    for s in range(1, sides):
        hits = hits | (places == picks[s] + s * count)
    picks = jnp.where(hits, 1.0, 0.0).astype(jnp.bfloat16)
    total = dot(picks, jnp.concatenate([piece[...] for piece in partials], axis=0))
    total = total.astype(jnp.bfloat16).astype(jnp.float32)
    wide = 2 * latent
    lines = [
        total[:, i * wide : (i + 1) * wide].reshape(count // half, 1, half, wide) for i in range(2)
    ]
    latents = jnp.concatenate(lines, axis=1).reshape(2 * count, wide)
    place = line_of(2 * count) & (half - 1)
    before = jnp.where(place == 0, 0.0, pltpu.roll(latents, 1, 0))
    after = jnp.where(place == half - 1, 0.0, pltpu.roll(latents, 2 * count - 1, 0))
    start = line * rows * PATCH - (LAYERS - 1)
    size = 2 * count - 2 * half
    for parity, (other, taps) in enumerate(((before, even_taps), (after, odd_taps))):
        current = jnp.concatenate([latents, other], axis=1).astype(jnp.bfloat16)
        summed = 0.0
        for above in range(3):
            summed = summed + dot(current[above * half : above * half + size], taps[above])
        summed = activated(summed, start, half, height).astype(jnp.bfloat16)
        for row in range(size // half):
            at = (2 * row + parity) * half
            held[at : at + half, :] = summed[row * half : (row + 1) * half]
    summed = shifted(convolved(held, kernels, half), half, own)
    out[...] = activated(summed, start + 1, 2 * half, height).astype(jnp.bfloat16)


def met(kernels, above, places):
    own = kernels.shape[2]
    lanes = [pl.ds(pl.multiple_of(place * own, own), own) for place in places]
    taps = [kernels[above, :, :, lane].reshape(3 * own, own) for lane in lanes]
    return jnp.concatenate(taps, axis=1)


def near_kernel(layer, sides, half, *refs):
    near = sides // 2
    pieces, kernels, total, later = refs[:near], refs[near].at[layer], refs[-2], refs[-1]
    side = lax.axis_index("uly")
    current = jnp.concatenate([piece[...] for piece in pieces], axis=1)
    taps = [met(kernels, above, [side ^ s for s in range(near)]) for above in range(3)]
    total[...] = convolved(current, taps, half)
    for above in range(3):
        later[above] = met(kernels, above, [side ^ s for s in range(near, sides)])


def layer_kernel(layer, sides, half, step, height, *refs):
    total, pieces, (later, mate, out) = refs[0], refs[1 : 1 + sides], refs[1 + sides :]
    line = lax.axis_index("blk")
    own = mate.shape[2]
    first = line * step + layer + 1 - LAYERS
    current = jnp.concatenate([piece[...] for piece in pieces], axis=1)
    rest = current[:, sides // 2 * own :]
    sums = (total[...] + convolved(rest, later, half), convolved(current, mate, half))
    for place, summed in enumerate(sums):
        summed = shifted(summed, half, own)
        result = activated(summed, first, 2 * half, height).astype(jnp.bfloat16)
        out[:, place * own : (place + 1) * own] = result


def early_kernel(layer, sides, half, *refs):
    piece, kernels, total, later = refs[0], refs[1].at[layer], refs[2], refs[3:]
    side = lax.axis_index("uly")
    own = kernels.shape[2]

    def met(above, s):
        places = [side ^ s, side ^ s ^ (sides // 2)]
        lanes = [pl.ds(pl.multiple_of(place * own, own), own) for place in places]
        taps = [kernels[above, :, :, lane].reshape(3 * own, own) for lane in lanes]
        return jnp.concatenate(taps, axis=1)

    total[...] = convolved(piece, [met(above, 0) for above in range(3)], half)
    for s, out in enumerate(later, 1):
        for above in range(3):
            out[above] = met(above, s)


def last_kernel(layer, half, step, height, *refs):
    count = (len(refs) - 2) // 2
    total, pieces, kernels, out = refs[0], refs[1 : 1 + count], refs[1 + count : -1], refs[-1]
    summed = total[...]
    for piece, taps in zip(pieces, kernels):
        summed = summed + convolved(piece, taps, half)
    width = 2 * half
    first = lax.axis_index("blk") * step + layer + 1 - LAYERS
    summed = shifted(summed, half, summed.shape[1] // 3)
    result = activated(summed, first, width, height).astype(jnp.bfloat16)
    at = line_of(result.shape[0])
    column = at & (width - 1)
    source = (at - column) + ((column & 1) << bits(half)) + (column >> 1)
    out[...] = dot(picked(source, result.shape[0]), result).astype(jnp.bfloat16)


def fits_kernels(qkv, lift_weight, conv_weight):
    frames, rows, cols, _, heads, size = qkv.shape
    lines, sides = lax.axis_size("blk"), lax.axis_size("uly")
    powers = all(n & (n - 1) == 0 for n in (lines, sides, rows, cols, heads))
    return (
        powers
        and lax.axis_size("grp") == 2
        and sides == 4
        and frames == 1
        and LAYERS == SHARED + 2
        and rows * PATCH == LAYERS
        and heads % (lines * sides) == 0
        and rows * cols % 8 == 0
        and rows * cols * heads // (lines * sides) % 16 == 0
        and rows * cols * sides % 32 == 0
        and sides * cols % 16 == 0
        and heads // sides % 8 == 0
        and size % 128 == 0
        and conv_weight.shape[3] % 128 == 0
        and lift_weight.size % (heads // sides * size) == 0
        and conv_weight.shape[3] == size
        and lift_weight.shape[0] * 2 % 128 == 0
    )


def body_by_kernels(qkv, out_weight, lift_weight, conv_weight):
    _, rows, cols, _, heads, size = qkv.shape
    lines, sides = lax.axis_size("blk"), lax.axis_size("uly")
    group, share = heads // sides, heads // sides // lines
    latent, own = lift_weight.shape
    tokens, half = rows * cols, sides * cols
    height = lines * rows * PATCH
    width, all_ch = 2 * half, sides * own
    pieces = call(
        functools.partial(pack_kernel, sides),
        0,
        [qkv.reshape(3 * tokens, heads, size), lift_weight.reshape(-1, group, size)],
        [(3 * tokens + lift_weight.size // (group * size), group, size)] * sides,
        [pltpu.SemaphoreType.DMA((2 * sides,))],
        far=(0, 1),
    )
    got = swap(pieces, "uly")

    def load(layers, extra):
        shapes = [conv_weight.shape[1:]] * len(layers) + extra
        return call(
            functools.partial(load_kernel, layers),
            10**8,
            [conv_weight],
            shapes,
            [pltpu.SemaphoreType.DMA((len(shapes),))],
            far=(0,),
        )

    far = sides // 2
    across = [(i, i ^ far) for i in range(sides)]
    kernels = {}
    quarter = conv_weight.shape[1:4] + (all_ch // 4,)
    kernels[0], *parts = load([0], [quarter] * 2)
    others = []
    for place in range(2):
        parts[place] = lax.ppermute(parts[place], "uly", across)
        others.append(lax.ppermute(parts[place], "grp", [(0, 1), (1, 0)]))
    (mate,) = call(join_kernel, 10**7, parts + others, [conv_weight.shape[1:]])
    span = (share * tokens, sides * 3 * size)
    shared = call(
        functools.partial(regroup_kernel, sides, lines, tokens),
        2 * (group * tokens) ** 2 * span[1],
        got,
        [span] * lines,
        [(group * tokens, span[1])],
    )
    (folded,) = call(
        functools.partial(fold_kernel, sides, 3 * tokens),
        2 * 9 * latent * all_ch * own,
        [*got, kernels[0]],
        [(9 * latent, own)],
        [(latent, all_ch)],
    )
    got = swap(shared, "blk")
    beyond = lax.ppermute(folded, "uly", across)
    folded = swap([folded] * far, "uly") + swap([beyond] * far, "uly")
    (*taps,) = call(
        functools.partial(taps_kernel, sides), 10**7, folded, [(3, 4 * latent, all_ch)] * 2
    )
    block = sides * tokens
    windows = call(
        functools.partial(attention_kernel, sides, lines, share),
        4 * share * size * (lines * block) ** 2,
        got,
        [(3 * block, share * size)] * lines,
        [((lines + 2) * block, share * size)],
    )
    got = swap(windows, "blk")
    (partial,) = call(
        functools.partial(project_kernel, lines),
        2 * 3 * block * lines * share * size * out_weight.shape[1],
        [*got, out_weight],
        [(3 * block, out_weight.shape[1])],
    )
    got = spread(partial, "uly")
    count = (rows + 2) * PATCH
    (current,) = call(
        functools.partial(first_kernel, sides, rows, cols, height),
        18 * count * width * all_ch * own,
        [*got, *taps, conv_weight],
        [(count * width, own)],
        [((count + 2) * width, all_ch)],
    )
    layer, last = SHARED, SHARED + 1
    got = spread(current, "uly")
    total, later = call(
        functools.partial(near_kernel, layer, sides, half),
        9 * count * width * all_ch * own,
        [*got[:far], conv_weight],
        [((count - 2) * width, 3 * own), (3, 3 * own, far * own)],
        sums=(0,),
    )
    (current,) = call(
        functools.partial(layer_kernel, layer, sides, half, rows * PATCH, height),
        36 * count * width * all_ch * own,
        [total, *got, later, mate],
        [((count - 2) * width, 2 * own)],
    )
    count -= 4
    _, *got = swap([current] * far, "uly")
    total, *later = call(
        functools.partial(early_kernel, last, sides, half),
        9 * count * width * all_ch * own,
        [current, conv_weight],
        [(count * width, 3 * own)] + [(3, 3 * own, 2 * own)] * len(got),
        sums=(0,),
    )
    (current,) = call(
        functools.partial(last_kernel, last, half, rows * PATCH, height),
        9 * count * width * all_ch * own,
        [total, *got, *later],
        [(count * width, own)],
    )
    return current.reshape(1, count, width, own)


def body(qkv, out_weight, lift_weight, conv_weight):
    if fits_kernels(qkv, lift_weight, conv_weight):
        return body_by_kernels(qkv, out_weight, lift_weight, conv_weight)
    rows, heads = qkv.shape[1], qkv.shape[4]
    lines, sides = lax.axis_size("blk"), lax.axis_size("uly")
    side = lax.axis_index("uly")
    latent_ch = lift_weight.shape[0]
    own = conv_weight.shape[3]
    reach = -(-LAYERS // PATCH)
    lifts = gathered(lift_weight, side)
    folded = jnp.einsum(
        "abdc,ec->abde", conv_weight[0], lifts, preferred_element_type=jnp.float32
    )
    folded = ordered(spread(folded.astype(jnp.bfloat16), "uly"), side)
    folded = jnp.transpose(folded, (1, 2, 0, 3, 4)).reshape(3, 3, sides * own, latent_ch)
    powers = lines & (lines - 1) == 0 and sides & (sides - 1) == 0
    if powers and heads % (lines * sides) == 0:
        patches = window_by_swaps(qkv, out_weight, reach)
    else:
        patches = window_by_gathers(qkv, out_weight, reach)
    height = lines * rows * PATCH
    margin = LAYERS - 1
    start = lax.axis_index("blk") * rows * PATCH
    latent = unfold_patches(patches, latent_ch)
    spare = reach * PATCH - LAYERS
    latent = latent[:, spare : latent.shape[1] - spare]
    current = activate(convolve(latent, folded), start - margin, height)
    for layer in range(1, LAYERS):
        margin -= 1
        kernels = conv_weight[layer]
        if layer > 1:
            current = gathered(current, side)
        current = activate(convolve(current, kernels), start - margin, height)
    return current


def solution(mesh):
    in_specs = (
        P("grp", "blk", "uly", None, None, None),
        P(),
        P(None, "uly"),
        P(None, None, None, "uly", None),
    )
    out_specs = P("grp", "blk", None, "uly")
    return jax.shard_map(
        body, mesh=mesh, in_specs=in_specs, out_specs=out_specs, check_vma=False
    )
```
